256 devices in a mesh: prow: 16 (over y, x), pcol: 16 (over z, core).
Axes of the slice: x: 4, y: 4, z: 8, core: 2. Of those that a mesh axis runs over, the one named last changes fastest.
Arguments:
- blocked: float32 [16384, 16384], P('prow', 'pcol'), may hold values from -6 to 6, as said below
Outputs:
- factored: float32 [16384, 16384], P('prow', 'pcol')
The draws below stay inside these ranges and needn't reach their ends.
Inputs may be any that keep to these rules, and one draw needn't show every extreme that they name: blocked is the block-cyclic storage of a symmetric positive definite matrix whose diagonal is at least 1 plus a nonnegative Gram diagonal and whose condition number is below about 40.
All inputs are finite; a program needn't handle non-finite values.
Results may differ from the reference program's by a relative error of at most 0.0003.
Values sent between devices are 32-bit elements.
No kernel may reach another device: no remote copies, remote signals or barrier semaphores. Data moves between devices by JAX's collectives and lax.ppermute only.
A program may use at most 128 MiB of HBM per device.

```python
import jax
import jax.numpy as jnp
from jax import lax

EMB = 2048
BLOCK = 128
STEPS = 8
N = 16384
N_PROW = 16
N_PCOL = 16


def draw_blocked(key, part):
    first_key, second_key = jax.random.split(jax.random.fold_in(key, 7))
    features = jax.random.normal(first_key, (N, EMB), jnp.float32)
    gram = jnp.dot(features, features.T, precision=lax.Precision.HIGHEST) / EMB
    gram = 0.5 * (gram + gram.T) + jnp.eye(N, dtype=jnp.float32)
    row_blocks = N // (N_PROW * BLOCK)
    col_blocks = N // (N_PCOL * BLOCK)
    gram = gram.reshape(row_blocks, N_PROW, BLOCK, col_blocks, N_PCOL, BLOCK)
    return gram.transpose(1, 0, 2, 4, 3, 5).reshape(N, N)


def setup_inputs(seed: int = 0) -> dict:
    key_of = jax.random.split(jax.random.key(seed), 2)
    blocked = draw_blocked(jax.random.fold_in(key_of[1], 71), 0)
    return dict(blocked=blocked)


def reference(blocked):
    row_blocks = N // (N_PROW * BLOCK)
    col_blocks = N // (N_PCOL * BLOCK)
    matrix = blocked.reshape(N_PROW, row_blocks, BLOCK, N_PCOL, col_blocks, BLOCK)
    matrix = matrix.transpose(1, 0, 2, 4, 3, 5).reshape(N, N)
    width = STEPS * BLOCK
    leading = jnp.tril(jnp.linalg.cholesky(matrix[:width, :width]))
    lower = jax.scipy.linalg.solve_triangular(leading, matrix[width:, :width].T, lower=True).T
    schur = matrix[width:, width:] - jnp.dot(lower, lower.T, precision=lax.Precision.HIGHEST)
    upper_part = jnp.concatenate([leading, jnp.zeros((width, N - width), jnp.float32)], axis=1)
    lower_part = jnp.concatenate([lower, schur], axis=1)
    result = jnp.concatenate([upper_part, lower_part], axis=0)
    result = result.reshape(row_blocks, N_PROW, BLOCK, col_blocks, N_PCOL, BLOCK)
    return result.transpose(1, 0, 2, 4, 3, 5).reshape(N, N)
```

```python
import functools

import jax
import jax.numpy as jnp
from jax import lax
from jax.experimental import pallas as pl
from jax.experimental.pallas import tpu as pltpu
from jax.sharding import PartitionSpec as P

BLOCK = 128
STEPS = 8
WIDTH = STEPS * BLOCK
NB = 32
CHUNK = 256


bf16 = jnp.bfloat16
f32 = jnp.float32


def split(x):
    hi = x.astype(bf16)
    return hi, (x - hi.astype(f32)).astype(bf16)


def dot(a, b, dims=((1,), (0,))):
    return lax.dot_general(a, b, (dims, ((), ())), preferred_element_type=f32)


def dot_split(a, b, dims=((1,), (0,))):
    return dot(a[0], b[0], dims) + dot(a[1], b[0], dims) + dot(a[0], b[1], dims)


def dot_split_128(a, b):
    (ah, al), (bh, bl) = a, b
    return dot(jnp.concatenate([ah, al], 1), jnp.concatenate([bh, bh], 0)) + dot(ah, bl)


def spread(row):
    return jnp.broadcast_to(row, (8, row.shape[1]))


def factor_tile(work_ref):
    tiles = NB // 8
    sub = lax.broadcasted_iota(jnp.int32, (8, 128), 0)
    for base in range(0, BLOCK, NB):
        rows = [
            [work_ref[base + 8 * t : base + 8 * t + 8, h * 128 : h * 128 + 128] for h in range(2)]
            for t in range(tiles)
        ]
        cols = {
            (j, t): jnp.broadcast_to(rows[t][0][:, base + j : base + j + 1], (8, 128))
            for j in range(NB)
            for t in range(j // 8, tiles)
        }
        scale = [None] * tiles
        for k in range(NB):
            tk, rk = divmod(k, 8)
            pivot = spread(cols[k, tk][rk : rk + 1])
            recip = 1.0 / pivot
            root = lax.rsqrt(pivot)
            scale[tk] = root if rk == 0 else jnp.where(sub == rk, root, scale[tk])
            mult = {t: cols[k, t] * recip for t in range(tk, tiles)}
            mult[tk] = jnp.where(sub > rk, mult[tk], 0.0)
            for j in range(k + 1, NB):
                tj, rj = divmod(j, 8)
                c = spread(cols[k, tj][rj : rj + 1])
                for t in range(tj, tiles):
                    cols[j, t] = cols[j, t] - mult[t] * c
            for h in range(2):
                r = spread(rows[tk][h][rk : rk + 1])
                for t in range(tk + rk // 7, tiles):
                    rows[t][h] = rows[t][h] - mult[t] * r
        done = jnp.concatenate(
            [jnp.concatenate([rows[t][h] * scale[t] for h in range(2)], 1) for t in range(tiles)], 0
        )
        end = base + NB
        work_ref[base:end, :] = done
        if end < BLOCK:
            lh, ll = split(jnp.transpose(done[:, :128])[end:])
            uh, ul = split(done)
            left = jnp.concatenate([lh, lh, ll], 1)
            right = jnp.concatenate([uh, ul, uh], 0)
            work_ref[end:, :] = work_ref[end:, :] - dot(left, right)


def factor_kernel(w_ref, x_ref, d_ref, work_ref):
    for j in range(STEPS):
        x_ref[:, j * BLOCK : (j + 1) * BLOCK] = w_ref[j]
    r = lax.broadcasted_iota(jnp.int32, (BLOCK, BLOCK), 0)
    c = lax.broadcasted_iota(jnp.int32, (BLOCK, BLOCK), 1)

    def step(k, _):
        here = pl.ds(pl.multiple_of(k * BLOCK, BLOCK), BLOCK)
        work_ref[:, :128] = x_ref[here, here]
        work_ref[:, 128:] = jnp.where(r == c, 1.0, 0.0).astype(f32)
        factor_tile(work_ref)
        d_ref[here, :] = jnp.where(r <= c, work_ref[:, :128], 0.0)
        inverse = work_ref[:, 128:]
        x_ref[here, :] = dot_split_128(split(inverse), split(x_ref[here, :]))
        x_ref[here, here] = inverse
        right = split(x_ref[here, :])

        def update(j, _):
            there = pl.ds(pl.multiple_of(j * BLOCK, BLOCK), BLOCK)
            left = split(jnp.transpose(x_ref[here, there]))
            x_ref[there, here] = jnp.zeros((BLOCK, BLOCK), f32)
            x_ref[there, :] = x_ref[there, :] - dot_split_128(left, right)
            return 0

        lax.fori_loop(k + 1, STEPS, update, 0)
        return 0

    lax.fori_loop(0, STEPS, step, 0)


def factor(gathered):
    vmem = pl.BlockSpec(memory_space=pltpu.VMEM)
    return pl.pallas_call(
        factor_kernel,
        grid=(1,),
        in_specs=[pl.BlockSpec((STEPS, WIDTH, BLOCK), lambda i: (1, 0, 0))],
        out_specs=(
            pl.BlockSpec((WIDTH, WIDTH), lambda i: (0, 0)),
            pl.BlockSpec((WIDTH, BLOCK), lambda i: (0, 0)),
        ),
        out_shape=(
            jax.ShapeDtypeStruct((WIDTH, WIDTH), f32),
            jax.ShapeDtypeStruct((WIDTH, BLOCK), f32),
        ),
        scratch_shapes=[pltpu.VMEM((BLOCK, 2 * BLOCK), f32)],
        compiler_params=pltpu.CompilerParams(vmem_limit_bytes=40 * 2**20),
        cost_estimate=pl.CostEstimate(flops=40_000_000_000, bytes_accessed=2**23, transcendentals=0),
        name="factor",
    )(gathered)


def update_kernel(place_ref, a_ref, u_ref, v_ref, x_ref, d_ref, out_ref, mh, ml, vh, vl, ch, cl, r_ref):
    row, col, step = place_ref[0], place_ref[1], pl.program_id(0)

    @pl.when(step == 0)
    def _():
        rb = lax.broadcasted_iota(jnp.int32, (BLOCK, WIDTH), 1) // BLOCK
        for k in range(STEPS):
            at = slice(k * BLOCK, (k + 1) * BLOCK)
            mh[at], ml[at] = split(jnp.where(rb <= k, x_ref[at], 0.0))
            vh[at], vl[at] = split(v_ref[at])
        for k in range(0, WIDTH, CHUNK):
            at, upto = slice(k, k + CHUNK), slice(0, k + CHUNK)
            ch[at], cl[at] = split(dot_split((mh[at, upto], ml[at, upto]), (vh[upto], vl[upto])))

    uh, ul = split(jnp.concatenate([u_ref[j] for j in range(STEPS)], 1))
    for k in range(0, WIDTH, CHUNK):
        at, upto = slice(k, k + CHUNK), slice(0, k + CHUNK)
        r_ref[:, at] = dot_split((uh[:, upto], ul[:, upto]), (mh[at, upto], ml[at, upto]), ((1,), (1,)))
    out_ref[...] = a_ref[...] - dot_split(split(r_ref[...]), (ch[...], cl[...]))

    @pl.when(col < STEPS)
    def _():
        out_ref[:, :BLOCK] = r_ref[:, pl.ds(pl.multiple_of(col * BLOCK, BLOCK), BLOCK)]

    @pl.when((step == 0) & (row < STEPS))
    def _():
        out_ref[:BLOCK, :] = jnp.zeros((BLOCK, WIDTH), f32)
        mine = pl.ds(pl.multiple_of(jnp.minimum(row, STEPS - 1) * BLOCK, BLOCK), BLOCK)
        other = pl.ds(pl.multiple_of(jnp.minimum(col, STEPS - 1) * BLOCK, BLOCK), BLOCK)

        @pl.when(row == col)
        def _():
            out_ref[:BLOCK, :BLOCK] = jnp.transpose(d_ref[mine, :])

        @pl.when(row > col)
        def _():
            out_ref[:BLOCK, :BLOCK] = jnp.transpose(x_ref[other, mine])


def update(place, blocked, gathered, across, x, d):
    whole = lambda *shape: pl.BlockSpec(shape, lambda i: (0,) * len(shape))
    half = functools.partial(pltpu.VMEM, dtype=bf16)
    return pl.pallas_call(
        update_kernel,
        grid=(WIDTH // CHUNK,),
        in_specs=[
            pl.BlockSpec(memory_space=pltpu.SMEM),
            pl.BlockSpec((CHUNK, WIDTH), lambda i: (i, 0)),
            pl.BlockSpec((STEPS, CHUNK, BLOCK), lambda i: (0, i, 0)),
            whole(WIDTH, WIDTH),
            whole(WIDTH, WIDTH),
            whole(WIDTH, BLOCK),
        ],
        out_specs=pl.BlockSpec((CHUNK, WIDTH), lambda i: (i, 0)),
        out_shape=jax.ShapeDtypeStruct((WIDTH, WIDTH), f32),
        scratch_shapes=[half((WIDTH, WIDTH)) for _ in range(6)] + [pltpu.VMEM((CHUNK, WIDTH), f32)],
        compiler_params=pltpu.CompilerParams(vmem_limit_bytes=56 * 2**20),
        name="update",
    )(place, blocked, gathered, across, x, d)


def per_device(blocked):
    rows, cols = lax.axis_size("prow"), lax.axis_size("pcol")
    row, col = lax.axis_index("prow"), lax.axis_index("pcol")
    half = BLOCK // 2

    parts = [
        lax.ppermute(
            blocked[h * half : (h + 1) * half, :BLOCK],
            ("prow", "pcol"),
            [(i * cols + k, (2 * i + h) * cols + STEPS + k) for i in range(STEPS) for k in range(STEPS)],
        )
        for h in range(2)
    ]
    part = parts[0] + parts[1]
    strip = lax.all_to_all(jnp.broadcast_to(part, (rows, half, BLOCK)), "prow", 0, 0)
    payload = jnp.where(col < STEPS, blocked[:, :BLOCK], strip.reshape(WIDTH, BLOCK))
    gathered = lax.all_gather(payload, "pcol", axis=0)

    parts = [
        lax.ppermute(
            blocked[h * half : (h + 1) * half],
            "prow",
            [(i, 2 * i + h) for i in range(STEPS)],
        )
        for h in range(2)
    ]
    part = jnp.where(row % 2 == 0, parts[0], parts[1])
    part, gathered = lax.optimization_barrier((part, gathered))
    across = lax.all_gather(part, "prow", axis=0, tiled=True)

    x, d = factor(gathered)
    return update(jnp.stack([row, col]), blocked, gathered, across, x, d)


def solution(mesh):
    return jax.shard_map(
        per_device,
        mesh=mesh,
        in_specs=(P("prow", "pcol"),),
        out_specs=P("prow", "pcol"),
        check_vma=False,
    )
```

```python
import functools

import jax
import jax.numpy as jnp
from jax import lax
from jax.experimental import pallas as pl
from jax.experimental.pallas import tpu as pltpu
from jax.sharding import PartitionSpec as P

BLOCK = 128
STEPS = 8
WIDTH = STEPS * BLOCK
HALF = WIDTH // 2
SIDE = 4
NB = 32
CHUNK = 256


bf16 = jnp.bfloat16
f32 = jnp.float32


def split(x):
    hi = x.astype(bf16)
    return hi, (x - hi.astype(f32)).astype(bf16)


def dot(a, b, dims=((1,), (0,))):
    return lax.dot_general(a, b, (dims, ((), ())), preferred_element_type=f32)


def dot_split(a, b, dims=((1,), (0,))):
    return dot(a[0], b[0], dims) + dot(a[1], b[0], dims) + dot(a[0], b[1], dims)


def dot_split_128(a, b):
    (ah, al), (bh, bl) = a, b
    return dot(jnp.concatenate([ah, al], 1), jnp.concatenate([bh, bh], 0)) + dot(ah, bl)


def other_half(k):
    return 14 - k + 2 * (k % 2)


def spread(row):
    return jnp.broadcast_to(row, (8, row.shape[1]))


def factor_tile(work_ref):
    tiles = NB // 8
    sub = lax.broadcasted_iota(jnp.int32, (8, 128), 0)
    for base in range(0, BLOCK, NB):
        rows = [
            [work_ref[base + 8 * t : base + 8 * t + 8, h * 128 : h * 128 + 128] for h in range(2)]
            for t in range(tiles)
        ]
        cols = {
            (j, t): jnp.broadcast_to(rows[t][0][:, base + j : base + j + 1], (8, 128))
            for j in range(NB)
            for t in range(j // 8, tiles)
        }
        scale = [None] * tiles
        for k in range(NB):
            tk, rk = divmod(k, 8)
            pivot = spread(cols[k, tk][rk : rk + 1])
            recip = 1.0 / pivot
            root = lax.rsqrt(pivot)
            scale[tk] = root if rk == 0 else jnp.where(sub == rk, root, scale[tk])
            mult = {t: cols[k, t] * recip for t in range(tk, tiles)}
            mult[tk] = jnp.where(sub > rk, mult[tk], 0.0)
            for j in range(k + 1, NB):
                tj, rj = divmod(j, 8)
                c = spread(cols[k, tj][rj : rj + 1])
                for t in range(tj, tiles):
                    cols[j, t] = cols[j, t] - mult[t] * c
            for h in range(2):
                r = spread(rows[tk][h][rk : rk + 1])
                for t in range(tk + rk // 7, tiles):
                    rows[t][h] = rows[t][h] - mult[t] * r
        done = jnp.concatenate(
            [jnp.concatenate([rows[t][h] * scale[t] for h in range(2)], 1) for t in range(tiles)], 0
        )
        end = base + NB
        work_ref[base:end, :] = done
        if end < BLOCK:
            lh, ll = split(jnp.transpose(done[:, :128])[end:])
            uh, ul = split(done)
            left = jnp.concatenate([lh, lh, ll], 1)
            right = jnp.concatenate([uh, ul, uh], 0)
            work_ref[end:, :] = work_ref[end:, :] - dot(left, right)


def factor_kernel(w_ref, x_ref, d_ref, work_ref, sems):
    copies = []
    for j in range(STEPS):
        for h, slot in enumerate((j, other_half(j))):
            dst = x_ref.at[h * HALF : (h + 1) * HALF, j * BLOCK : (j + 1) * BLOCK]
            copies.append(pltpu.make_async_copy(w_ref.at[slot], dst, sems.at[slot]))
    for copy in copies:
        copy.start()
    for copy in copies:
        copy.wait()
    r = lax.broadcasted_iota(jnp.int32, (BLOCK, BLOCK), 0)
    c = lax.broadcasted_iota(jnp.int32, (BLOCK, BLOCK), 1)

    def step(k, _):
        here = pl.ds(pl.multiple_of(k * BLOCK, BLOCK), BLOCK)
        work_ref[:, :128] = x_ref[here, here]
        work_ref[:, 128:] = jnp.where(r == c, 1.0, 0.0).astype(f32)
        factor_tile(work_ref)
        d_ref[here, :] = jnp.where(r <= c, work_ref[:, :128], 0.0)
        inverse = work_ref[:, 128:]
        x_ref[here, :] = dot_split_128(split(inverse), split(x_ref[here, :]))
        x_ref[here, here] = inverse
        right = split(x_ref[here, :])

        def update(j, _):
            there = pl.ds(pl.multiple_of(j * BLOCK, BLOCK), BLOCK)
            left = split(jnp.transpose(x_ref[here, there]))
            x_ref[there, here] = jnp.zeros((BLOCK, BLOCK), f32)
            x_ref[there, :] = x_ref[there, :] - dot_split_128(left, right)
            return 0

        lax.fori_loop(k + 1, STEPS, update, 0)
        return 0

    lax.fori_loop(0, STEPS, step, 0)


def factor(gathered):
    return pl.pallas_call(
        factor_kernel,
        in_specs=[pl.BlockSpec(memory_space=pltpu.HBM)],
        out_specs=(pl.BlockSpec(memory_space=pltpu.VMEM), pl.BlockSpec(memory_space=pltpu.VMEM)),
        out_shape=(
            jax.ShapeDtypeStruct((WIDTH, WIDTH), f32),
            jax.ShapeDtypeStruct((WIDTH, BLOCK), f32),
        ),
        scratch_shapes=[pltpu.VMEM((BLOCK, 2 * BLOCK), f32), pltpu.SemaphoreType.DMA((2 * STEPS,))],
        compiler_params=pltpu.CompilerParams(vmem_limit_bytes=24 * 2**20),
        cost_estimate=pl.CostEstimate(flops=40_000_000_000, bytes_accessed=2**23, transcendentals=0),
        name="factor",
    )(gathered)


def apply_kernel(place_ref, x_ref, d_ref, *refs):
    v_refs, (yh_ref, yl_ref, panel_ref, corner_ref, mh, ml, vh, vl) = refs[:4], refs[4:]
    row, col = place_ref[0], place_ref[1]
    my_y, my_x = row // SIDE, row % SIDE
    rb = lax.broadcasted_iota(jnp.int32, (BLOCK, WIDTH), 1) // BLOCK
    for k in range(STEPS):
        at = slice(k * BLOCK, (k + 1) * BLOCK)
        mh[at], ml[at] = split(jnp.where(rb <= k, x_ref[at], 0.0))
    swapped = jnp.where((my_y == 1) | (my_y == 2), 1, 0)
    for d, v_ref in enumerate(v_refs):
        for e in range(2):
            block = SIDE * (e + swapped - 2 * e * swapped) + (my_x + d) % SIDE
            at = pl.ds(pl.multiple_of(block * BLOCK, BLOCK), BLOCK)
            vh[at], vl[at] = split(v_ref[e * BLOCK : (e + 1) * BLOCK])
    for k in reversed(range(0, WIDTH, CHUNK)):
        at, upto = slice(k, k + CHUNK), slice(0, k + CHUNK)
        vh[at], vl[at] = split(dot_split((mh[at, upto], ml[at, upto]), (vh[upto], vl[upto])))
    for k in range(0, WIDTH, CHUNK):
        at, on = slice(k, k + CHUNK), slice(k, WIDTH)
        yh_ref[at], yl_ref[at] = split(dot_split((mh[on, at], ml[on, at]), (vh[on], vl[on]), ((0,), (0,))))

    mine = pl.ds(pl.multiple_of(jnp.minimum(row, STEPS - 1) * BLOCK, BLOCK), BLOCK)
    other = pl.ds(pl.multiple_of(jnp.minimum(col, STEPS - 1) * BLOCK, BLOCK), BLOCK)
    panel_ref[...] = jnp.where(rb <= col, x_ref[other, :], 0.0)
    block = jnp.where(row == col, d_ref[mine, :], x_ref[other, mine])
    corner_ref[...] = jnp.where((row >= col) & (row < STEPS), jnp.transpose(block), 0.0)


def apply(place, x, d, across):
    vmem = pl.BlockSpec(memory_space=pltpu.VMEM)
    half = functools.partial(pltpu.VMEM, dtype=bf16)
    return pl.pallas_call(
        apply_kernel,
        in_specs=[pl.BlockSpec(memory_space=pltpu.SMEM)] + [vmem] * 6,
        out_specs=(vmem,) * 4,
        out_shape=(
            jax.ShapeDtypeStruct((WIDTH, WIDTH), bf16),
            jax.ShapeDtypeStruct((WIDTH, WIDTH), bf16),
            jax.ShapeDtypeStruct((BLOCK, WIDTH), f32),
            jax.ShapeDtypeStruct((BLOCK, BLOCK), f32),
        ),
        scratch_shapes=[half((WIDTH, WIDTH)) for _ in range(4)],
        compiler_params=pltpu.CompilerParams(vmem_limit_bytes=22 * 2**20),
        cost_estimate=pl.CostEstimate(flops=8_000_000_000, bytes_accessed=2**23, transcendentals=0),
        name="apply",
    )(place, x, d, *across)


def update_kernel(place_ref, a_ref, u_ref, yh_ref, yl_ref, panel_ref, corner_ref, out_ref):
    row, col, step = place_ref[0], place_ref[1], pl.program_id(0)
    slots = [jnp.where(step < HALF // CHUNK, j, other_half(j) - STEPS) for j in range(STEPS)]
    u = split(jnp.concatenate([u_ref[s] for s in slots], 1))
    out_ref[...] = a_ref[...] - dot_split(u, (yh_ref[...], yl_ref[...]))

    @pl.when(col < STEPS)
    def _():
        out_ref[:, :BLOCK] = dot_split(u, split(panel_ref[...]), ((1,), (1,)))

    @pl.when((step == 0) & (row < STEPS))
    def _():
        out_ref[:BLOCK, :] = jnp.zeros((BLOCK, WIDTH), f32)

        @pl.when(col < STEPS)
        def _():
            out_ref[:BLOCK, :BLOCK] = corner_ref[...]


def update(place, blocked, gathered, yh, yl, panel, corner):
    whole = lambda *shape: pl.BlockSpec(shape, lambda i: (0,) * len(shape))
    per_half = HALF // CHUNK
    return pl.pallas_call(
        update_kernel,
        grid=(WIDTH // CHUNK,),
        in_specs=[
            pl.BlockSpec(memory_space=pltpu.SMEM),
            pl.BlockSpec((CHUNK, WIDTH), lambda i: (i, 0)),
            pl.BlockSpec((STEPS, CHUNK, BLOCK), lambda i: (i // per_half, i % per_half, 0)),
            whole(WIDTH, WIDTH),
            whole(WIDTH, WIDTH),
            whole(BLOCK, WIDTH),
            whole(BLOCK, BLOCK),
        ],
        out_specs=pl.BlockSpec((CHUNK, WIDTH), lambda i: (i, 0)),
        out_shape=jax.ShapeDtypeStruct((WIDTH, WIDTH), f32),
        compiler_params=pltpu.CompilerParams(vmem_limit_bytes=22 * 2**20),
        name="update",
    )(place, blocked, gathered, yh, yl, panel, corner)


def per_device(blocked):
    rows, cols = lax.axis_size("prow"), lax.axis_size("pcol")
    row, col = lax.axis_index("prow"), lax.axis_index("pcol")
    span = range(STEPS)

    quarter = BLOCK // 4
    parts = []
    for g in range(4):
        pairs = [
            (i * cols + k, (4 * (i % 4) + g) * cols + (k if i < 4 else other_half(k))) for i in span for k in span
        ]
        parts.append(lax.ppermute(blocked[g * quarter : (g + 1) * quarter, :BLOCK], ("prow", "pcol"), pairs))
    part = (parts[0] + parts[1]) + (parts[2] + parts[3])
    strip = lax.all_to_all(jnp.broadcast_to(part, (rows, quarter, BLOCK)), "prow", 0, 0)
    window = lax.all_gather(strip.reshape(HALF, BLOCK), "pcol", axis=0)

    lower = lax.ppermute(blocked[HALF:, :BLOCK], "pcol", [(k, other_half(k)) for k in span])
    payload = jnp.where(col < STEPS, blocked[:HALF, :BLOCK], lower)
    own = blocked[:BLOCK]
    moves = ([(0, 1), (1, 0)], [(0, 3), (1, 2)], [(0, 2), (1, 3)])
    got = [
        lax.ppermute(own, "prow", [(a * SIDE + x, b * SIDE + x) for a, b in move for x in range(SIDE)])
        for move in moves
    ]
    source = row < 2 * SIDE
    pair = jnp.concatenate([jnp.where(source, own, got[1]), jnp.where(source, got[0], got[2])], 0)
    payload, window, _ = lax.optimization_barrier((payload, window, pair))
    panels = lax.all_gather(payload, "pcol", axis=0)
    across = [pair] + [
        lax.ppermute(pair, "prow", [(r // SIDE * SIDE + (r + d) % SIDE, r) for r in range(rows)])
        for d in range(1, SIDE)
    ]

    place = jnp.stack([row, col])
    in_hbm = lambda a: pltpu.with_memory_space_constraint(a, pltpu.HBM)
    x, d = factor(in_hbm(window))
    return update(place, in_hbm(blocked), in_hbm(panels), *apply(place, x, d, across))


def solution(mesh):
    return jax.shard_map(
        per_device,
        mesh=mesh,
        in_specs=(P("prow", "pcol"),),
        out_specs=P("prow", "pcol"),
        check_vma=False,
    )
```

```python
import functools

import jax
import jax.numpy as jnp
from jax import lax
from jax.experimental import pallas as pl
from jax.experimental.pallas import tpu as pltpu
from jax.sharding import PartitionSpec as P

BLOCK = 128
STEPS = 8
WIDTH = STEPS * BLOCK
HALF = WIDTH // 2
SIDE = 4
NB = 32
GROUP = 16
CHUNK = 256


bf16 = jnp.bfloat16
f32 = jnp.float32


def split(x):
    hi = x.astype(bf16)
    return hi, (x - hi.astype(f32)).astype(bf16)


def dot(a, b, dims=((1,), (0,))):
    return lax.dot_general(a, b, (dims, ((), ())), preferred_element_type=f32)


def dot_split(a, b, dims=((1,), (0,))):
    return dot(a[0], b[0], dims) + dot(a[1], b[0], dims) + dot(a[0], b[1], dims)


def dot_split_128(a, b):
    (ah, al), (bh, bl) = a, b
    return dot(jnp.concatenate([ah, al], 1), jnp.concatenate([bh, bh], 0)) + dot(ah, bl)


def other_half(k):
    return 14 - k + 2 * (k % 2)


def spread(row):
    return jnp.broadcast_to(row, (8, row.shape[1]))


def factor_tile(work_ref):
    tiles = NB // 8
    sub = lax.broadcasted_iota(jnp.int32, (8, 128), 0)
    for base in range(0, BLOCK, NB):
        rows = [
            [work_ref[base + 8 * t : base + 8 * t + 8, h * 128 : h * 128 + 128] for h in range(2)]
            for t in range(tiles)
        ]
        scale = [None] * tiles
        for first in range(0, NB, GROUP):
            last = first + GROUP
            cols = {
                (j, t): jnp.broadcast_to(rows[t][0][:, base + j : base + j + 1], (8, 128))
                for j in range(first, last)
                for t in range(j // 8, tiles)
            }
            for k in range(first, last, 2):
                tk, rk = divmod(k, 8)
                a = spread(cols[k, tk][rk : rk + 1])
                b = spread(cols[k, tk][rk + 1 : rk + 2])
                c = spread(cols[k + 1, tk][rk + 1 : rk + 2])
                det = a * c - b * b
                inv, ra = 1.0 / det, 1.0 / a
                ai, bi, ci = a * inv, b * inv, c * inv
                r0, r1 = lax.rsqrt(a), lax.rsqrt(det * ra)
                scale[tk] = r0 if rk == 0 else jnp.where(sub == rk, r0, scale[tk])
                scale[tk] = jnp.where(sub == rk + 1, r1, scale[tk])
                p, q = {}, {}
                for t in range(tk + (rk == 6), tiles):
                    p[t] = ci * cols[k, t] - bi * cols[k + 1, t]
                    q[t] = ai * cols[k + 1, t] - bi * cols[k, t]
                    if t == tk:
                        p[t] = jnp.where(sub > rk + 1, p[t], 0.0)
                        q[t] = jnp.where(sub > rk + 1, q[t], 0.0)
                for j in range(k + 2, last):
                    tj, rj = divmod(j, 8)
                    c0 = spread(cols[k, tj][rj : rj + 1])
                    c1 = spread(cols[k + 1, tj][rj : rj + 1])
                    for t in range(tj, tiles):
                        cols[j, t] = cols[j, t] - (p[t] * c0 + q[t] * c1)
                second = jnp.where(sub == rk + 1, b * ra, 0.0)
                for h in range(2):
                    s0 = spread(rows[tk][h][rk : rk + 1])
                    s1 = spread(rows[tk][h][rk + 1 : rk + 2])
                    rows[tk][h] = rows[tk][h] - second * s0
                    for t in p:
                        rows[t][h] = rows[t][h] - (p[t] * s0 + q[t] * s1)
                yield
        done = jnp.concatenate(
            [jnp.concatenate([rows[t][h] * scale[t] for h in range(2)], 1) for t in range(tiles)], 0
        )
        end = base + NB
        work_ref[base:end, :] = done
        if end < BLOCK:
            lh, ll = split(jnp.transpose(done[:, :128])[end:])
            uh, ul = split(done)
            left = jnp.concatenate([lh, lh, ll], 1)
            right = jnp.concatenate([uh, ul, uh], 0)
            work_ref[end:, :] = work_ref[end:, :] - dot(left, right)


def factor_kernel(
    place_ref, w_ref, mh_out, ml_out, corner_ref,
    x_ref, d_ref, mh_ref, ml_ref, work_ref, inv_ref, left_ref, right_ref, rest_ref, sems, out_sems,
):
    copies = []
    for j in range(STEPS):
        for h, slot in enumerate((j, other_half(j))):
            dst = x_ref.at[h * HALF : (h + 1) * HALF, j * BLOCK : (j + 1) * BLOCK]
            copies.append(pltpu.make_async_copy(w_ref.at[slot], dst, sems.at[slot]))
    for copy in copies:
        copy.start()
    for copy in copies:
        copy.wait()
    r = lax.broadcasted_iota(jnp.int32, (BLOCK, BLOCK), 0)
    c = lax.broadcasted_iota(jnp.int32, (BLOCK, BLOCK), 1)
    inv_ref[...] = jnp.zeros_like(inv_ref)
    work_ref[:, :BLOCK] = x_ref[:BLOCK, :BLOCK]

    def finish_row(k, live, b):
        here, at = pl.ds(pl.multiple_of(k * BLOCK, BLOCK), BLOCK), slice(b * BLOCK, (b + 1) * BLOCK)
        old, inverse = x_ref[here, at], inv_ref[...]
        new = jnp.where(k == b, inverse, dot_split_128(split(inverse), split(old)))
        new = jnp.where(live, new, old)
        x_ref[here, at] = new
        hi, lo = split(new)
        right_ref[:BLOCK, at], rest_ref[:, at] = hi, lo
        mh_ref[here, at] = jnp.where(b <= k, hi, jnp.zeros_like(hi))
        ml_ref[here, at] = jnp.where(b <= k, lo, jnp.zeros_like(lo))
        right_ref[BLOCK:, at] = hi
        left_ref[at, :BLOCK], left_ref[at, BLOCK:] = split(jnp.where(live & (b > k), jnp.transpose(new), 0.0))

    def send_row(k):
        here = pl.ds(pl.multiple_of(k * BLOCK, BLOCK), BLOCK)
        return [
            pltpu.make_async_copy(ref.at[here], out.at[here], out_sems.at[part, k])
            for part, (ref, out) in enumerate(((mh_ref, mh_out), (ml_ref, ml_out)))
        ]

    def clear(k, live):
        here = pl.ds(pl.multiple_of(k * BLOCK, BLOCK), BLOCK)
        block = lax.broadcasted_iota(jnp.int32, (WIDTH, BLOCK), 0) // BLOCK
        x_ref[:, here] = jnp.where(live & (block > k), 0.0, x_ref[:, here])

    def trail(m, n):
        at, to = slice(m * BLOCK, (m + 1) * BLOCK), slice(n * 2 * BLOCK, (n + 1) * 2 * BLOCK)
        product = dot(left_ref[at, :], right_ref[:, to]) + dot(left_ref[at, :BLOCK], rest_ref[:, to])
        x_ref[at, to] = x_ref[at, to] - product

    def step(k, _):
        here = pl.ds(pl.multiple_of(k * BLOCK, BLOCK), BLOCK)
        after = pl.ds(pl.multiple_of(jnp.minimum(k + 1, STEPS - 1) * BLOCK, BLOCK), BLOCK)
        work_ref[:, BLOCK:] = jnp.where(r == c, 1.0, 0.0).astype(f32)
        before, live = jnp.maximum(k - 1, 0), k > 0
        others = [functools.partial(finish_row, before, live, b) for b in range(STEPS)]
        others += [functools.partial(clear, before, live)]
        others += [functools.partial(trail, m, n) for n in range(STEPS // 2) for m in range(STEPS)]
        places = BLOCK // 2
        emitted = 0
        for place, _ in enumerate(factor_tile(work_ref)):
            until = -(-len(others) * (place + 1) // places)
            for other in others[emitted:until]:
                other()
            emitted = until

        @pl.when(live)
        def _():
            for copy in send_row(before):
                copy.start()

        d_ref[here, :] = jnp.where(r <= c, work_ref[:, :BLOCK], 0.0)
        inverse = work_ref[:, BLOCK:]
        inv_ref[...] = inverse
        u = dot_split_128(split(inverse), split(x_ref[here, after]))
        work_ref[:, :BLOCK] = x_ref[after, after] - dot_split_128(split(jnp.transpose(u)), split(u))
        return 0

    lax.fori_loop(0, STEPS, step, 0)
    for b in range(STEPS):
        finish_row(STEPS - 1, True, b)
    for copy in send_row(STEPS - 1):
        copy.start()
    row, col = place_ref[0], place_ref[1]
    mine = pl.ds(pl.multiple_of(jnp.minimum(row, STEPS - 1) * BLOCK, BLOCK), BLOCK)
    other = pl.ds(pl.multiple_of(jnp.minimum(col, STEPS - 1) * BLOCK, BLOCK), BLOCK)
    block = jnp.where(row == col, d_ref[mine, :], x_ref[other, mine])
    corner_ref[...] = jnp.where(row >= col, jnp.transpose(block), 0.0)
    for k in range(STEPS):
        for copy in send_row(k):
            copy.wait()


def factor(place, gathered):
    square = lambda dtype: pltpu.VMEM((WIDTH, WIDTH), dtype)
    hbm = pl.BlockSpec(memory_space=pltpu.HBM)
    return pl.pallas_call(
        factor_kernel,
        in_specs=[pl.BlockSpec(memory_space=pltpu.SMEM), hbm],
        out_specs=(hbm, hbm, pl.BlockSpec(memory_space=pltpu.VMEM)),
        out_shape=(
            pltpu.HBM((WIDTH, WIDTH), bf16),
            pltpu.HBM((WIDTH, WIDTH), bf16),
            jax.ShapeDtypeStruct((BLOCK, BLOCK), f32),
        ),
        scratch_shapes=[
            square(f32),
            pltpu.VMEM((WIDTH, BLOCK), f32),
            square(bf16),
            square(bf16),
            pltpu.VMEM((BLOCK, 2 * BLOCK), f32),
            pltpu.VMEM((BLOCK, BLOCK), f32),
            pltpu.VMEM((WIDTH, 2 * BLOCK), bf16),
            pltpu.VMEM((2 * BLOCK, WIDTH), bf16),
            pltpu.VMEM((BLOCK, WIDTH), bf16),
            pltpu.SemaphoreType.DMA((2 * STEPS,)),
            pltpu.SemaphoreType.DMA((2, STEPS)),
        ],
        compiler_params=pltpu.CompilerParams(vmem_limit_bytes=24 * 2**20),
        cost_estimate=pl.CostEstimate(flops=40_000_000_000, bytes_accessed=2**23, transcendentals=0),
        name="factor",
    )(place, gathered)


def update_kernel(place_ref, a_ref, u_ref, corner_ref, mh_hbm, ml_hbm, *refs):
    v_hbm, (out_ref, mh, ml, vh, vl, v_ref, sems) = refs[:SIDE], refs[SIDE:]
    row, col, step = place_ref[0], place_ref[1], pl.program_id(0)
    other = pl.ds(pl.multiple_of(jnp.minimum(col, STEPS - 1) * BLOCK, BLOCK), BLOCK)

    @pl.when(step == 0)
    def _():
        pairs = [(v, v_ref.at[d]) for d, v in enumerate(v_hbm)] + [(mh_hbm, mh), (ml_hbm, ml)]
        copies = [pltpu.make_async_copy(src, dst, sems.at[n]) for n, (src, dst) in enumerate(pairs)]
        for copy in copies:
            copy.start()
        my_y, my_x = row // SIDE, row % SIDE
        swapped = jnp.where((my_y == 1) | (my_y == 2), 1, 0)
        for d in range(SIDE):
            copies[d].wait()
            for e in range(2):
                block = SIDE * (e + swapped - 2 * e * swapped) + (my_x + d) % SIDE
                at = pl.ds(pl.multiple_of(block * BLOCK, BLOCK), BLOCK)
                vh[at], vl[at] = split(v_ref[d, e * BLOCK : (e + 1) * BLOCK])
        for copy in copies[SIDE:]:
            copy.wait()
        for k in reversed(range(0, WIDTH, CHUNK)):
            at, upto = slice(k, k + CHUNK), slice(0, k + CHUNK)
            vh[at], vl[at] = split(dot_split((mh[at, upto], ml[at, upto]), (vh[upto], vl[upto])))
        for k in range(0, WIDTH, CHUNK):
            at, on = slice(k, k + CHUNK), slice(k, WIDTH)
            vh[at], vl[at] = split(dot_split((mh[on, at], ml[on, at]), (vh[on], vl[on]), ((0,), (0,))))

    slots = [jnp.where(step < HALF // CHUNK, j, other_half(j) - STEPS) for j in range(STEPS)]
    u = split(jnp.concatenate([u_ref[s] for s in slots], 1))
    out_ref[...] = a_ref[...] - dot_split(u, (vh[...], vl[...]))

    @pl.when(col < STEPS)
    def _():
        out_ref[:, :BLOCK] = dot_split(u, (mh[other, :], ml[other, :]), ((1,), (1,)))

    @pl.when((step == 0) & (row < STEPS))
    def _():
        out_ref[:BLOCK, :] = jnp.zeros((BLOCK, WIDTH), f32)

        @pl.when(col < STEPS)
        def _():
            out_ref[:BLOCK, :BLOCK] = corner_ref[...]


def update(place, blocked, gathered, corner, mh, ml, across):
    per_half = HALF // CHUNK
    square = pltpu.VMEM((WIDTH, WIDTH), bf16)
    return pl.pallas_call(
        update_kernel,
        grid=(WIDTH // CHUNK,),
        in_specs=[
            pl.BlockSpec(memory_space=pltpu.SMEM),
            pl.BlockSpec((CHUNK, WIDTH), lambda i: (i, 0)),
            pl.BlockSpec((STEPS, CHUNK, BLOCK), lambda i: (i // per_half, i % per_half, 0)),
            pl.BlockSpec((BLOCK, BLOCK), lambda i: (0, 0)),
        ]
        + [pl.BlockSpec(memory_space=pltpu.HBM)] * (2 + SIDE),
        out_specs=pl.BlockSpec((CHUNK, WIDTH), lambda i: (i, 0)),
        out_shape=jax.ShapeDtypeStruct((WIDTH, WIDTH), f32),
        scratch_shapes=[square] * 4
        + [pltpu.VMEM((SIDE, 2 * BLOCK, WIDTH), f32), pltpu.SemaphoreType.DMA((SIDE + 2,))],
        compiler_params=pltpu.CompilerParams(vmem_limit_bytes=32 * 2**20),
        name="update",
    )(place, blocked, gathered, corner, mh, ml, *across)


def per_device(blocked):
    rows, cols = lax.axis_size("prow"), lax.axis_size("pcol")
    row, col = lax.axis_index("prow"), lax.axis_index("pcol")
    span = range(STEPS)

    quarter = BLOCK // 4
    parts = []
    for g in range(4):
        pairs = [
            (i * cols + k, (4 * (i % 4) + g) * cols + (k if i < 4 else other_half(k))) for i in span for k in span
        ]
        parts.append(lax.ppermute(blocked[g * quarter : (g + 1) * quarter, :BLOCK], ("prow", "pcol"), pairs))
    part = (parts[0] + parts[1]) + (parts[2] + parts[3])
    strip = lax.all_to_all(jnp.broadcast_to(part, (rows, quarter, BLOCK)), "prow", 0, 0)
    window = lax.all_gather(strip.reshape(HALF, BLOCK), "pcol", axis=0)

    lower = lax.ppermute(blocked[HALF:, :BLOCK], "pcol", [(k, other_half(k)) for k in span])
    payload = jnp.where(col < STEPS, blocked[:HALF, :BLOCK], lower)
    own = blocked[:BLOCK]
    moves = ([(0, 1), (1, 0)], [(0, 3), (1, 2)], [(0, 2), (1, 3)])
    got = [
        lax.ppermute(own, "prow", [(a * SIDE + x, b * SIDE + x) for a, b in move for x in range(SIDE)])
        for move in moves
    ]
    source = row < 2 * SIDE
    pair = jnp.concatenate([jnp.where(source, own, got[1]), jnp.where(source, got[0], got[2])], 0)
    payload, window, _ = lax.optimization_barrier((payload, window, pair))
    panels = lax.all_gather(payload, "pcol", axis=0)
    across = [pair] + [
        lax.ppermute(pair, "prow", [(r // SIDE * SIDE + (r + d) % SIDE, r) for r in range(rows)])
        for d in range(1, SIDE)
    ]

    place = jnp.stack([row, col])
    in_hbm = lambda a: pltpu.with_memory_space_constraint(a, pltpu.HBM)
    mh, ml, corner, *across = (in_hbm(v) for v in (*factor(place, in_hbm(window)), *across))
    return update(place, in_hbm(blocked), in_hbm(panels), corner, mh, ml, across)


def solution(mesh):
    return jax.shard_map(
        per_device,
        mesh=mesh,
        in_specs=(P("prow", "pcol"),),
        out_specs=P("prow", "pcol"),
        check_vma=False,
    )
```

```python
import functools

import jax
import jax.numpy as jnp
from jax import lax
from jax.experimental import pallas as pl
from jax.experimental.pallas import tpu as pltpu
from jax.sharding import PartitionSpec as P


BLOCK = 128
STEPS = 8
WIDTH = STEPS * BLOCK
HALF = WIDTH // 2
SIDE = 4
NB = 32
GROUP = 16
CHUNK = 256


bf16 = jnp.bfloat16
f32 = jnp.float32


def split(x):
    hi = x.astype(bf16)
    return hi, (x - hi.astype(f32)).astype(bf16)


def dot(a, b, dims=((1,), (0,))):
    return lax.dot_general(a, b, (dims, ((), ())), preferred_element_type=f32)


def dot_split(a, b, dims=((1,), (0,))):
    return dot(a[0], b[0], dims) + dot(a[1], b[0], dims) + dot(a[0], b[1], dims)


def dot_split_128(a, b):
    (ah, al), (bh, bl) = a, b
    return dot(jnp.concatenate([ah, al], 1), jnp.concatenate([bh, bh], 0)) + dot(ah, bl)


def other_half(k):
    return 14 - k + 2 * (k % 2)


def spread(row):
    return jnp.broadcast_to(row, (8, row.shape[1]))


def factor_tile(work_ref):
    tiles = NB // 8
    sub = lax.broadcasted_iota(jnp.int32, (8, 128), 0)
    for base in range(0, BLOCK, NB):
        rows = [
            [work_ref[base + 8 * t : base + 8 * t + 8, h * 128 : h * 128 + 128] for h in range(2)]
            for t in range(tiles)
        ]
        scale = [None] * tiles
        for first in range(0, NB, GROUP):
            last = first + GROUP
            cols = {
                (j, t): jnp.broadcast_to(rows[t][0][:, base + j : base + j + 1], (8, 128))
                for j in range(first, last)
                for t in range(j // 8, tiles)
            }
            for k in range(first, last, 2):
                tk, rk = divmod(k, 8)
                a = spread(cols[k, tk][rk : rk + 1])
                b = spread(cols[k, tk][rk + 1 : rk + 2])
                c = spread(cols[k + 1, tk][rk + 1 : rk + 2])
                det = a * c - b * b
                inv, ra = 1.0 / det, 1.0 / a
                ai, bi, ci = a * inv, b * inv, c * inv
                r0, r1 = lax.rsqrt(a), lax.rsqrt(det * ra)
                scale[tk] = r0 if rk == 0 else jnp.where(sub == rk, r0, scale[tk])
                scale[tk] = jnp.where(sub == rk + 1, r1, scale[tk])
                p, q = {}, {}
                for t in range(tk + (rk == 6), tiles):
                    p[t] = ci * cols[k, t] - bi * cols[k + 1, t]
                    q[t] = ai * cols[k + 1, t] - bi * cols[k, t]
                    if t == tk:
                        p[t] = jnp.where(sub > rk + 1, p[t], 0.0)
                        q[t] = jnp.where(sub > rk + 1, q[t], 0.0)
                for j in range(k + 2, last):
                    tj, rj = divmod(j, 8)
                    c0 = spread(cols[k, tj][rj : rj + 1])
                    c1 = spread(cols[k + 1, tj][rj : rj + 1])
                    for t in range(tj, tiles):
                        cols[j, t] = cols[j, t] - (p[t] * c0 + q[t] * c1)
                second = jnp.where(sub == rk + 1, b * ra, 0.0)
                for h in range(2):
                    s0 = spread(rows[tk][h][rk : rk + 1])
                    s1 = spread(rows[tk][h][rk + 1 : rk + 2])
                    rows[tk][h] = rows[tk][h] - second * s0
                    for t in p:
                        rows[t][h] = rows[t][h] - (p[t] * s0 + q[t] * s1)
                yield
        done = jnp.concatenate(
            [jnp.concatenate([rows[t][h] * scale[t] for h in range(2)], 1) for t in range(tiles)], 0
        )
        end = base + NB
        work_ref[base:end, :] = done
        if end < BLOCK:
            lh, ll = split(jnp.transpose(done[:, :128])[end:])
            uh, ul = split(done)
            left = jnp.concatenate([lh, lh, ll], 1)
            right = jnp.concatenate([uh, ul, uh], 0)
            work_ref[end:, :] = work_ref[end:, :] - dot(left, right)


def factor_kernel(
    place_ref, w_ref, mh_out, ml_out, corner_ref,
    x_ref, d_ref, mh_ref, ml_ref, work_ref, inv_ref, left_ref, right_ref, rest_ref, sems, out_sems,
):
    copies = []
    for j in range(STEPS):
        for h, slot in enumerate((j, other_half(j))):
            dst = x_ref.at[h * HALF : (h + 1) * HALF, j * BLOCK : (j + 1) * BLOCK]
            copies.append(pltpu.make_async_copy(w_ref.at[slot], dst, sems.at[slot]))
    for copy in copies:
        copy.start()
    for copy in copies:
        copy.wait()
    r = lax.broadcasted_iota(jnp.int32, (BLOCK, BLOCK), 0)
    c = lax.broadcasted_iota(jnp.int32, (BLOCK, BLOCK), 1)
    inv_ref[...] = jnp.zeros_like(inv_ref)
    work_ref[:, :BLOCK] = x_ref[:BLOCK, :BLOCK]

    def finish_row(k, live, b):
        here, at = pl.ds(pl.multiple_of(k * BLOCK, BLOCK), BLOCK), slice(b * BLOCK, (b + 1) * BLOCK)
        old, inverse = x_ref[here, at], inv_ref[...]
        new = jnp.where(k == b, inverse, dot_split_128(split(inverse), split(old)))
        new = jnp.where(live, new, old)
        x_ref[here, at] = new
        hi, lo = split(new)
        right_ref[:BLOCK, at], rest_ref[:, at] = hi, lo
        mh_ref[here, at] = jnp.where(b <= k, hi, jnp.zeros_like(hi))
        ml_ref[here, at] = jnp.where(b <= k, lo, jnp.zeros_like(lo))
        right_ref[BLOCK:, at] = hi
        left_ref[at, :BLOCK], left_ref[at, BLOCK:] = split(jnp.where(live & (b > k), jnp.transpose(new), 0.0))

    def send_row(k):
        here = pl.ds(pl.multiple_of(k * BLOCK, BLOCK), BLOCK)
        return [
            pltpu.make_async_copy(ref.at[here], out.at[here], out_sems.at[part, k])
            for part, (ref, out) in enumerate(((mh_ref, mh_out), (ml_ref, ml_out)))
        ]

    def clear(k, live):
        here = pl.ds(pl.multiple_of(k * BLOCK, BLOCK), BLOCK)
        block = lax.broadcasted_iota(jnp.int32, (WIDTH, BLOCK), 0) // BLOCK
        x_ref[:, here] = jnp.where(live & (block > k), 0.0, x_ref[:, here])

    def trail(m, n):
        at, to = slice(m * BLOCK, (m + 1) * BLOCK), slice(n * 2 * BLOCK, (n + 1) * 2 * BLOCK)
        product = dot(left_ref[at, :], right_ref[:, to]) + dot(left_ref[at, :BLOCK], rest_ref[:, to])
        x_ref[at, to] = x_ref[at, to] - product

    def step(k, _):
        here = pl.ds(pl.multiple_of(k * BLOCK, BLOCK), BLOCK)
        after = pl.ds(pl.multiple_of(jnp.minimum(k + 1, STEPS - 1) * BLOCK, BLOCK), BLOCK)
        work_ref[:, BLOCK:] = jnp.where(r == c, 1.0, 0.0).astype(f32)
        before, live = jnp.maximum(k - 1, 0), k > 0
        others = [functools.partial(finish_row, before, live, b) for b in range(STEPS)]
        others += [functools.partial(clear, before, live)]
        others += [functools.partial(trail, m, n) for n in range(STEPS // 2) for m in range(STEPS)]
        places = BLOCK // 2
        emitted = 0
        for place, _ in enumerate(factor_tile(work_ref)):
            until = -(-len(others) * (place + 1) // places)
            for other in others[emitted:until]:
                other()
            emitted = until

        @pl.when(live)
        def _():
            for copy in send_row(before):
                copy.start()

        d_ref[here, :] = jnp.where(r <= c, work_ref[:, :BLOCK], 0.0)
        inverse = work_ref[:, BLOCK:]
        inv_ref[...] = inverse
        u = dot_split_128(split(inverse), split(x_ref[here, after]))
        work_ref[:, :BLOCK] = x_ref[after, after] - dot_split_128(split(jnp.transpose(u)), split(u))
        return 0

    lax.fori_loop(0, STEPS, step, 0)
    end = slice(WIDTH - BLOCK, WIDTH)
    x_ref[end, :] = dot_split_128(split(inv_ref[...]), split(x_ref[end, :]))
    x_ref[end, end] = inv_ref[...]
    mh_ref[end, :], ml_ref[end, :] = split(x_ref[end, :])
    for copy in send_row(STEPS - 1):
        copy.start()
    row, col = place_ref[0], place_ref[1]
    mine = pl.ds(pl.multiple_of(jnp.minimum(row, STEPS - 1) * BLOCK, BLOCK), BLOCK)
    other = pl.ds(pl.multiple_of(jnp.minimum(col, STEPS - 1) * BLOCK, BLOCK), BLOCK)
    block = jnp.where(row == col, d_ref[mine, :], x_ref[other, mine])
    corner_ref[...] = jnp.where(row >= col, jnp.transpose(block), 0.0)
    for k in range(STEPS):
        for copy in send_row(k):
            copy.wait()


def factor(place, gathered):
    square = lambda dtype: pltpu.VMEM((WIDTH, WIDTH), dtype)
    hbm = pl.BlockSpec(memory_space=pltpu.HBM)
    return pl.pallas_call(
        factor_kernel,
        in_specs=[pl.BlockSpec(memory_space=pltpu.SMEM), hbm],
        out_specs=(hbm, hbm, pl.BlockSpec(memory_space=pltpu.VMEM)),
        out_shape=(
            pltpu.HBM((WIDTH, WIDTH), bf16),
            pltpu.HBM((WIDTH, WIDTH), bf16),
            jax.ShapeDtypeStruct((BLOCK, BLOCK), f32),
        ),
        scratch_shapes=[
            square(f32),
            pltpu.VMEM((WIDTH, BLOCK), f32),
            square(bf16),
            square(bf16),
            pltpu.VMEM((BLOCK, 2 * BLOCK), f32),
            pltpu.VMEM((BLOCK, BLOCK), f32),
            pltpu.VMEM((WIDTH, 2 * BLOCK), bf16),
            pltpu.VMEM((2 * BLOCK, WIDTH), bf16),
            pltpu.VMEM((BLOCK, WIDTH), bf16),
            pltpu.SemaphoreType.DMA((2 * STEPS,)),
            pltpu.SemaphoreType.DMA((2, STEPS)),
        ],
        compiler_params=pltpu.CompilerParams(vmem_limit_bytes=24 * 2**20),
        cost_estimate=pl.CostEstimate(flops=40_000_000_000, bytes_accessed=2**23, transcendentals=0),
        name="factor",
    )(place, gathered)


def apply_kernel(place_ref, mh_hbm, ml_hbm, *refs):
    v_hbm, (ch_hbm, cl_hbm, mh, ml, vh, vl, ch, cl, v_ref, sems) = refs[:SIDE], refs[SIDE:]
    pairs = [(v, v_ref.at[d]) for d, v in enumerate(v_hbm)] + [(mh_hbm, mh), (ml_hbm, ml)]
    copies = [pltpu.make_async_copy(src, dst, sems.at[n]) for n, (src, dst) in enumerate(pairs)]
    for copy in copies:
        copy.start()
    row = place_ref[0]
    my_y, my_x = row // SIDE, row % SIDE
    swapped = jnp.where((my_y == 1) | (my_y == 2), 1, 0)
    for d in range(SIDE):
        copies[d].wait()
        for e in range(2):
            block = SIDE * (e + swapped - 2 * e * swapped) + (my_x + d) % SIDE
            at = pl.ds(pl.multiple_of(block * BLOCK, BLOCK), BLOCK)
            vh[at], vl[at] = split(v_ref[d, e * BLOCK : (e + 1) * BLOCK])
    for copy in copies[SIDE:]:
        copy.wait()
    sent = []
    for n, k in enumerate(range(0, WIDTH, CHUNK)):
        at, upto = slice(k, k + CHUNK), slice(0, k + CHUNK)
        ch[at], cl[at] = split(dot_split((mh[at, upto], ml[at, upto]), (vh[upto], vl[upto])))
        for m, (src, dst) in enumerate(((ch, ch_hbm), (cl, cl_hbm))):
            sent.append(pltpu.make_async_copy(src.at[at], dst.at[at], sems.at[SIDE + 2 + 2 * n + m]))
            sent[-1].start()
    for copy in sent:
        copy.wait()


def apply(place, mh, ml, across):
    hbm = pl.BlockSpec(memory_space=pltpu.HBM)
    square = pltpu.VMEM((WIDTH, WIDTH), bf16)
    return pl.pallas_call(
        apply_kernel,
        in_specs=[pl.BlockSpec(memory_space=pltpu.SMEM)] + [hbm] * (2 + SIDE),
        out_specs=(hbm, hbm),
        out_shape=(pltpu.HBM((WIDTH, WIDTH), bf16), pltpu.HBM((WIDTH, WIDTH), bf16)),
        scratch_shapes=[square] * 6
        + [
            pltpu.VMEM((SIDE, 2 * BLOCK, WIDTH), f32),
            pltpu.SemaphoreType.DMA((SIDE + 2 + 2 * (WIDTH // CHUNK),)),
        ],
        compiler_params=pltpu.CompilerParams(vmem_limit_bytes=28 * 2**20),
        cost_estimate=pl.CostEstimate(flops=6_000_000_000, bytes_accessed=2**23, transcendentals=0),
        name="apply",
    )(place, mh, ml, *across)


def update_kernel(place_ref, a_ref, u_ref, corner_ref, mh_hbm, ml_hbm, ch_hbm, cl_hbm, out_ref, mh, ml, ch, cl, r_ref, sems):
    row, col, step = place_ref[0], place_ref[1], pl.program_id(0)
    pairs = ((mh_hbm, mh), (ml_hbm, ml), (ch_hbm, ch), (cl_hbm, cl))
    copies = [pltpu.make_async_copy(src, dst, sems.at[n]) for n, (src, dst) in enumerate(pairs)]

    @pl.when(step == 0)
    def _():
        for copy in copies:
            copy.start()
        for copy in copies[:2]:
            copy.wait()

    slots = [jnp.where(step < HALF // CHUNK, j, other_half(j) - STEPS) for j in range(STEPS)]
    uh, ul = split(jnp.concatenate([u_ref[s] for s in slots], 1))
    for k in range(0, WIDTH, CHUNK):
        at, upto = slice(k, k + CHUNK), slice(0, k + CHUNK)
        r_ref[:, at] = dot_split((uh[:, upto], ul[:, upto]), (mh[at, upto], ml[at, upto]), ((1,), (1,)))

    @pl.when(step == 0)
    def _():
        for copy in copies[2:]:
            copy.wait()

    out_ref[...] = a_ref[...] - dot_split(split(r_ref[...]), (ch[...], cl[...]))

    @pl.when(col < STEPS)
    def _():
        out_ref[:, :BLOCK] = r_ref[:, pl.ds(pl.multiple_of(col * BLOCK, BLOCK), BLOCK)]

    @pl.when((step == 0) & (row < STEPS))
    def _():
        out_ref[:BLOCK, :] = jnp.zeros((BLOCK, WIDTH), f32)

        @pl.when(col < STEPS)
        def _():
            out_ref[:BLOCK, :BLOCK] = corner_ref[...]


def update(place, blocked, gathered, corner, mh, ml, ch, cl):
    per_half = HALF // CHUNK
    square = pltpu.VMEM((WIDTH, WIDTH), bf16)
    return pl.pallas_call(
        update_kernel,
        grid=(WIDTH // CHUNK,),
        in_specs=[
            pl.BlockSpec(memory_space=pltpu.SMEM),
            pl.BlockSpec((CHUNK, WIDTH), lambda i: (i, 0)),
            pl.BlockSpec((STEPS, CHUNK, BLOCK), lambda i: (i // per_half, i % per_half, 0)),
            pl.BlockSpec((BLOCK, BLOCK), lambda i: (0, 0)),
        ]
        + [pl.BlockSpec(memory_space=pltpu.HBM)] * 4,
        out_specs=pl.BlockSpec((CHUNK, WIDTH), lambda i: (i, 0)),
        out_shape=jax.ShapeDtypeStruct((WIDTH, WIDTH), f32),
        scratch_shapes=[square] * 4 + [pltpu.VMEM((CHUNK, WIDTH), f32), pltpu.SemaphoreType.DMA((4,))],
        compiler_params=pltpu.CompilerParams(vmem_limit_bytes=32 * 2**20),
        name="update",
    )(place, blocked, gathered, corner, mh, ml, ch, cl)


def per_device(blocked):
    rows, cols = lax.axis_size("prow"), lax.axis_size("pcol")
    row, col = lax.axis_index("prow"), lax.axis_index("pcol")
    span = range(STEPS)
    in_hbm = lambda a: pltpu.with_memory_space_constraint(a, pltpu.HBM)

    quarter = BLOCK // 4
    parts = []
    for g in range(4):
        pairs = [
            (i * cols + k, (4 * (i % 4) + g) * cols + (k if i < 4 else other_half(k))) for i in span for k in span
        ]
        parts.append(lax.ppermute(blocked[g * quarter : (g + 1) * quarter, :BLOCK], ("prow", "pcol"), pairs))
    part = (parts[0] + parts[1]) + (parts[2] + parts[3])
    lower = lax.ppermute(blocked[HALF:, :BLOCK], "pcol", [(k, other_half(k)) for k in span])
    strip = lax.all_to_all(jnp.broadcast_to(part, (rows, quarter, BLOCK)), "prow", 0, 0)
    window = lax.all_gather(strip.reshape(HALF, BLOCK), "pcol", axis=0)
    payload = jnp.where(col < STEPS, blocked[:HALF, :BLOCK], lower)

    own = blocked[:BLOCK]
    moves = ([(0, 1), (1, 0)], [(0, 3), (1, 2)], [(0, 2), (1, 3)])
    got = [
        lax.ppermute(own, "prow", [(a * SIDE + x, b * SIDE + x) for a, b in move for x in range(SIDE)])
        for move in moves
    ]
    source = row < 2 * SIDE
    pair = jnp.concatenate([jnp.where(source, own, got[1]), jnp.where(source, got[0], got[2])], 0)
    payload, window, _ = lax.optimization_barrier((payload, window, pair))
    panels = lax.all_gather(payload, "pcol", axis=0)
    across = [pair]
    for d in range(1, SIDE):
        across.append(lax.ppermute(pair, "prow", [(r // SIDE * SIDE + (r + d) % SIDE, r) for r in range(rows)]))

    place = jnp.stack([row, col])
    mh, ml, corner, *across = (in_hbm(v) for v in (*factor(place, in_hbm(window)), *across))
    ch, cl = (in_hbm(v) for v in apply(place, mh, ml, across))
    return update(place, in_hbm(blocked), in_hbm(panels), corner, mh, ml, ch, cl)


def solution(mesh):
    return jax.shard_map(
        per_device,
        mesh=mesh,
        in_specs=(P("prow", "pcol"),),
        out_specs=P("prow", "pcol"),
        check_vma=False,
    )
```

```python
import functools

import jax
import jax.numpy as jnp
from jax import lax
from jax.experimental import pallas as pl
from jax.experimental.pallas import tpu as pltpu
from jax.sharding import PartitionSpec as P


BLOCK = 128
STEPS = 8
WIDTH = STEPS * BLOCK
HALF = WIDTH // 2
SIDE = 4
NB = 32
GROUP = 16
CHUNK = 256


bf16 = jnp.bfloat16
f32 = jnp.float32


def split(x):
    hi = x.astype(bf16)
    return hi, (x - hi.astype(f32)).astype(bf16)


def dot(a, b, dims=((1,), (0,))):
    return lax.dot_general(a, b, (dims, ((), ())), preferred_element_type=f32)


def dot_split(a, b, dims=((1,), (0,))):
    return dot(a[0], b[0], dims) + dot(a[1], b[0], dims) + dot(a[0], b[1], dims)


def dot_split_128(a, b):
    (ah, al), (bh, bl) = a, b
    return dot(jnp.concatenate([ah, al], 1), jnp.concatenate([bh, bh], 0)) + dot(ah, bl)


def other_half(k):
    return 14 - k + 2 * (k % 2)


def spread(row):
    return jnp.broadcast_to(row, (8, row.shape[1]))


def factor_tile(work_ref):
    tiles = NB // 8
    sub = lax.broadcasted_iota(jnp.int32, (8, 128), 0)
    for base in range(0, BLOCK, NB):
        rows = [
            [work_ref[base + 8 * t : base + 8 * t + 8, h * 128 : h * 128 + 128] for h in range(2)]
            for t in range(tiles)
        ]
        scale = [None] * tiles
        for first in range(0, NB, GROUP):
            last = first + GROUP
            cols = {
                (j, t): jnp.broadcast_to(rows[t][0][:, base + j : base + j + 1], (8, 128))
                for j in range(first, last)
                for t in range(j // 8, tiles)
            }
            for k in range(first, last, 2):
                tk, rk = divmod(k, 8)
                a = spread(cols[k, tk][rk : rk + 1])
                b = spread(cols[k, tk][rk + 1 : rk + 2])
                c = spread(cols[k + 1, tk][rk + 1 : rk + 2])
                det = a * c - b * b
                inv, ra = 1.0 / det, 1.0 / a
                ai, bi, ci = a * inv, b * inv, c * inv
                r0, r1 = lax.rsqrt(a), lax.rsqrt(det * ra)
                scale[tk] = r0 if rk == 0 else jnp.where(sub == rk, r0, scale[tk])
                scale[tk] = jnp.where(sub == rk + 1, r1, scale[tk])
                p, q = {}, {}
                for t in range(tk + (rk == 6), tiles):
                    p[t] = ci * cols[k, t] - bi * cols[k + 1, t]
                    q[t] = ai * cols[k + 1, t] - bi * cols[k, t]
                    if t == tk:
                        p[t] = jnp.where(sub > rk + 1, p[t], 0.0)
                        q[t] = jnp.where(sub > rk + 1, q[t], 0.0)
                for j in range(k + 2, last):
                    tj, rj = divmod(j, 8)
                    c0 = spread(cols[k, tj][rj : rj + 1])
                    c1 = spread(cols[k + 1, tj][rj : rj + 1])
                    for t in range(tj, tiles):
                        cols[j, t] = cols[j, t] - (p[t] * c0 + q[t] * c1)
                second = jnp.where(sub == rk + 1, b * ra, 0.0)
                for h in range(2):
                    s0 = spread(rows[tk][h][rk : rk + 1])
                    s1 = spread(rows[tk][h][rk + 1 : rk + 2])
                    rows[tk][h] = rows[tk][h] - second * s0
                    for t in p:
                        rows[t][h] = rows[t][h] - (p[t] * s0 + q[t] * s1)
                yield
        done = jnp.concatenate(
            [jnp.concatenate([rows[t][h] * scale[t] for h in range(2)], 1) for t in range(tiles)], 0
        )
        end = base + NB
        work_ref[base:end, :] = done
        if end < BLOCK:
            lh, ll = split(jnp.transpose(done[:, :128])[end:])
            uh, ul = split(done)
            left = jnp.concatenate([lh, lh, ll], 1)
            right = jnp.concatenate([uh, ul, uh], 0)
            work_ref[end:, :] = work_ref[end:, :] - dot(left, right)


def factor_kernel(
    place_ref, w_ref, mh_ref, ml_ref, corner_hbm,
    x_ref, d_ref, corner_ref, work_ref, inv_ref, left_ref, right_ref, rest_ref, sems,
):
    copies = []
    for j in range(STEPS):
        for h, slot in enumerate((j, other_half(j))):
            dst = x_ref.at[h * HALF : (h + 1) * HALF, j * BLOCK : (j + 1) * BLOCK]
            copies.append(pltpu.make_async_copy(w_ref.at[slot], dst, sems.at[slot]))
    for copy in copies:
        copy.start()
    for copy in copies:
        copy.wait()
    r = lax.broadcasted_iota(jnp.int32, (BLOCK, BLOCK), 0)
    c = lax.broadcasted_iota(jnp.int32, (BLOCK, BLOCK), 1)
    inv_ref[...] = jnp.zeros_like(inv_ref)
    work_ref[:, :BLOCK] = x_ref[:BLOCK, :BLOCK]

    def finish_row(k, live, b):
        here, at = pl.ds(pl.multiple_of(k * BLOCK, BLOCK), BLOCK), slice(b * BLOCK, (b + 1) * BLOCK)
        old, inverse = x_ref[here, at], inv_ref[...]
        new = jnp.where(k == b, inverse, dot_split_128(split(inverse), split(old)))
        new = jnp.where(live, new, old)
        x_ref[here, at] = new
        hi, lo = split(new)
        right_ref[:BLOCK, at], rest_ref[:, at] = hi, lo
        mh_ref[here, at] = jnp.where(b <= k, hi, jnp.zeros_like(hi))
        ml_ref[here, at] = jnp.where(b <= k, lo, jnp.zeros_like(lo))
        right_ref[BLOCK:, at] = hi
        left_ref[at, :BLOCK], left_ref[at, BLOCK:] = split(jnp.where(live & (b > k), jnp.transpose(new), 0.0))

    def clear(k, live):
        here = pl.ds(pl.multiple_of(k * BLOCK, BLOCK), BLOCK)
        block = lax.broadcasted_iota(jnp.int32, (WIDTH, BLOCK), 0) // BLOCK
        x_ref[:, here] = jnp.where(live & (block > k), 0.0, x_ref[:, here])

    def trail(m, n):
        at, to = slice(m * BLOCK, (m + 1) * BLOCK), slice(n * 2 * BLOCK, (n + 1) * 2 * BLOCK)
        product = dot(left_ref[at, :], right_ref[:, to]) + dot(left_ref[at, :BLOCK], rest_ref[:, to])
        x_ref[at, to] = x_ref[at, to] - product

    def step(k, _):
        here = pl.ds(pl.multiple_of(k * BLOCK, BLOCK), BLOCK)
        after = pl.ds(pl.multiple_of(jnp.minimum(k + 1, STEPS - 1) * BLOCK, BLOCK), BLOCK)
        work_ref[:, BLOCK:] = jnp.where(r == c, 1.0, 0.0).astype(f32)
        before, live = jnp.maximum(k - 1, 0), k > 0
        others = [functools.partial(finish_row, before, live, b) for b in range(STEPS)]
        others += [functools.partial(clear, before, live)]
        others += [functools.partial(trail, m, n) for n in range(STEPS // 2) for m in range(STEPS)]
        places = BLOCK // 2
        emitted = 0
        for place, _ in enumerate(factor_tile(work_ref)):
            until = -(-len(others) * (place + 1) // places)
            for other in others[emitted:until]:
                other()
            emitted = until

        d_ref[here, :] = jnp.where(r <= c, work_ref[:, :BLOCK], 0.0)
        inverse = work_ref[:, BLOCK:]
        inv_ref[...] = inverse
        u = dot_split_128(split(inverse), split(x_ref[here, after]))
        work_ref[:, :BLOCK] = x_ref[after, after] - dot_split_128(split(jnp.transpose(u)), split(u))
        return 0

    lax.fori_loop(0, STEPS, step, 0)
    end = slice(WIDTH - BLOCK, WIDTH)
    x_ref[end, :] = dot_split_128(split(inv_ref[...]), split(x_ref[end, :]))
    x_ref[end, end] = inv_ref[...]
    mh_ref[end, :], ml_ref[end, :] = split(x_ref[end, :])
    row, col = place_ref[0], place_ref[1]
    mine = pl.ds(pl.multiple_of(jnp.minimum(row, STEPS - 1) * BLOCK, BLOCK), BLOCK)
    other = pl.ds(pl.multiple_of(jnp.minimum(col, STEPS - 1) * BLOCK, BLOCK), BLOCK)
    block = jnp.where(row == col, d_ref[mine, :], x_ref[other, mine])
    corner_ref[...] = jnp.where(row >= col, jnp.transpose(block), 0.0)
    copy = pltpu.make_async_copy(corner_ref, corner_hbm, sems.at[2 * STEPS])
    copy.start()
    copy.wait()


def factor(place, gathered):
    vmem, hbm = pl.BlockSpec(memory_space=pltpu.VMEM), pl.BlockSpec(memory_space=pltpu.HBM)
    return pl.pallas_call(
        factor_kernel,
        in_specs=[pl.BlockSpec(memory_space=pltpu.SMEM), hbm],
        out_specs=(vmem, vmem, hbm),
        out_shape=(
            jax.ShapeDtypeStruct((WIDTH, WIDTH), bf16),
            jax.ShapeDtypeStruct((WIDTH, WIDTH), bf16),
            pltpu.HBM((BLOCK, BLOCK), f32),
        ),
        scratch_shapes=[
            pltpu.VMEM((WIDTH, WIDTH), f32),
            pltpu.VMEM((WIDTH, BLOCK), f32),
            pltpu.VMEM((BLOCK, BLOCK), f32),
            pltpu.VMEM((BLOCK, 2 * BLOCK), f32),
            pltpu.VMEM((BLOCK, BLOCK), f32),
            pltpu.VMEM((WIDTH, 2 * BLOCK), bf16),
            pltpu.VMEM((2 * BLOCK, WIDTH), bf16),
            pltpu.VMEM((BLOCK, WIDTH), bf16),
            pltpu.SemaphoreType.DMA((2 * STEPS + 1,)),
        ],
        compiler_params=pltpu.CompilerParams(vmem_limit_bytes=24 * 2**20),
        cost_estimate=pl.CostEstimate(flops=40_000_000_000, bytes_accessed=2**23, transcendentals=0),
        name="factor",
    )(place, gathered)


def apply_kernel(place_ref, mh, ml, *refs):
    v_hbm, outs, (vh, vl, v_ref, sems) = refs[:SIDE], refs[SIDE : SIDE + 4], refs[SIDE + 4 :]
    count = iter(range(sems.shape[0]))
    copy = lambda src, dst: pltpu.make_async_copy(src, dst, sems.at[next(count)])
    arriving = [copy(v, v_ref.at[d]) for d, v in enumerate(v_hbm)]
    for c in arriving:
        c.start()
    row, col = place_ref[0], place_ref[1]
    other = pl.ds(pl.multiple_of(jnp.minimum(col, STEPS - 1) * BLOCK, BLOCK), BLOCK)
    sent = [copy(m.at[other], out) for m, out in zip((mh, ml), outs[2:])]
    for c in sent:
        c.start()
    my_y, my_x = row // SIDE, row % SIDE
    swapped = jnp.where((my_y == 1) | (my_y == 2), 1, 0)
    for d in range(SIDE):
        arriving[d].wait()
        for e in range(2):
            block = SIDE * (e + swapped - 2 * e * swapped) + (my_x + d) % SIDE
            at = pl.ds(pl.multiple_of(block * BLOCK, BLOCK), BLOCK)
            vh[at], vl[at] = split(v_ref[d, e * BLOCK : (e + 1) * BLOCK])
    for k in reversed(range(0, WIDTH, CHUNK)):
        at, upto = slice(k, k + CHUNK), slice(0, k + CHUNK)
        vh[at], vl[at] = split(dot_split((mh[at, upto], ml[at, upto]), (vh[upto], vl[upto])))
    for k in range(0, WIDTH, CHUNK):
        at, on = slice(k, k + CHUNK), slice(k, WIDTH)
        vh[at], vl[at] = split(dot_split((mh[on, at], ml[on, at]), (vh[on], vl[on]), ((0,), (0,))))
        for v, out in zip((vh, vl), outs):
            sent.append(copy(v.at[at], out.at[at]))
            sent[-1].start()
    for c in sent:
        c.wait()


def apply(place, mh, ml, across):
    vmem, hbm = pl.BlockSpec(memory_space=pltpu.VMEM), pl.BlockSpec(memory_space=pltpu.HBM)
    square = pltpu.VMEM((WIDTH, WIDTH), bf16)
    return pl.pallas_call(
        apply_kernel,
        in_specs=[pl.BlockSpec(memory_space=pltpu.SMEM), vmem, vmem] + [hbm] * SIDE,
        out_specs=(hbm,) * 4,
        out_shape=tuple(pltpu.HBM((rows, WIDTH), bf16) for rows in (WIDTH, WIDTH, BLOCK, BLOCK)),
        scratch_shapes=[square, square]
        + [
            pltpu.VMEM((SIDE, 2 * BLOCK, WIDTH), f32),
            pltpu.SemaphoreType.DMA((SIDE + 2 + 2 * (WIDTH // CHUNK),)),
        ],
        compiler_params=pltpu.CompilerParams(vmem_limit_bytes=20 * 2**20),
        cost_estimate=pl.CostEstimate(flops=10_000_000_000, bytes_accessed=2**23, transcendentals=0),
        name="apply",
    )(place, mh, ml, *across)


def update_kernel(place_ref, a_ref, u_ref, corner_ref, yh_ref, yl_ref, ph_ref, pl_ref, out_ref):
    row, col, step = place_ref[0], place_ref[1], pl.program_id(0)
    slots = [jnp.where(step < HALF // CHUNK, j, other_half(j) - STEPS) for j in range(STEPS)]
    u = split(jnp.concatenate([u_ref[s] for s in slots], 1))
    out_ref[...] = a_ref[...] - dot_split(u, (yh_ref[...], yl_ref[...]))

    @pl.when(col < STEPS)
    def _():
        out_ref[:, :BLOCK] = dot_split(u, (ph_ref[...], pl_ref[...]), ((1,), (1,)))

    @pl.when((step == 0) & (row < STEPS))
    def _():
        out_ref[:BLOCK, :] = jnp.zeros((BLOCK, WIDTH), f32)

        @pl.when(col < STEPS)
        def _():
            out_ref[:BLOCK, :BLOCK] = corner_ref[...]


def update(place, blocked, gathered, corner, yh, yl, ph, pl_):
    per_half = HALF // CHUNK
    whole = lambda *shape: pl.BlockSpec(shape, lambda i: (0, 0))
    return pl.pallas_call(
        update_kernel,
        grid=(WIDTH // CHUNK,),
        in_specs=[
            pl.BlockSpec(memory_space=pltpu.SMEM),
            pl.BlockSpec((CHUNK, WIDTH), lambda i: (i, 0)),
            pl.BlockSpec((STEPS, CHUNK, BLOCK), lambda i: (i // per_half, i % per_half, 0)),
            whole(BLOCK, BLOCK),
            whole(WIDTH, WIDTH),
            whole(WIDTH, WIDTH),
            whole(BLOCK, WIDTH),
            whole(BLOCK, WIDTH),
        ],
        out_specs=pl.BlockSpec((CHUNK, WIDTH), lambda i: (i, 0)),
        out_shape=jax.ShapeDtypeStruct((WIDTH, WIDTH), f32),
        compiler_params=pltpu.CompilerParams(vmem_limit_bytes=28 * 2**20),
        name="update",
    )(place, blocked, gathered, corner, yh, yl, ph, pl_)


def per_device(blocked):
    rows, cols = lax.axis_size("prow"), lax.axis_size("pcol")
    row, col = lax.axis_index("prow"), lax.axis_index("pcol")
    span = range(STEPS)
    in_hbm = lambda a: pltpu.with_memory_space_constraint(a, pltpu.HBM)

    quarter = BLOCK // 4
    parts = []
    for g in range(4):
        pairs = [
            (i * cols + k, (4 * (i % 4) + g) * cols + (k if i < 4 else other_half(k))) for i in span for k in span
        ]
        parts.append(lax.ppermute(blocked[g * quarter : (g + 1) * quarter, :BLOCK], ("prow", "pcol"), pairs))
    part = (parts[0] + parts[1]) + (parts[2] + parts[3])
    lower = lax.ppermute(blocked[HALF:, :BLOCK], "pcol", [(k, other_half(k)) for k in span])
    strip = lax.all_to_all(jnp.broadcast_to(part, (rows, quarter, BLOCK)), "prow", 0, 0)
    window = lax.all_gather(strip.reshape(HALF, BLOCK), "pcol", axis=0)
    payload = jnp.where(col < STEPS, blocked[:HALF, :BLOCK], lower)

    own = blocked[:BLOCK]
    moves = ([(0, 1), (1, 0)], [(0, 3), (1, 2)], [(0, 2), (1, 3)])
    got = [
        lax.ppermute(own, "prow", [(a * SIDE + x, b * SIDE + x) for a, b in move for x in range(SIDE)])
        for move in moves
    ]
    source = row < 2 * SIDE
    pair = jnp.concatenate([jnp.where(source, own, got[1]), jnp.where(source, got[0], got[2])], 0)
    payload, window, _ = lax.optimization_barrier((payload, window, pair))
    panels = lax.all_gather(payload, "pcol", axis=0)
    across = [pair]
    for d in range(1, SIDE):
        across.append(lax.ppermute(pair, "prow", [(r // SIDE * SIDE + (r + d) % SIDE, r) for r in range(rows)]))

    place = jnp.stack([row, col])
    mh, ml, corner = factor(place, in_hbm(window))
    applied = apply(place, mh, ml, [in_hbm(v) for v in across])
    return update(place, *(in_hbm(v) for v in (blocked, panels, corner, *applied)))


def solution(mesh):
    return jax.shard_map(
        per_device,
        mesh=mesh,
        in_specs=(P("prow", "pcol"),),
        out_specs=P("prow", "pcol"),
        check_vma=False,
    )
```

```python
import functools

import jax
import jax.numpy as jnp
from jax import lax
from jax.experimental import pallas as pl
from jax.experimental.pallas import tpu as pltpu
from jax.sharding import PartitionSpec as P


BLOCK = 128
STEPS = 8
WIDTH = STEPS * BLOCK
HALF = WIDTH // 2
SIDE = 4
NB = 32
GROUP = 16
CHUNK = 256


bf16 = jnp.bfloat16
f32 = jnp.float32


def split(x):
    hi = x.astype(bf16)
    return hi, (x - hi.astype(f32)).astype(bf16)


def dot(a, b, dims=((1,), (0,))):
    return lax.dot_general(a, b, (dims, ((), ())), preferred_element_type=f32)


def dot_split(a, b, dims=((1,), (0,))):
    return dot(a[0], b[0], dims) + dot(a[1], b[0], dims) + dot(a[0], b[1], dims)


def dot_split_128(a, b):
    (ah, al), (bh, bl) = a, b
    return dot(jnp.concatenate([ah, al], 1), jnp.concatenate([bh, bh], 0)) + dot(ah, bl)


def other_half(k):
    return 14 - k + 2 * (k % 2)


def spread(row):
    return jnp.broadcast_to(row, (8, row.shape[1]))


def factor_tile(work_ref):
    tiles = NB // 8
    sub = lax.broadcasted_iota(jnp.int32, (8, 128), 0)
    for base in range(0, BLOCK, NB):
        rows = [
            [work_ref[base + 8 * t : base + 8 * t + 8, h * 128 : h * 128 + 128] for h in range(2)]
            for t in range(tiles)
        ]
        scale = [None] * tiles
        for first in range(0, NB, GROUP):
            last = first + GROUP
            cols = {
                (j, t): jnp.broadcast_to(rows[t][0][:, base + j : base + j + 1], (8, 128))
                for j in range(first, last)
                for t in range(j // 8, tiles)
            }
            for k in range(first, last, 2):
                tk, rk = divmod(k, 8)
                a = spread(cols[k, tk][rk : rk + 1])
                b = spread(cols[k, tk][rk + 1 : rk + 2])
                c = spread(cols[k + 1, tk][rk + 1 : rk + 2])
                det = a * c - b * b
                inv, ra = 1.0 / det, 1.0 / a
                r0, r1 = lax.rsqrt(a), lax.rsqrt(det * ra)
                scale[tk] = r0 if rk == 0 else jnp.where(sub == rk, r0, scale[tk])
                scale[tk] = jnp.where(sub == rk + 1, r1, scale[tk])
                p, q = {}, {}
                for t in range(tk + (rk == 6), tiles):
                    p[t] = c * cols[k, t] - b * cols[k + 1, t]
                    q[t] = a * cols[k + 1, t] - b * cols[k, t]
                pd, qd = {t: v * inv for t, v in p.items()}, {t: v * inv for t, v in q.items()}
                for j in range(k + 2, last):
                    tj, rj = divmod(j, 8)
                    c0 = spread(cols[k, tj][rj : rj + 1])
                    c1 = spread(cols[k + 1, tj][rj : rj + 1])
                    for t in range(tj, tiles):
                        if j < k + 4:
                            cols[j, t] = cols[j, t] - (p[t] * c0 + q[t] * c1) * inv
                        else:
                            cols[j, t] = cols[j, t] - (pd[t] * c0 + qd[t] * c1)
                if tk in pd:
                    pd[tk], qd[tk] = (jnp.where(sub > rk + 1, v[tk], 0.0) for v in (pd, qd))
                second = jnp.where(sub == rk + 1, b * ra, 0.0)
                for h in range(2):
                    s0 = spread(rows[tk][h][rk : rk + 1])
                    s1 = spread(rows[tk][h][rk + 1 : rk + 2])
                    rows[tk][h] = rows[tk][h] - second * s0
                    for t in pd:
                        rows[t][h] = rows[t][h] - (pd[t] * s0 + qd[t] * s1)
                yield
        done = jnp.concatenate(
            [jnp.concatenate([rows[t][h] * scale[t] for h in range(2)], 1) for t in range(tiles)], 0
        )
        end = base + NB
        work_ref[base:end, :] = done
        if end < BLOCK:
            lh, ll = split(jnp.transpose(done[:, :128])[end:])
            uh, ul = split(done)
            left = jnp.concatenate([lh, lh, ll], 1)
            right = jnp.concatenate([uh, ul, uh], 0)
            work_ref[end:, :] = work_ref[end:, :] - dot(left, right)


def factor_kernel(
    place_ref, w_ref, mh_ref, ml_ref, corner_ref,
    x_ref, d_ref, work_ref, inv_ref, left_ref, right_ref, rest_ref, sems,
):
    copies = []
    for j in range(STEPS):
        for h, slot in enumerate((j, other_half(j))):
            dst = x_ref.at[h * HALF : (h + 1) * HALF, j * BLOCK : (j + 1) * BLOCK]
            copies.append(pltpu.make_async_copy(w_ref.at[slot], dst, sems.at[slot]))
    for copy in copies:
        copy.start()
    copies[0].wait()
    r = lax.broadcasted_iota(jnp.int32, (BLOCK, BLOCK), 0)
    c = lax.broadcasted_iota(jnp.int32, (BLOCK, BLOCK), 1)
    work_ref[:, :BLOCK] = x_ref[:BLOCK, :BLOCK]

    def finish_row(k, b):
        here, at = pl.ds(pl.multiple_of(k * BLOCK, BLOCK), BLOCK), slice(b * BLOCK, (b + 1) * BLOCK)
        old, inverse = x_ref[here, at], inv_ref[...]
        new = jnp.where(k == b, inverse, dot_split_128(split(inverse), split(old)))
        x_ref[here, at] = new
        hi, lo = split(new)
        right_ref[:BLOCK, at], rest_ref[:, at] = hi, lo
        mh_ref[here, at] = jnp.where(b <= k, hi, jnp.zeros_like(hi))
        ml_ref[here, at] = jnp.where(b <= k, lo, jnp.zeros_like(lo))
        right_ref[BLOCK:, at] = hi
        left_ref[at, :BLOCK], left_ref[at, BLOCK:] = split(jnp.where(b > k, jnp.transpose(new), 0.0))

    def clear(k):
        here = pl.ds(pl.multiple_of(k * BLOCK, BLOCK), BLOCK)
        block = lax.broadcasted_iota(jnp.int32, (WIDTH, BLOCK), 0) // BLOCK
        x_ref[:, here] = jnp.where(block > k, 0.0, x_ref[:, here])

    def trail(m, n):
        at, to = slice(m * BLOCK, (m + 1) * BLOCK), slice(n * 2 * BLOCK, (n + 1) * 2 * BLOCK)
        product = dot(left_ref[at, :], right_ref[:, to]) + dot(left_ref[at, :BLOCK], rest_ref[:, to])
        x_ref[at, to] = x_ref[at, to] - product

    def factor_block(others):
        work_ref[:, BLOCK:] = jnp.where(r == c, 1.0, 0.0).astype(f32)
        emitted = 0
        for place, _ in enumerate(factor_tile(work_ref)):
            until = -(-len(others) * (place + 1) // (BLOCK // 2))
            for other in others[emitted:until]:
                other()
            emitted = until

    def prepare(k):
        here = pl.ds(pl.multiple_of(k * BLOCK, BLOCK), BLOCK)
        after = pl.ds(pl.multiple_of(jnp.minimum(k + 1, STEPS - 1) * BLOCK, BLOCK), BLOCK)
        d_ref[here, :] = jnp.where(r <= c, work_ref[:, :BLOCK], 0.0)
        inverse = work_ref[:, BLOCK:]
        inv_ref[...] = inverse
        u = dot_split_128(split(inverse), split(x_ref[here, after]))
        work_ref[:, :BLOCK] = x_ref[after, after] - dot_split_128(split(jnp.transpose(u)), split(u))

    def step(k, _):
        others = [functools.partial(finish_row, k - 1, b) for b in range(STEPS)]
        others += [functools.partial(clear, k - 1)]
        others += [functools.partial(trail, m, n) for n in range(STEPS // 2) for m in range(STEPS)]
        factor_block(others)
        prepare(k)
        return 0

    factor_block([])
    for copy in copies[1:]:
        copy.wait()
    prepare(0)
    lax.fori_loop(1, STEPS, step, 0)
    end = slice(WIDTH - BLOCK, WIDTH)
    x_ref[end, :] = dot_split_128(split(inv_ref[...]), split(x_ref[end, :]))
    x_ref[end, end] = inv_ref[...]
    mh_ref[end, :], ml_ref[end, :] = split(x_ref[end, :])
    row, col = place_ref[0], place_ref[1]
    mine = pl.ds(pl.multiple_of(jnp.minimum(row, STEPS - 1) * BLOCK, BLOCK), BLOCK)
    other = pl.ds(pl.multiple_of(jnp.minimum(col, STEPS - 1) * BLOCK, BLOCK), BLOCK)
    block = jnp.where(row == col, d_ref[mine, :], x_ref[other, mine])
    corner_ref[...] = jnp.where(row >= col, jnp.transpose(block), 0.0)


def factor(place, gathered):
    vmem, hbm = pl.BlockSpec(memory_space=pltpu.VMEM), pl.BlockSpec(memory_space=pltpu.HBM)
    return pl.pallas_call(
        factor_kernel,
        in_specs=[pl.BlockSpec(memory_space=pltpu.SMEM), hbm],
        out_specs=(vmem, vmem, vmem),
        out_shape=(
            jax.ShapeDtypeStruct((WIDTH, WIDTH), bf16),
            jax.ShapeDtypeStruct((WIDTH, WIDTH), bf16),
            jax.ShapeDtypeStruct((BLOCK, BLOCK), f32),
        ),
        scratch_shapes=[
            pltpu.VMEM((WIDTH, WIDTH), f32),
            pltpu.VMEM((WIDTH, BLOCK), f32),
            pltpu.VMEM((BLOCK, 2 * BLOCK), f32),
            pltpu.VMEM((BLOCK, BLOCK), f32),
            pltpu.VMEM((WIDTH, 2 * BLOCK), bf16),
            pltpu.VMEM((2 * BLOCK, WIDTH), bf16),
            pltpu.VMEM((BLOCK, WIDTH), bf16),
            pltpu.SemaphoreType.DMA((2 * STEPS,)),
        ],
        compiler_params=pltpu.CompilerParams(vmem_limit_bytes=24 * 2**20),
        cost_estimate=pl.CostEstimate(flops=40_000_000_000, bytes_accessed=2**23, transcendentals=0),
        name="factor",
    )(place, gathered)


def apply_kernel(place_ref, mh, ml, corner_ref, *refs):
    v_hbm, outs, (vh, vl, v_ref, sems) = refs[:SIDE], refs[SIDE : SIDE + 3], refs[SIDE + 3 :]
    count = iter(range(sems.shape[0]))
    copy = lambda src, dst: pltpu.make_async_copy(src, dst, sems.at[next(count)])
    arriving = [copy(v, v_ref.at[d]) for d, v in enumerate(v_hbm)]
    for c in arriving:
        c.start()
    row, col = place_ref[0], place_ref[1]
    other = pl.ds(pl.multiple_of(jnp.minimum(col, STEPS - 1) * BLOCK, BLOCK), BLOCK)
    sent = [copy(corner_ref, outs[2])]
    sent[0].start()
    my_y, my_x = row // SIDE, row % SIDE
    swapped = jnp.where((my_y == 1) | (my_y == 2), 1, 0)
    for d in range(SIDE):
        arriving[d].wait()
        for e in range(2):
            block = SIDE * (e + swapped - 2 * e * swapped) + (my_x + d) % SIDE
            at = pl.ds(pl.multiple_of(block * BLOCK, BLOCK), BLOCK)
            vh[at], vl[at] = split(v_ref[d, e * BLOCK : (e + 1) * BLOCK])
    for k in reversed(range(0, WIDTH, CHUNK)):
        at, upto = slice(k, k + CHUNK), slice(0, k + CHUNK)
        vh[at], vl[at] = split(dot_split((mh[at, upto], ml[at, upto]), (vh[upto], vl[upto])))
    for k in range(0, WIDTH, CHUNK):
        at, on = slice(k, k + CHUNK), slice(k, WIDTH)
        vh[at], vl[at] = split(dot_split((mh[on, at], ml[on, at]), (vh[on], vl[on]), ((0,), (0,))))
        for v, m in ((vh, mh), (vl, ml)):
            panel = jnp.transpose(m[other, at].astype(f32)).astype(bf16)
            v[at, :BLOCK] = jnp.where(col < STEPS, panel, v[at, :BLOCK])
        for v, out in zip((vh, vl), outs):
            sent.append(copy(v.at[at], out.at[at]))
            sent[-1].start()
    for c in sent:
        c.wait()


def apply(place, mh, ml, corner, across):
    vmem, hbm = pl.BlockSpec(memory_space=pltpu.VMEM), pl.BlockSpec(memory_space=pltpu.HBM)
    square = pltpu.VMEM((WIDTH, WIDTH), bf16)
    return pl.pallas_call(
        apply_kernel,
        in_specs=[pl.BlockSpec(memory_space=pltpu.SMEM), vmem, vmem, vmem] + [hbm] * SIDE,
        out_specs=(hbm,) * 3,
        out_shape=(pltpu.HBM((WIDTH, WIDTH), bf16), pltpu.HBM((WIDTH, WIDTH), bf16), pltpu.HBM((BLOCK, BLOCK), f32)),
        scratch_shapes=[square, square]
        + [
            pltpu.VMEM((SIDE, 2 * BLOCK, WIDTH), f32),
            pltpu.SemaphoreType.DMA((SIDE + 1 + 2 * (WIDTH // CHUNK),)),
        ],
        compiler_params=pltpu.CompilerParams(vmem_limit_bytes=20 * 2**20),
        cost_estimate=pl.CostEstimate(flops=10_000_000_000, bytes_accessed=2**23, transcendentals=0),
        name="apply",
    )(place, mh, ml, corner, *across)


def update_kernel(place_ref, a_ref, u_ref, yh_ref, yl_ref, corner_ref, out_ref):
    row, col, step = place_ref[0], place_ref[1], pl.program_id(0)
    slots = [jnp.where(step < HALF // CHUNK, j, other_half(j) - STEPS) for j in range(STEPS)]
    u = split(jnp.concatenate([u_ref[s] for s in slots], 1))
    product = dot_split(u, (yh_ref[...], yl_ref[...]))
    out_ref[:, :BLOCK] = jnp.where(col < STEPS, product[:, :BLOCK], a_ref[:, :BLOCK] - product[:, :BLOCK])
    out_ref[:, BLOCK:] = a_ref[:, BLOCK:] - product[:, BLOCK:]

    @pl.when((step == 0) & (row < STEPS))
    def _():
        out_ref[:BLOCK, :] = jnp.zeros((BLOCK, WIDTH), f32)

        @pl.when(col < STEPS)
        def _():
            out_ref[:BLOCK, :BLOCK] = corner_ref[...]


def update(place, blocked, gathered, yh, yl, corner):
    per_half = HALF // CHUNK
    whole = lambda *shape: pl.BlockSpec(shape, lambda i: (0, 0))
    return pl.pallas_call(
        update_kernel,
        grid=(WIDTH // CHUNK,),
        in_specs=[
            pl.BlockSpec(memory_space=pltpu.SMEM),
            pl.BlockSpec((CHUNK, WIDTH), lambda i: (i, 0)),
            pl.BlockSpec((STEPS, CHUNK, BLOCK), lambda i: (i // per_half, i % per_half, 0)),
            whole(WIDTH, WIDTH),
            whole(WIDTH, WIDTH),
            whole(BLOCK, BLOCK),
        ],
        out_specs=pl.BlockSpec((CHUNK, WIDTH), lambda i: (i, 0)),
        out_shape=jax.ShapeDtypeStruct((WIDTH, WIDTH), f32),
        compiler_params=pltpu.CompilerParams(vmem_limit_bytes=28 * 2**20),
        name="update",
    )(place, blocked, gathered, yh, yl, corner)


def per_device(blocked):
    rows, cols = lax.axis_size("prow"), lax.axis_size("pcol")
    row, col = lax.axis_index("prow"), lax.axis_index("pcol")
    span = range(STEPS)
    in_hbm = lambda a: pltpu.with_memory_space_constraint(a, pltpu.HBM)

    quarter = BLOCK // 4
    parts = []
    for g in range(4):
        pairs = [
            (i * cols + k, (4 * (i % 4) + g) * cols + (k if i < 4 else other_half(k))) for i in span for k in span
        ]
        parts.append(lax.ppermute(blocked[g * quarter : (g + 1) * quarter, :BLOCK], ("prow", "pcol"), pairs))
    part = (parts[0] + parts[1]) + (parts[2] + parts[3])
    lower = lax.ppermute(blocked[HALF:, :BLOCK], "pcol", [(k, other_half(k)) for k in span])
    strip = lax.all_to_all(jnp.broadcast_to(part, (rows, quarter, BLOCK)), "prow", 0, 0)
    window = lax.all_gather(strip.reshape(HALF, BLOCK), "pcol", axis=0)
    payload = jnp.where(col < STEPS, blocked[:HALF, :BLOCK], lower)

    own = blocked[:BLOCK]
    moves = ([(0, 1), (1, 0)], [(0, 3), (1, 2)], [(0, 2), (1, 3)])
    got = [
        lax.ppermute(own, "prow", [(a * SIDE + x, b * SIDE + x) for a, b in move for x in range(SIDE)])
        for move in moves
    ]
    source = row < 2 * SIDE
    pair = jnp.concatenate([jnp.where(source, own, got[1]), jnp.where(source, got[0], got[2])], 0)
    payload, window, _ = lax.optimization_barrier((payload, window, pair))
    panels = lax.all_gather(payload, "pcol", axis=0)
    across = [pair]
    for d in range(1, SIDE):
        across.append(lax.ppermute(pair, "prow", [(r // SIDE * SIDE + (r + d) % SIDE, r) for r in range(rows)]))

    place = jnp.stack([row, col])
    mh, ml, corner = factor(place, in_hbm(window))
    applied = apply(place, mh, ml, corner, [in_hbm(v) for v in across])
    return update(place, *(in_hbm(v) for v in (blocked, panels, *applied)))


def solution(mesh):
    return jax.shard_map(
        per_device,
        mesh=mesh,
        in_specs=(P("prow", "pcol"),),
        out_specs=P("prow", "pcol"),
        check_vma=False,
    )
```

```python
import functools

import jax
import jax.numpy as jnp
from jax import lax
from jax.experimental import pallas as pl
from jax.experimental.pallas import tpu as pltpu
from jax.sharding import PartitionSpec as P


BLOCK = 128
STEPS = 8
WIDTH = STEPS * BLOCK
HALF = WIDTH // 2
SIDE = 4
NB = 32
GROUP = 16
CHUNK = 256


bf16 = jnp.bfloat16
f32 = jnp.float32


def split(x):
    hi = x.astype(bf16)
    return hi, (x - hi.astype(f32)).astype(bf16)


def dot(a, b, dims=((1,), (0,))):
    return lax.dot_general(a, b, (dims, ((), ())), preferred_element_type=f32)


def dot_split(a, b, dims=((1,), (0,))):
    return dot(a[0], b[0], dims) + dot(a[1], b[0], dims) + dot(a[0], b[1], dims)


def dot_split_128(a, b):
    (ah, al), (bh, bl) = a, b
    return dot(jnp.concatenate([ah, al], 1), jnp.concatenate([bh, bh], 0)) + dot(ah, bl)


def other_half(k):
    return 14 - k + 2 * (k % 2)


def window_place(i, k):
    if i < 3:
        return k, i
    if i == 3:
        return (other_half(k), 2) if k < 4 else (other_half(k - 4), 1)
    if k < 4:
        return None
    return (other_half(k - 4), 0) if i == 7 else (other_half(k), i - 4)


def spread(row):
    return jnp.broadcast_to(row, (8, row.shape[1]))


def factor_tile(work_ref):
    tiles = NB // 8
    sub = lax.broadcasted_iota(jnp.int32, (8, 128), 0)
    for base in range(0, BLOCK, NB):
        rows = [
            [work_ref[base + 8 * t : base + 8 * t + 8, h * 128 : h * 128 + 128] for h in range(2)]
            for t in range(tiles)
        ]
        scale = [None] * tiles
        for first in range(0, NB, GROUP):
            last = first + GROUP
            cols = {
                (j, t): jnp.broadcast_to(rows[t][0][:, base + j : base + j + 1], (8, 128))
                for j in range(first, last)
                for t in range(j // 8, tiles)
            }
            for k in range(first, last, 2):
                tk, rk = divmod(k, 8)
                a = spread(cols[k, tk][rk : rk + 1])
                b = spread(cols[k, tk][rk + 1 : rk + 2])
                c = spread(cols[k + 1, tk][rk + 1 : rk + 2])
                det = a * c - b * b
                inv, ra = 1.0 / det, 1.0 / a
                r0, r1 = lax.rsqrt(a), lax.rsqrt(det * ra)
                scale[tk] = r0 if rk == 0 else jnp.where(sub == rk, r0, scale[tk])
                scale[tk] = jnp.where(sub == rk + 1, r1, scale[tk])
                p, q = {}, {}
                for t in range(tk + (rk == 6), tiles):
                    p[t] = c * cols[k, t] - b * cols[k + 1, t]
                    q[t] = a * cols[k + 1, t] - b * cols[k, t]
                pd, qd = {t: v * inv for t, v in p.items()}, {t: v * inv for t, v in q.items()}
                for j in range(k + 2, last):
                    tj, rj = divmod(j, 8)
                    c0 = spread(cols[k, tj][rj : rj + 1])
                    c1 = spread(cols[k + 1, tj][rj : rj + 1])
                    for t in range(tj, tiles):
                        if j < k + 4:
                            cols[j, t] = cols[j, t] - (p[t] * c0 + q[t] * c1) * inv
                        else:
                            cols[j, t] = cols[j, t] - (pd[t] * c0 + qd[t] * c1)
                if tk in pd:
                    pd[tk], qd[tk] = (jnp.where(sub > rk + 1, v[tk], 0.0) for v in (pd, qd))
                second = jnp.where(sub == rk + 1, b * ra, 0.0)
                for h in range(2):
                    s0 = spread(rows[tk][h][rk : rk + 1])
                    s1 = spread(rows[tk][h][rk + 1 : rk + 2])
                    rows[tk][h] = rows[tk][h] - second * s0
                    for t in pd:
                        rows[t][h] = rows[t][h] - (pd[t] * s0 + qd[t] * s1)
                yield
        done = jnp.concatenate(
            [jnp.concatenate([rows[t][h] * scale[t] for h in range(2)], 1) for t in range(tiles)], 0
        )
        end = base + NB
        work_ref[base:end, :] = done
        if end < BLOCK:
            lh, ll = split(jnp.transpose(done[:, :128])[end:])
            uh, ul = split(done)
            left = jnp.concatenate([lh, lh, ll], 1)
            right = jnp.concatenate([uh, ul, uh], 0)
            work_ref[end:, :] = work_ref[end:, :] - dot(left, right)


def factor_kernel(
    place_ref, w_ref, mh_ref, ml_ref, corner_ref,
    x_ref, d_ref, work_ref, inv_ref, left_ref, right_ref, rest_ref, sems,
):
    copies = []
    for i in range(STEPS):
        for k in range(STEPS):
            if window_place(i, k):
                slot, third = window_place(i, k)
                src = w_ref.at[slot, third * BLOCK : (third + 1) * BLOCK]
                dst = x_ref.at[i * BLOCK : (i + 1) * BLOCK, k * BLOCK : (k + 1) * BLOCK]
                copies.append(pltpu.make_async_copy(src, dst, sems.at[len(copies)]))
    for copy in copies:
        copy.start()
    copies[0].wait()
    r = lax.broadcasted_iota(jnp.int32, (BLOCK, BLOCK), 0)
    c = lax.broadcasted_iota(jnp.int32, (BLOCK, BLOCK), 1)
    work_ref[:, :BLOCK] = x_ref[:BLOCK, :BLOCK]

    def finish_row(k, b):
        here, at = pl.ds(pl.multiple_of(k * BLOCK, BLOCK), BLOCK), slice(b * BLOCK, (b + 1) * BLOCK)
        old, inverse = x_ref[here, at], inv_ref[...]
        new = jnp.where(k == b, inverse, dot_split_128(split(inverse), split(old)))
        x_ref[here, at] = new
        hi, lo = split(new)
        right_ref[:BLOCK, at], rest_ref[:, at] = hi, lo
        mh_ref[here, at] = jnp.where(b <= k, hi, jnp.zeros_like(hi))
        ml_ref[here, at] = jnp.where(b <= k, lo, jnp.zeros_like(lo))
        right_ref[BLOCK:, at] = hi
        left_ref[at, :BLOCK], left_ref[at, BLOCK:] = split(jnp.where(b > k, jnp.transpose(new), 0.0))

    def clear(k):
        here = pl.ds(pl.multiple_of(k * BLOCK, BLOCK), BLOCK)
        block = lax.broadcasted_iota(jnp.int32, (WIDTH, BLOCK), 0) // BLOCK
        x_ref[:, here] = jnp.where(block > k, 0.0, x_ref[:, here])

    def trail(m, n):
        at, to = slice(m * BLOCK, (m + 1) * BLOCK), slice(n * 2 * BLOCK, (n + 1) * 2 * BLOCK)
        product = dot(left_ref[at, :], right_ref[:, to]) + dot(left_ref[at, :BLOCK], rest_ref[:, to])
        x_ref[at, to] = x_ref[at, to] - product

    def factor_block(others):
        work_ref[:, BLOCK:] = jnp.where(r == c, 1.0, 0.0).astype(f32)
        emitted = 0
        for place, _ in enumerate(factor_tile(work_ref)):
            until = -(-len(others) * (place + 1) // (BLOCK // 2))
            for other in others[emitted:until]:
                other()
            emitted = until

    def prepare(k):
        here = pl.ds(pl.multiple_of(k * BLOCK, BLOCK), BLOCK)
        after = pl.ds(pl.multiple_of(jnp.minimum(k + 1, STEPS - 1) * BLOCK, BLOCK), BLOCK)
        d_ref[here, :] = jnp.where(r <= c, work_ref[:, :BLOCK], 0.0)
        inverse = work_ref[:, BLOCK:]
        inv_ref[...] = inverse
        u = dot_split_128(split(inverse), split(x_ref[here, after]))
        work_ref[:, :BLOCK] = x_ref[after, after] - dot_split_128(split(jnp.transpose(u)), split(u))

    def step(k, _):
        others = [functools.partial(finish_row, k - 1, b) for b in range(STEPS)]
        others += [functools.partial(clear, k - 1)]
        others += [functools.partial(trail, m, n) for n in range(STEPS // 2) for m in range(STEPS)]
        factor_block(others)
        prepare(k)
        return 0

    factor_block([])
    for copy in copies[1:]:
        copy.wait()
    prepare(0)
    lax.fori_loop(1, STEPS, step, 0)
    end = slice(WIDTH - BLOCK, WIDTH)
    x_ref[end, :] = dot_split_128(split(inv_ref[...]), split(x_ref[end, :]))
    x_ref[end, end] = inv_ref[...]
    mh_ref[end, :], ml_ref[end, :] = split(x_ref[end, :])
    row, col = place_ref[0], place_ref[1]
    mine = pl.ds(pl.multiple_of(jnp.minimum(row, STEPS - 1) * BLOCK, BLOCK), BLOCK)
    other = pl.ds(pl.multiple_of(jnp.minimum(col, STEPS - 1) * BLOCK, BLOCK), BLOCK)
    block = jnp.where(row == col, d_ref[mine, :], x_ref[other, mine])
    corner_ref[...] = jnp.where(row >= col, jnp.transpose(block), 0.0)


def factor(place, gathered):
    vmem, hbm = pl.BlockSpec(memory_space=pltpu.VMEM), pl.BlockSpec(memory_space=pltpu.HBM)
    return pl.pallas_call(
        factor_kernel,
        in_specs=[pl.BlockSpec(memory_space=pltpu.SMEM), hbm],
        out_specs=(vmem, vmem, vmem),
        out_shape=(
            jax.ShapeDtypeStruct((WIDTH, WIDTH), bf16),
            jax.ShapeDtypeStruct((WIDTH, WIDTH), bf16),
            jax.ShapeDtypeStruct((BLOCK, BLOCK), f32),
        ),
        scratch_shapes=[
            pltpu.VMEM((WIDTH, WIDTH), f32),
            pltpu.VMEM((WIDTH, BLOCK), f32),
            pltpu.VMEM((BLOCK, 2 * BLOCK), f32),
            pltpu.VMEM((BLOCK, BLOCK), f32),
            pltpu.VMEM((WIDTH, 2 * BLOCK), bf16),
            pltpu.VMEM((2 * BLOCK, WIDTH), bf16),
            pltpu.VMEM((BLOCK, WIDTH), bf16),
            pltpu.SemaphoreType.DMA((3 * STEPS * 2,)),
        ],
        compiler_params=pltpu.CompilerParams(vmem_limit_bytes=24 * 2**20),
        cost_estimate=pl.CostEstimate(flops=40_000_000_000, bytes_accessed=2**23, transcendentals=0),
        name="factor",
    )(place, gathered)


def apply_kernel(place_ref, mh, ml, corner_ref, *refs):
    v_hbm, outs, (vh, vl, v_ref, sems) = refs[:SIDE], refs[SIDE : SIDE + 3], refs[SIDE + 3 :]
    count = iter(range(sems.shape[0]))
    copy = lambda src, dst: pltpu.make_async_copy(src, dst, sems.at[next(count)])
    arriving = [copy(v, v_ref.at[d]) for d, v in enumerate(v_hbm)]
    for c in arriving:
        c.start()
    row, col = place_ref[0], place_ref[1]
    other = pl.ds(pl.multiple_of(jnp.minimum(col, STEPS - 1) * BLOCK, BLOCK), BLOCK)
    sent = [copy(corner_ref, outs[2])]
    sent[0].start()
    my_y, my_x = row // SIDE, row % SIDE
    swapped = jnp.where((my_y == 1) | (my_y == 2), 1, 0)
    for d in range(SIDE):
        arriving[d].wait()
        for e in range(2):
            block = SIDE * (e + swapped - 2 * e * swapped) + (my_x + d) % SIDE
            at = pl.ds(pl.multiple_of(block * BLOCK, BLOCK), BLOCK)
            vh[at], vl[at] = split(v_ref[d, e * BLOCK : (e + 1) * BLOCK])
    for k in reversed(range(0, WIDTH, CHUNK)):
        at, upto = slice(k, k + CHUNK), slice(0, k + CHUNK)
        vh[at], vl[at] = split(dot_split((mh[at, upto], ml[at, upto]), (vh[upto], vl[upto])))
    for k in range(0, WIDTH, CHUNK):
        at, on = slice(k, k + CHUNK), slice(k, WIDTH)
        vh[at], vl[at] = split(dot_split((mh[on, at], ml[on, at]), (vh[on], vl[on]), ((0,), (0,))))
        for v, m in ((vh, mh), (vl, ml)):
            panel = jnp.transpose(m[other, at].astype(f32)).astype(bf16)
            v[at, :BLOCK] = jnp.where(col < STEPS, panel, v[at, :BLOCK])
        for v, out in zip((vh, vl), outs):
            sent.append(copy(v.at[at], out.at[at]))
            sent[-1].start()
    for c in sent:
        c.wait()


def apply(place, mh, ml, corner, across):
    vmem, hbm = pl.BlockSpec(memory_space=pltpu.VMEM), pl.BlockSpec(memory_space=pltpu.HBM)
    square = pltpu.VMEM((WIDTH, WIDTH), bf16)
    return pl.pallas_call(
        apply_kernel,
        in_specs=[pl.BlockSpec(memory_space=pltpu.SMEM), vmem, vmem, vmem] + [hbm] * SIDE,
        out_specs=(hbm,) * 3,
        out_shape=(pltpu.HBM((WIDTH, WIDTH), bf16), pltpu.HBM((WIDTH, WIDTH), bf16), pltpu.HBM((BLOCK, BLOCK), f32)),
        scratch_shapes=[square, square]
        + [
            pltpu.VMEM((SIDE, 2 * BLOCK, WIDTH), f32),
            pltpu.SemaphoreType.DMA((SIDE + 1 + 2 * (WIDTH // CHUNK),)),
        ],
        compiler_params=pltpu.CompilerParams(vmem_limit_bytes=20 * 2**20),
        cost_estimate=pl.CostEstimate(flops=10_000_000_000, bytes_accessed=2**23, transcendentals=0),
        name="apply",
    )(place, mh, ml, corner, *across)


def update_kernel(place_ref, a_ref, u_ref, yh_ref, yl_ref, corner_ref, out_ref):
    row, col, step = place_ref[0], place_ref[1], pl.program_id(0)
    slots = [jnp.where(step < HALF // CHUNK, j, other_half(j) - STEPS) for j in range(STEPS)]
    u = split(jnp.concatenate([u_ref[s] for s in slots], 1))
    product = dot_split(u, (yh_ref[...], yl_ref[...]))
    out_ref[:, :BLOCK] = jnp.where(col < STEPS, product[:, :BLOCK], a_ref[:, :BLOCK] - product[:, :BLOCK])
    out_ref[:, BLOCK:] = a_ref[:, BLOCK:] - product[:, BLOCK:]

    @pl.when((step == 0) & (row < STEPS))
    def _():
        out_ref[:BLOCK, :] = jnp.zeros((BLOCK, WIDTH), f32)

        @pl.when(col < STEPS)
        def _():
            out_ref[:BLOCK, :BLOCK] = corner_ref[...]


def update(place, blocked, gathered, yh, yl, corner):
    per_half = HALF // CHUNK
    whole = lambda *shape: pl.BlockSpec(shape, lambda i: (0, 0))
    return pl.pallas_call(
        update_kernel,
        grid=(WIDTH // CHUNK,),
        in_specs=[
            pl.BlockSpec(memory_space=pltpu.SMEM),
            pl.BlockSpec((CHUNK, WIDTH), lambda i: (i, 0)),
            pl.BlockSpec((STEPS, CHUNK, BLOCK), lambda i: (i // per_half, i % per_half, 0)),
            whole(WIDTH, WIDTH),
            whole(WIDTH, WIDTH),
            whole(BLOCK, BLOCK),
        ],
        out_specs=pl.BlockSpec((CHUNK, WIDTH), lambda i: (i, 0)),
        out_shape=jax.ShapeDtypeStruct((WIDTH, WIDTH), f32),
        compiler_params=pltpu.CompilerParams(vmem_limit_bytes=28 * 2**20),
        name="update",
    )(place, blocked, gathered, yh, yl, corner)


def per_device(blocked):
    rows, cols = lax.axis_size("prow"), lax.axis_size("pcol")
    row, col = lax.axis_index("prow"), lax.axis_index("pcol")
    span = range(STEPS)
    in_hbm = lambda a: pltpu.with_memory_space_constraint(a, pltpu.HBM)

    piece = 3 * BLOCK // rows
    third = jnp.where(row < 3, row, jnp.where(row == 3, jnp.where(col < 4, 2, 1), jnp.where(row == 7, 0, row - 4)))
    padded = jnp.pad(blocked[:BLOCK, :BLOCK], ((16, 16), (0, 0)))
    parts = []
    for g in range(6):
        pairs = []
        for i in span:
            for k in span:
                if window_place(i, k):
                    to, b = window_place(i, k)
                    pairs.append((i * cols + k, (5 * b + g) * cols + to))
        part = lax.dynamic_slice(padded, (16 + piece * g - 8 * jnp.clip(third, 0, 2), 0), (piece, BLOCK))
        parts.append(lax.ppermute(part, ("prow", "pcol"), pairs))
    part = functools.reduce(jnp.add, parts)
    lower = lax.ppermute(blocked[HALF:, :BLOCK], "pcol", [(k, other_half(k)) for k in span])
    strip = lax.all_to_all(jnp.broadcast_to(part, (rows, piece, BLOCK)), "prow", 0, 0)
    window = lax.all_gather(strip.reshape(3 * BLOCK, BLOCK), "pcol", axis=0)
    payload = jnp.where(col < STEPS, blocked[:HALF, :BLOCK], lower)

    own = blocked[:BLOCK]
    moves = ([(0, 1), (1, 0)], [(0, 3), (1, 2)], [(0, 2), (1, 3)])
    got = [
        lax.ppermute(own, "prow", [(a * SIDE + x, b * SIDE + x) for a, b in move for x in range(SIDE)])
        for move in moves
    ]
    source = row < 2 * SIDE
    pair = jnp.concatenate([jnp.where(source, own, got[1]), jnp.where(source, got[0], got[2])], 0)
    payload, window, _ = lax.optimization_barrier((payload, window, pair))
    panels = lax.all_gather(payload, "pcol", axis=0)
    across = [pair]
    for d in range(1, SIDE):
        across.append(lax.ppermute(pair, "prow", [(r // SIDE * SIDE + (r + d) % SIDE, r) for r in range(rows)]))

    place = jnp.stack([row, col])
    mh, ml, corner = factor(place, in_hbm(window))
    applied = apply(place, mh, ml, corner, [in_hbm(v) for v in across])
    return update(place, *(in_hbm(v) for v in (blocked, panels, *applied)))


def solution(mesh):
    return jax.shard_map(
        per_device,
        mesh=mesh,
        in_specs=(P("prow", "pcol"),),
        out_specs=P("prow", "pcol"),
        check_vma=False,
    )
```

```python
import functools

import jax
import jax.numpy as jnp
from jax import lax
from jax.experimental import pallas as pl
from jax.experimental.pallas import tpu as pltpu
from jax.sharding import PartitionSpec as P


BLOCK = 128
STEPS = 8
WIDTH = STEPS * BLOCK
HALF = WIDTH // 2
SIDE = 4
NB = 32
GROUP = 16
CHUNK = 256


bf16 = jnp.bfloat16
f32 = jnp.float32


def split(x):
    hi = x.astype(bf16)
    return hi, (x - hi.astype(f32)).astype(bf16)


def dot(a, b, dims=((1,), (0,))):
    return lax.dot_general(a, b, (dims, ((), ())), preferred_element_type=f32)


def dot_split(a, b, dims=((1,), (0,))):
    return dot(a[0], b[0], dims) + dot(a[1], b[0], dims) + dot(a[0], b[1], dims)


def dot_split_128(a, b):
    (ah, al), (bh, bl) = a, b
    return dot(jnp.concatenate([ah, al], 1), jnp.concatenate([bh, bh], 0)) + dot(ah, bl)


def other_half(k):
    return 14 - k + 2 * (k % 2)


def spread(row):
    return jnp.broadcast_to(row, (8, row.shape[1]))


def factor_tile(work_ref):
    tiles = NB // 8
    sub = lax.broadcasted_iota(jnp.int32, (8, 128), 0)
    for base in range(0, BLOCK, NB):
        rows = [
            [work_ref[base + 8 * t : base + 8 * t + 8, h * 128 : h * 128 + 128] for h in range(2)]
            for t in range(tiles)
        ]
        scale = [None] * tiles
        for first in range(0, NB, GROUP):
            last = first + GROUP
            cols = {
                (j, t): jnp.broadcast_to(rows[t][0][:, base + j : base + j + 1], (8, 128))
                for j in range(first, last)
                for t in range(j // 8, tiles)
            }
            for k in range(first, last, 2):
                tk, rk = divmod(k, 8)
                a = spread(cols[k, tk][rk : rk + 1])
                b = spread(cols[k, tk][rk + 1 : rk + 2])
                c = spread(cols[k + 1, tk][rk + 1 : rk + 2])
                det = a * c - b * b
                inv, ra = 1.0 / det, 1.0 / a
                r0, r1 = lax.rsqrt(a), lax.rsqrt(det * ra)
                scale[tk] = r0 if rk == 0 else jnp.where(sub == rk, r0, scale[tk])
                scale[tk] = jnp.where(sub == rk + 1, r1, scale[tk])
                p, q = {}, {}
                for t in range(tk + (rk == 6), tiles):
                    p[t] = c * cols[k, t] - b * cols[k + 1, t]
                    q[t] = a * cols[k + 1, t] - b * cols[k, t]
                pd, qd = {t: v * inv for t, v in p.items()}, {t: v * inv for t, v in q.items()}
                for j in range(k + 2, last):
                    tj, rj = divmod(j, 8)
                    c0 = spread(cols[k, tj][rj : rj + 1])
                    c1 = spread(cols[k + 1, tj][rj : rj + 1])
                    for t in range(tj, tiles):
                        if j < k + 4:
                            cols[j, t] = cols[j, t] - (p[t] * c0 + q[t] * c1) * inv
                        else:
                            cols[j, t] = cols[j, t] - (pd[t] * c0 + qd[t] * c1)
                if tk in pd:
                    pd[tk], qd[tk] = (jnp.where(sub > rk + 1, v[tk], 0.0) for v in (pd, qd))
                second = jnp.where(sub == rk + 1, b * ra, 0.0)
                for h in range(2):
                    s0 = spread(rows[tk][h][rk : rk + 1])
                    s1 = spread(rows[tk][h][rk + 1 : rk + 2])
                    rows[tk][h] = rows[tk][h] - second * s0
                    for t in pd:
                        rows[t][h] = rows[t][h] - (pd[t] * s0 + qd[t] * s1)
                yield
        done = jnp.concatenate(
            [jnp.concatenate([rows[t][h] * scale[t] for h in range(2)], 1) for t in range(tiles)], 0
        )
        end = base + NB
        work_ref[base:end, :] = done
        if end < BLOCK:
            lh, ll = split(jnp.transpose(done[:, :128])[end:])
            uh, ul = split(done)
            left = jnp.concatenate([lh, lh, ll], 1)
            right = jnp.concatenate([uh, ul, uh], 0)
            work_ref[end:, :] = work_ref[end:, :] - dot(left, right)


def factor_kernel(
    place_ref, w_ref, mh_ref, ml_ref, corner_ref,
    x_ref, d_ref, work_ref, inv_ref, left_ref, right_ref, rest_ref, sems,
):
    quarters = x_ref.reshape(2, SIDE, 2, 2, BLOCK // 4, WIDTH)
    first, later = [], []
    for slot in range(2 * STEPS):
        b, k = (0, slot) if slot < STEPS else (1, other_half(slot))
        for side in range(SIDE):
            a, y = (0, side) if side < 2 else (1, SIDE - 1 - side)
            dst = quarters.at[y, :, b, a, :, k * BLOCK : (k + 1) * BLOCK]
            copy = pltpu.make_async_copy(w_ref.at[slot, side], dst, sems.at[slot * SIDE + side])
            (first if y == 0 and k == 0 else later).append(copy)
    for copy in first + later:
        copy.start()
    for copy in first:
        copy.wait()
    r = lax.broadcasted_iota(jnp.int32, (BLOCK, BLOCK), 0)
    c = lax.broadcasted_iota(jnp.int32, (BLOCK, BLOCK), 1)
    work_ref[:, :BLOCK] = x_ref[:BLOCK, :BLOCK]

    def finish_row(k, b):
        here, at = pl.ds(pl.multiple_of(k * BLOCK, BLOCK), BLOCK), slice(b * BLOCK, (b + 1) * BLOCK)
        old, inverse = x_ref[here, at], inv_ref[...]
        new = jnp.where(k == b, inverse, dot_split_128(split(inverse), split(old)))
        x_ref[here, at] = new
        hi, lo = split(new)
        right_ref[:BLOCK, at], rest_ref[:, at] = hi, lo
        mh_ref[here, at] = jnp.where(b <= k, hi, jnp.zeros_like(hi))
        ml_ref[here, at] = jnp.where(b <= k, lo, jnp.zeros_like(lo))
        right_ref[BLOCK:, at] = hi
        left_ref[at, :BLOCK], left_ref[at, BLOCK:] = split(jnp.where(b > k, jnp.transpose(new), 0.0))

    def clear(k):
        here = pl.ds(pl.multiple_of(k * BLOCK, BLOCK), BLOCK)
        block = lax.broadcasted_iota(jnp.int32, (WIDTH, BLOCK), 0) // BLOCK
        x_ref[:, here] = jnp.where(block > k, 0.0, x_ref[:, here])

    def trail(m, n):
        at, to = slice(m * BLOCK, (m + 1) * BLOCK), slice(n * 2 * BLOCK, (n + 1) * 2 * BLOCK)
        product = dot(left_ref[at, :], right_ref[:, to]) + dot(left_ref[at, :BLOCK], rest_ref[:, to])
        x_ref[at, to] = x_ref[at, to] - product

    def factor_block(others):
        work_ref[:, BLOCK:] = jnp.where(r == c, 1.0, 0.0).astype(f32)
        emitted = 0
        for place, _ in enumerate(factor_tile(work_ref)):
            until = -(-len(others) * (place + 1) // (BLOCK // 2))
            for other in others[emitted:until]:
                other()
            emitted = until

    def prepare(k):
        here = pl.ds(pl.multiple_of(k * BLOCK, BLOCK), BLOCK)
        after = pl.ds(pl.multiple_of(jnp.minimum(k + 1, STEPS - 1) * BLOCK, BLOCK), BLOCK)
        d_ref[here, :] = jnp.where(r <= c, work_ref[:, :BLOCK], 0.0)
        inverse = work_ref[:, BLOCK:]
        inv_ref[...] = inverse
        u = dot_split_128(split(inverse), split(x_ref[here, after]))
        work_ref[:, :BLOCK] = x_ref[after, after] - dot_split_128(split(jnp.transpose(u)), split(u))

    def step(k, _):
        others = [functools.partial(finish_row, k - 1, b) for b in range(STEPS)]
        others += [functools.partial(clear, k - 1)]
        others += [functools.partial(trail, m, n) for n in range(STEPS // 2) for m in range(STEPS)]
        factor_block(others)
        prepare(k)
        return 0

    factor_block([])
    for copy in later:
        copy.wait()
    prepare(0)
    lax.fori_loop(1, STEPS, step, 0)
    end = slice(WIDTH - BLOCK, WIDTH)
    x_ref[end, :] = dot_split_128(split(inv_ref[...]), split(x_ref[end, :]))
    x_ref[end, end] = inv_ref[...]
    mh_ref[end, :], ml_ref[end, :] = split(x_ref[end, :])
    row, col = place_ref[0], place_ref[1]
    mine = pl.ds(pl.multiple_of(jnp.minimum(row, STEPS - 1) * BLOCK, BLOCK), BLOCK)
    other = pl.ds(pl.multiple_of(jnp.minimum(col, STEPS - 1) * BLOCK, BLOCK), BLOCK)
    block = jnp.where(row == col, d_ref[mine, :], x_ref[other, mine])
    corner_ref[...] = jnp.where(row >= col, jnp.transpose(block), 0.0)


def factor(place, gathered):
    vmem, hbm = pl.BlockSpec(memory_space=pltpu.VMEM), pl.BlockSpec(memory_space=pltpu.HBM)
    return pl.pallas_call(
        factor_kernel,
        in_specs=[pl.BlockSpec(memory_space=pltpu.SMEM), hbm],
        out_specs=(vmem, vmem, vmem),
        out_shape=(
            jax.ShapeDtypeStruct((WIDTH, WIDTH), bf16),
            jax.ShapeDtypeStruct((WIDTH, WIDTH), bf16),
            jax.ShapeDtypeStruct((BLOCK, BLOCK), f32),
        ),
        scratch_shapes=[
            pltpu.VMEM((WIDTH, WIDTH), f32),
            pltpu.VMEM((WIDTH, BLOCK), f32),
            pltpu.VMEM((BLOCK, 2 * BLOCK), f32),
            pltpu.VMEM((BLOCK, BLOCK), f32),
            pltpu.VMEM((WIDTH, 2 * BLOCK), bf16),
            pltpu.VMEM((2 * BLOCK, WIDTH), bf16),
            pltpu.VMEM((BLOCK, WIDTH), bf16),
            pltpu.SemaphoreType.DMA((2 * STEPS * SIDE,)),
        ],
        compiler_params=pltpu.CompilerParams(vmem_limit_bytes=24 * 2**20),
        cost_estimate=pl.CostEstimate(flops=40_000_000_000, bytes_accessed=2**23, transcendentals=0),
        name="factor",
    )(place, gathered)


def apply_kernel(place_ref, mh, ml, corner_ref, *refs):
    v_hbm, outs, (vh, vl, v_ref, sems) = refs[:SIDE], refs[SIDE : SIDE + 3], refs[SIDE + 3 :]
    count = iter(range(sems.shape[0]))
    copy = lambda src, dst: pltpu.make_async_copy(src, dst, sems.at[next(count)])
    arriving = [copy(v, v_ref.at[d]) for d, v in enumerate(v_hbm)]
    for c in arriving:
        c.start()
    row, col = place_ref[0], place_ref[1]
    other = pl.ds(pl.multiple_of(jnp.minimum(col, STEPS - 1) * BLOCK, BLOCK), BLOCK)
    sent = [copy(corner_ref, outs[2])]
    sent[0].start()
    my_y, my_x = row // SIDE, row % SIDE
    swapped = jnp.where((my_y == 1) | (my_y == 2), 1, 0)
    for d in range(SIDE):
        arriving[d].wait()
        for e in range(2):
            block = SIDE * (e + swapped - 2 * e * swapped) + (my_x + d) % SIDE
            at = pl.ds(pl.multiple_of(block * BLOCK, BLOCK), BLOCK)
            vh[at], vl[at] = split(v_ref[d, e * BLOCK : (e + 1) * BLOCK])
    for k in reversed(range(0, WIDTH, CHUNK)):
        at, upto = slice(k, k + CHUNK), slice(0, k + CHUNK)
        vh[at], vl[at] = split(dot_split((mh[at, upto], ml[at, upto]), (vh[upto], vl[upto])))
    for k in range(0, WIDTH, CHUNK):
        at, on = slice(k, k + CHUNK), slice(k, WIDTH)
        vh[at], vl[at] = split(dot_split((mh[on, at], ml[on, at]), (vh[on], vl[on]), ((0,), (0,))))
        for v, m in ((vh, mh), (vl, ml)):
            panel = jnp.transpose(m[other, at].astype(f32)).astype(bf16)
            v[at, :BLOCK] = jnp.where(col < STEPS, panel, v[at, :BLOCK])
        for v, out in zip((vh, vl), outs):
            sent.append(copy(v.at[at], out.at[at]))
            sent[-1].start()
    for c in sent:
        c.wait()


def apply(place, mh, ml, corner, across):
    vmem, hbm = pl.BlockSpec(memory_space=pltpu.VMEM), pl.BlockSpec(memory_space=pltpu.HBM)
    square = pltpu.VMEM((WIDTH, WIDTH), bf16)
    return pl.pallas_call(
        apply_kernel,
        in_specs=[pl.BlockSpec(memory_space=pltpu.SMEM), vmem, vmem, vmem] + [hbm] * SIDE,
        out_specs=(hbm,) * 3,
        out_shape=(pltpu.HBM((WIDTH, WIDTH), bf16), pltpu.HBM((WIDTH, WIDTH), bf16), pltpu.HBM((BLOCK, BLOCK), f32)),
        scratch_shapes=[square, square]
        + [
            pltpu.VMEM((SIDE, 2 * BLOCK, WIDTH), f32),
            pltpu.SemaphoreType.DMA((SIDE + 1 + 2 * (WIDTH // CHUNK),)),
        ],
        compiler_params=pltpu.CompilerParams(vmem_limit_bytes=20 * 2**20),
        cost_estimate=pl.CostEstimate(flops=10_000_000_000, bytes_accessed=2**23, transcendentals=0),
        name="apply",
    )(place, mh, ml, corner, *across)


def update_kernel(place_ref, a_ref, u_ref, yh_ref, yl_ref, corner_ref, out_ref):
    row, col, step = place_ref[0], place_ref[1], pl.program_id(0)
    slots = [jnp.where(step < HALF // CHUNK, j, other_half(j) - STEPS) for j in range(STEPS)]
    u = split(jnp.concatenate([u_ref[s] for s in slots], 1))
    product = dot_split(u, (yh_ref[...], yl_ref[...]))
    out_ref[:, :BLOCK] = jnp.where(col < STEPS, product[:, :BLOCK], a_ref[:, :BLOCK] - product[:, :BLOCK])
    out_ref[:, BLOCK:] = a_ref[:, BLOCK:] - product[:, BLOCK:]

    @pl.when((step == 0) & (row < STEPS))
    def _():
        out_ref[:BLOCK, :] = jnp.zeros((BLOCK, WIDTH), f32)

        @pl.when(col < STEPS)
        def _():
            out_ref[:BLOCK, :BLOCK] = corner_ref[...]


def update(place, blocked, gathered, yh, yl, corner):
    per_half = HALF // CHUNK
    whole = lambda *shape: pl.BlockSpec(shape, lambda i: (0, 0))
    return pl.pallas_call(
        update_kernel,
        grid=(WIDTH // CHUNK,),
        in_specs=[
            pl.BlockSpec(memory_space=pltpu.SMEM),
            pl.BlockSpec((CHUNK, WIDTH), lambda i: (i, 0)),
            pl.BlockSpec((STEPS, CHUNK, BLOCK), lambda i: (i // per_half, i % per_half, 0)),
            whole(WIDTH, WIDTH),
            whole(WIDTH, WIDTH),
            whole(BLOCK, BLOCK),
        ],
        out_specs=pl.BlockSpec((CHUNK, WIDTH), lambda i: (i, 0)),
        out_shape=jax.ShapeDtypeStruct((WIDTH, WIDTH), f32),
        compiler_params=pltpu.CompilerParams(vmem_limit_bytes=28 * 2**20),
        name="update",
    )(place, blocked, gathered, yh, yl, corner)


def per_device(blocked):
    rows, cols = lax.axis_size("prow"), lax.axis_size("pcol")
    row, col = lax.axis_index("prow"), lax.axis_index("pcol")
    span = range(STEPS)
    in_hbm = lambda a: pltpu.with_memory_space_constraint(a, pltpu.HBM)

    quarter = BLOCK // 4
    corner = blocked[:BLOCK, :BLOCK]
    parts = []
    for b, a in ((0, 1), (1, 0), (1, 1)):
        pairs = []
        for i in span:
            to_row = (SIDE - 1 - i // SIDE) * SIDE + i % SIDE if a else i
            for k in span:
                pairs.append((i * cols + k, to_row * cols + (other_half(k) if b else k)))
        at = (2 * b + a) * quarter
        parts.append(lax.ppermute(corner[at : at + quarter], ("prow", "pcol"), pairs))
    stays = (row < STEPS) & (col < STEPS)
    part = jnp.where(stays, corner[:quarter], parts[0] + parts[1] + parts[2])
    lower = lax.ppermute(blocked[HALF:, :BLOCK], "pcol", [(k, other_half(k)) for k in span])
    strip = lax.all_to_all(jnp.broadcast_to(part, (rows, quarter, BLOCK)), "prow", 0, 0)
    window = lax.all_gather(strip.reshape(HALF, BLOCK), "pcol", axis=0)
    window = window.reshape(cols, SIDE, SIDE, quarter, BLOCK)
    payload = jnp.where(col < STEPS, blocked[:HALF, :BLOCK], lower)

    own = blocked[:BLOCK]
    moves = ([(0, 1), (1, 0)], [(0, 3), (1, 2)], [(0, 2), (1, 3)])
    got = [
        lax.ppermute(own, "prow", [(a * SIDE + x, b * SIDE + x) for a, b in move for x in range(SIDE)])
        for move in moves
    ]
    source = row < 2 * SIDE
    pair = jnp.concatenate([jnp.where(source, own, got[1]), jnp.where(source, got[0], got[2])], 0)
    payload, window, _ = lax.optimization_barrier((payload, window, pair))
    panels = lax.all_gather(payload, "pcol", axis=0)
    across = [pair]
    for d in range(1, SIDE):
        across.append(lax.ppermute(pair, "prow", [(r // SIDE * SIDE + (r + d) % SIDE, r) for r in range(rows)]))

    place = jnp.stack([row, col])
    mh, ml, corner = factor(place, in_hbm(window))
    applied = apply(place, mh, ml, corner, [in_hbm(v) for v in across])
    return update(place, *(in_hbm(v) for v in (blocked, panels, *applied)))


def solution(mesh):
    return jax.shard_map(
        per_device,
        mesh=mesh,
        in_specs=(P("prow", "pcol"),),
        out_specs=P("prow", "pcol"),
        check_vma=False,
    )
```

```python
import functools

import jax
import jax.numpy as jnp
from jax import lax
from jax.experimental import pallas as pl
from jax.experimental.pallas import tpu as pltpu
from jax.sharding import PartitionSpec as P


BLOCK = 128
STEPS = 8
WIDTH = STEPS * BLOCK
HALF = WIDTH // 2
SIDE = 4
NB = 32
GROUP = 16
CHUNK = 256


bf16 = jnp.bfloat16
f32 = jnp.float32


def split(x):
    hi = x.astype(bf16)
    return hi, (x - hi.astype(f32)).astype(bf16)


def dot(a, b, dims=((1,), (0,))):
    return lax.dot_general(a, b, (dims, ((), ())), preferred_element_type=f32)


def dot_split(a, b, dims=((1,), (0,))):
    return dot(a[0], b[0], dims) + dot(a[1], b[0], dims) + dot(a[0], b[1], dims)


def dot_split_128(a, b):
    (ah, al), (bh, bl) = a, b
    return dot(jnp.concatenate([ah, al], 1), jnp.concatenate([bh, bh], 0)) + dot(ah, bl)


def other_half(k):
    return 14 - k + 2 * (k % 2)


def spread(row):
    return jnp.broadcast_to(row, (8, row.shape[1]))


def factor_tile(work_ref):
    tiles = NB // 8
    sub = lax.broadcasted_iota(jnp.int32, (8, 128), 0)
    for base in range(0, BLOCK, NB):
        rows = [
            [work_ref[base + 8 * t : base + 8 * t + 8, h * 128 : h * 128 + 128] for h in range(2)]
            for t in range(tiles)
        ]
        scale = [None] * tiles
        for first in range(0, NB, GROUP):
            last = first + GROUP
            cols = {
                (j, t): jnp.broadcast_to(rows[t][0][:, base + j : base + j + 1], (8, 128))
                for j in range(first, last)
                for t in range(j // 8, tiles)
            }
            for k in range(first, last, 2):
                tk, rk = divmod(k, 8)
                a = spread(cols[k, tk][rk : rk + 1])
                b = spread(cols[k, tk][rk + 1 : rk + 2])
                c = spread(cols[k + 1, tk][rk + 1 : rk + 2])
                det = a * c - b * b
                inv, ra = 1.0 / det, 1.0 / a
                r0, r1 = lax.rsqrt(a), lax.rsqrt(det * ra)
                scale[tk] = r0 if rk == 0 else jnp.where(sub == rk, r0, scale[tk])
                scale[tk] = jnp.where(sub == rk + 1, r1, scale[tk])
                p, q = {}, {}
                for t in range(tk + (rk == 6), tiles):
                    p[t] = c * cols[k, t] - b * cols[k + 1, t]
                    q[t] = a * cols[k + 1, t] - b * cols[k, t]
                pd, qd = {t: v * inv for t, v in p.items()}, {t: v * inv for t, v in q.items()}
                for j in range(k + 2, last):
                    tj, rj = divmod(j, 8)
                    c0 = spread(cols[k, tj][rj : rj + 1])
                    c1 = spread(cols[k + 1, tj][rj : rj + 1])
                    for t in range(tj, tiles):
                        if j < k + 4:
                            cols[j, t] = cols[j, t] - (p[t] * c0 + q[t] * c1) * inv
                        else:
                            cols[j, t] = cols[j, t] - (pd[t] * c0 + qd[t] * c1)
                if tk in pd:
                    pd[tk], qd[tk] = (jnp.where(sub > rk + 1, v[tk], 0.0) for v in (pd, qd))
                second = jnp.where(sub == rk + 1, b * ra, 0.0)
                for h in range(2):
                    s0 = spread(rows[tk][h][rk : rk + 1])
                    s1 = spread(rows[tk][h][rk + 1 : rk + 2])
                    rows[tk][h] = rows[tk][h] - second * s0
                    for t in pd:
                        rows[t][h] = rows[t][h] - (pd[t] * s0 + qd[t] * s1)
                yield
        done = jnp.concatenate(
            [jnp.concatenate([rows[t][h] * scale[t] for h in range(2)], 1) for t in range(tiles)], 0
        )
        end = base + NB
        work_ref[base:end, :] = done
        if end < BLOCK:
            lh, ll = split(jnp.transpose(done[:, :128])[end:])
            uh, ul = split(done)
            left = jnp.concatenate([lh, lh, ll], 1)
            right = jnp.concatenate([uh, ul, uh], 0)
            work_ref[end:, :] = work_ref[end:, :] - dot(left, right)


def factor_kernel(
    place_ref, w_ref, mh_ref, ml_ref, corner_ref,
    x_ref, d_ref, work_ref, inv_ref, left_ref, right_ref, rest_ref, sems,
):
    quarters = x_ref.reshape(2, SIDE, 2, 2, BLOCK // 4, WIDTH)
    first, later = [], []
    for slot in range(2 * STEPS):
        b, k = (0, slot) if slot < STEPS else (1, other_half(slot))
        for side in range(SIDE):
            a, y = (0, side) if side < 2 else (1, SIDE - 1 - side)
            dst = quarters.at[y, :, b, a, :, k * BLOCK : (k + 1) * BLOCK]
            copy = pltpu.make_async_copy(w_ref.at[slot, side], dst, sems.at[slot * SIDE + side])
            (first if y == 0 and k == 0 else later).append(copy)
    for copy in first + later:
        copy.start()
    for copy in first:
        copy.wait()
    r = lax.broadcasted_iota(jnp.int32, (BLOCK, BLOCK), 0)
    c = lax.broadcasted_iota(jnp.int32, (BLOCK, BLOCK), 1)
    work_ref[:, :BLOCK] = x_ref[:BLOCK, :BLOCK]

    def finish_row(k, b):
        here, at = pl.ds(pl.multiple_of(k * BLOCK, BLOCK), BLOCK), slice(b * BLOCK, (b + 1) * BLOCK)
        old, inverse = x_ref[here, at], inv_ref[...]
        new = jnp.where(k == b, inverse, dot_split_128(split(inverse), split(old)))
        x_ref[here, at] = new
        hi, lo = split(new)
        right_ref[:BLOCK, at], rest_ref[:, at] = hi, lo
        mh_ref[here, at] = jnp.where(b <= k, hi, jnp.zeros_like(hi))
        ml_ref[here, at] = jnp.where(b <= k, lo, jnp.zeros_like(lo))
        right_ref[BLOCK:, at] = hi
        left_ref[at, :BLOCK], left_ref[at, BLOCK:] = split(jnp.where(b > k, jnp.transpose(new), 0.0))

    def clear(k):
        here = pl.ds(pl.multiple_of(k * BLOCK, BLOCK), BLOCK)
        block = lax.broadcasted_iota(jnp.int32, (WIDTH, BLOCK), 0) // BLOCK
        x_ref[:, here] = jnp.where(block > k, 0.0, x_ref[:, here])

    def trail(m, n):
        at, to = slice(m * BLOCK, (m + 1) * BLOCK), slice(n * 2 * BLOCK, (n + 1) * 2 * BLOCK)
        product = dot(left_ref[at, :], right_ref[:, to]) + dot(left_ref[at, :BLOCK], rest_ref[:, to])
        x_ref[at, to] = x_ref[at, to] - product

    def factor_block(others):
        work_ref[:, BLOCK:] = jnp.where(r == c, 1.0, 0.0).astype(f32)
        emitted = 0
        for place, _ in enumerate(factor_tile(work_ref)):
            until = -(-len(others) * (place + 1) // (BLOCK // 2))
            for other in others[emitted:until]:
                other()
            emitted = until

    def prepare(k):
        here = pl.ds(pl.multiple_of(k * BLOCK, BLOCK), BLOCK)
        after = pl.ds(pl.multiple_of(jnp.minimum(k + 1, STEPS - 1) * BLOCK, BLOCK), BLOCK)
        d_ref[here, :] = jnp.where(r <= c, work_ref[:, :BLOCK], 0.0)
        inverse = work_ref[:, BLOCK:]
        inv_ref[...] = inverse
        u = dot_split_128(split(inverse), split(x_ref[here, after]))
        work_ref[:, :BLOCK] = x_ref[after, after] - dot_split_128(split(jnp.transpose(u)), split(u))

    def step(k, _, lowest=1):
        others = [functools.partial(finish_row, k - 1, b) for b in range(STEPS)]
        others += [functools.partial(clear, k - 1)]
        others += [functools.partial(trail, m, n) for n in range(STEPS // 2) for m in range(lowest, STEPS)]
        factor_block(others)
        prepare(k)
        return 0

    factor_block([])
    for copy in later:
        copy.wait()
    prepare(0)
    lax.fori_loop(1, STEPS // 2, step, 0)
    lax.fori_loop(STEPS // 2, STEPS, functools.partial(step, lowest=STEPS // 2), 0)
    end = slice(WIDTH - BLOCK, WIDTH)
    x_ref[end, :] = dot_split_128(split(inv_ref[...]), split(x_ref[end, :]))
    x_ref[end, end] = inv_ref[...]
    mh_ref[end, :], ml_ref[end, :] = split(x_ref[end, :])
    row, col = place_ref[0], place_ref[1]
    mine = pl.ds(pl.multiple_of(jnp.minimum(row, STEPS - 1) * BLOCK, BLOCK), BLOCK)
    other = pl.ds(pl.multiple_of(jnp.minimum(col, STEPS - 1) * BLOCK, BLOCK), BLOCK)
    block = jnp.where(row == col, d_ref[mine, :], x_ref[other, mine])
    corner_ref[...] = jnp.where(row >= col, jnp.transpose(block), 0.0)


def factor(place, gathered):
    vmem, hbm = pl.BlockSpec(memory_space=pltpu.VMEM), pl.BlockSpec(memory_space=pltpu.HBM)
    return pl.pallas_call(
        factor_kernel,
        in_specs=[pl.BlockSpec(memory_space=pltpu.SMEM), hbm],
        out_specs=(vmem, vmem, vmem),
        out_shape=(
            jax.ShapeDtypeStruct((WIDTH, WIDTH), bf16),
            jax.ShapeDtypeStruct((WIDTH, WIDTH), bf16),
            jax.ShapeDtypeStruct((BLOCK, BLOCK), f32),
        ),
        scratch_shapes=[
            pltpu.VMEM((WIDTH, WIDTH), f32),
            pltpu.VMEM((WIDTH, BLOCK), f32),
            pltpu.VMEM((BLOCK, 2 * BLOCK), f32),
            pltpu.VMEM((BLOCK, BLOCK), f32),
            pltpu.VMEM((WIDTH, 2 * BLOCK), bf16),
            pltpu.VMEM((2 * BLOCK, WIDTH), bf16),
            pltpu.VMEM((BLOCK, WIDTH), bf16),
            pltpu.SemaphoreType.DMA((2 * STEPS * SIDE,)),
        ],
        compiler_params=pltpu.CompilerParams(vmem_limit_bytes=24 * 2**20),
        cost_estimate=pl.CostEstimate(flops=40_000_000_000, bytes_accessed=2**23, transcendentals=0),
        name="factor",
    )(place, gathered)


def apply_kernel(place_ref, mh, ml, corner_ref, *refs):
    v_hbm, outs, (vh, vl, v_ref, sems) = refs[:SIDE], refs[SIDE : SIDE + 3], refs[SIDE + 3 :]
    count = iter(range(sems.shape[0]))
    copy = lambda src, dst: pltpu.make_async_copy(src, dst, sems.at[next(count)])
    arriving = [copy(v, v_ref.at[d]) for d, v in enumerate(v_hbm)]
    for c in arriving:
        c.start()
    row, col = place_ref[0], place_ref[1]
    other = pl.ds(pl.multiple_of(jnp.minimum(col, STEPS - 1) * BLOCK, BLOCK), BLOCK)
    sent = [copy(corner_ref, outs[2])]
    sent[0].start()
    my_y, my_x = row // SIDE, row % SIDE
    swapped = jnp.where((my_y == 1) | (my_y == 2), 1, 0)
    for d in range(SIDE):
        arriving[d].wait()
        for e in range(2):
            block = SIDE * (e + swapped - 2 * e * swapped) + (my_x + d) % SIDE
            at = pl.ds(pl.multiple_of(block * BLOCK, BLOCK), BLOCK)
            vh[at], vl[at] = split(v_ref[d, e * BLOCK : (e + 1) * BLOCK])
    for k in reversed(range(0, WIDTH, CHUNK)):
        at, upto = slice(k, k + CHUNK), slice(0, k + CHUNK)
        vh[at], vl[at] = split(dot_split((mh[at, upto], ml[at, upto]), (vh[upto], vl[upto])))
    for k in range(0, WIDTH, CHUNK):
        at, on = slice(k, k + CHUNK), slice(k, WIDTH)
        vh[at], vl[at] = split(dot_split((mh[on, at], ml[on, at]), (vh[on], vl[on]), ((0,), (0,))))
        for v, m in ((vh, mh), (vl, ml)):
            panel = jnp.transpose(m[other, at].astype(f32)).astype(bf16)
            v[at, :BLOCK] = jnp.where(col < STEPS, panel, v[at, :BLOCK])
        for v, out in zip((vh, vl), outs):
            sent.append(copy(v.at[at], out.at[at]))
            sent[-1].start()
    for c in sent:
        c.wait()


def apply(place, mh, ml, corner, across):
    vmem, hbm = pl.BlockSpec(memory_space=pltpu.VMEM), pl.BlockSpec(memory_space=pltpu.HBM)
    square = pltpu.VMEM((WIDTH, WIDTH), bf16)
    return pl.pallas_call(
        apply_kernel,
        in_specs=[pl.BlockSpec(memory_space=pltpu.SMEM), vmem, vmem, vmem] + [hbm] * SIDE,
        out_specs=(hbm,) * 3,
        out_shape=(pltpu.HBM((WIDTH, WIDTH), bf16), pltpu.HBM((WIDTH, WIDTH), bf16), pltpu.HBM((BLOCK, BLOCK), f32)),
        scratch_shapes=[square, square]
        + [
            pltpu.VMEM((SIDE, 2 * BLOCK, WIDTH), f32),
            pltpu.SemaphoreType.DMA((SIDE + 1 + 2 * (WIDTH // CHUNK),)),
        ],
        compiler_params=pltpu.CompilerParams(vmem_limit_bytes=20 * 2**20),
        cost_estimate=pl.CostEstimate(flops=10_000_000_000, bytes_accessed=2**23, transcendentals=0),
        name="apply",
    )(place, mh, ml, corner, *across)


def update_kernel(place_ref, a_ref, u_ref, corner_ref, yh_hbm, yl_hbm, out_ref, yh, yl, sems):
    row, col, step = place_ref[0], place_ref[1], pl.program_id(0)
    blocks = [slice(k, k + CHUNK) for k in range(0, WIDTH, CHUNK)]
    arriving = [
        [pltpu.make_async_copy(src.at[at], dst.at[at], sems.at[m, n]) for m, (src, dst) in enumerate(((yh_hbm, yh), (yl_hbm, yl)))]
        for n, at in enumerate(blocks)
    ]

    @pl.when(step == 0)
    def _():
        for copies in arriving:
            for copy in copies:
                copy.start()

    slots = [jnp.where(step < HALF // CHUNK, j, other_half(j) - STEPS) for j in range(STEPS)]
    uh, ul = split(jnp.concatenate([u_ref[s] for s in slots], 1))

    def finish(product):
        out_ref[:, :BLOCK] = jnp.where(col < STEPS, product[:, :BLOCK], a_ref[:, :BLOCK] - product[:, :BLOCK])
        out_ref[:, BLOCK:] = a_ref[:, BLOCK:] - product[:, BLOCK:]

    @pl.when(step == 0)
    def _():
        total = None
        for copies, at in zip(arriving, blocks):
            for copy in copies:
                copy.wait()
            part = dot_split((uh[:, at], ul[:, at]), (yh[at], yl[at]))
            total = part if total is None else total + part
        finish(total)

    @pl.when(step > 0)
    def _():
        finish(dot_split((uh, ul), (yh[...], yl[...])))

    @pl.when((step == 0) & (row < STEPS))
    def _():
        out_ref[:BLOCK, :] = jnp.zeros((BLOCK, WIDTH), f32)

        @pl.when(col < STEPS)
        def _():
            out_ref[:BLOCK, :BLOCK] = corner_ref[...]


def update(place, blocked, gathered, yh, yl, corner):
    per_half = HALF // CHUNK
    whole = lambda *shape: pl.BlockSpec(shape, lambda i: (0, 0))
    return pl.pallas_call(
        update_kernel,
        grid=(WIDTH // CHUNK,),
        in_specs=[
            pl.BlockSpec(memory_space=pltpu.SMEM),
            pl.BlockSpec((CHUNK, WIDTH), lambda i: (i, 0)),
            pl.BlockSpec((STEPS, CHUNK, BLOCK), lambda i: (i // per_half, i % per_half, 0)),
            whole(BLOCK, BLOCK),
            pl.BlockSpec(memory_space=pltpu.HBM),
            pl.BlockSpec(memory_space=pltpu.HBM),
        ],
        out_specs=pl.BlockSpec((CHUNK, WIDTH), lambda i: (i, 0)),
        out_shape=jax.ShapeDtypeStruct((WIDTH, WIDTH), f32),
        scratch_shapes=[
            pltpu.VMEM((WIDTH, WIDTH), bf16),
            pltpu.VMEM((WIDTH, WIDTH), bf16),
            pltpu.SemaphoreType.DMA((2, WIDTH // CHUNK)),
        ],
        compiler_params=pltpu.CompilerParams(vmem_limit_bytes=28 * 2**20),
        name="update",
    )(place, blocked, gathered, corner, yh, yl)


def per_device(blocked):
    rows, cols = lax.axis_size("prow"), lax.axis_size("pcol")
    row, col = lax.axis_index("prow"), lax.axis_index("pcol")
    span = range(STEPS)
    in_hbm = lambda a: pltpu.with_memory_space_constraint(a, pltpu.HBM)

    quarter = BLOCK // 4
    corner = blocked[:BLOCK, :BLOCK]
    parts = []
    for b, a in ((1, 1), (1, 0), (0, 1)):
        pairs = []
        for i in span:
            to_row = (SIDE - 1 - i // SIDE) * SIDE + i % SIDE if a else i
            for k in span:
                pairs.append((i * cols + k, to_row * cols + (other_half(k) if b else k)))
        at = (2 * b + a) * quarter
        parts.append(lax.ppermute(corner[at : at + quarter], ("prow", "pcol"), pairs))
    stays = (row < STEPS) & (col < STEPS)
    part = jnp.where(stays, corner[:quarter], parts[0] + parts[1] + parts[2])
    lower = lax.ppermute(blocked[HALF:, :BLOCK], "pcol", [(k, other_half(k)) for k in span])
    strip = lax.all_to_all(jnp.broadcast_to(part, (rows, quarter, BLOCK)), "prow", 0, 0)
    window = lax.all_gather(strip.reshape(HALF, BLOCK), "pcol", axis=0)
    window = window.reshape(cols, SIDE, SIDE, quarter, BLOCK)
    payload = jnp.where(col < STEPS, blocked[:HALF, :BLOCK], lower)

    own = blocked[:BLOCK]
    moves = ([(0, 1), (1, 0)], [(0, 3), (1, 2)], [(0, 2), (1, 3)])
    got = [
        lax.ppermute(own, "prow", [(a * SIDE + x, b * SIDE + x) for a, b in move for x in range(SIDE)])
        for move in moves
    ]
    source = row < 2 * SIDE
    pair = jnp.concatenate([jnp.where(source, own, got[1]), jnp.where(source, got[0], got[2])], 0)
    payload, window, _ = lax.optimization_barrier((payload, window, pair))
    panels = lax.all_gather(payload, "pcol", axis=0)
    across = [pair]
    for d in range(1, SIDE):
        across.append(lax.ppermute(pair, "prow", [(r // SIDE * SIDE + (r + d) % SIDE, r) for r in range(rows)]))

    place = jnp.stack([row, col])
    mh, ml, corner = factor(place, in_hbm(window))
    applied = apply(place, mh, ml, corner, across)
    return update(place, *(in_hbm(v) for v in (blocked, panels, *applied)))


def solution(mesh):
    return jax.shard_map(
        per_device,
        mesh=mesh,
        in_specs=(P("prow", "pcol"),),
        out_specs=P("prow", "pcol"),
        check_vma=False,
    )
```

```python
import functools

import jax
import jax.numpy as jnp
from jax import lax
from jax.experimental import pallas as pl
from jax.experimental.pallas import tpu as pltpu
from jax.sharding import PartitionSpec as P


BLOCK = 128
STEPS = 8
WIDTH = STEPS * BLOCK
HALF = WIDTH // 2
SIDE = 4
ARRIVING = 2 * SIDE
NB = 32
GROUP = 16
CHUNK = 256


bf16 = jnp.bfloat16
f32 = jnp.float32


def split(x):
    hi = x.astype(bf16)
    return hi, (x - hi.astype(f32)).astype(bf16)


def dot(a, b, dims=((1,), (0,))):
    return lax.dot_general(a, b, (dims, ((), ())), preferred_element_type=f32)


def dot_split(a, b, dims=((1,), (0,))):
    return dot(a[0], b[0], dims) + dot(a[1], b[0], dims) + dot(a[0], b[1], dims)


def dot_split_128(a, b):
    (ah, al), (bh, bl) = a, b
    return dot(jnp.concatenate([ah, al], 1), jnp.concatenate([bh, bh], 0)) + dot(ah, bl)


def other_half(k):
    return 14 - k + 2 * (k % 2)


def spread(row):
    return jnp.broadcast_to(row, (8, row.shape[1]))


def factor_tile(work_ref):
    tiles = NB // 8
    sub = lax.broadcasted_iota(jnp.int32, (8, 128), 0)
    for base in range(0, BLOCK, NB):
        rows = [
            [work_ref[base + 8 * t : base + 8 * t + 8, h * 128 : h * 128 + 128] for h in range(2)]
            for t in range(tiles)
        ]
        scale = [None] * tiles
        for first in range(0, NB, GROUP):
            last = first + GROUP
            cols = {
                (j, t): jnp.broadcast_to(rows[t][0][:, base + j : base + j + 1], (8, 128))
                for j in range(first, last)
                for t in range(j // 8, tiles)
            }
            for k in range(first, last, 2):
                tk, rk = divmod(k, 8)
                a = spread(cols[k, tk][rk : rk + 1])
                b = spread(cols[k, tk][rk + 1 : rk + 2])
                c = spread(cols[k + 1, tk][rk + 1 : rk + 2])
                det = a * c - b * b
                inv, ra = 1.0 / det, 1.0 / a
                r0, r1 = lax.rsqrt(a), lax.rsqrt(det * ra)
                scale[tk] = r0 if rk == 0 else jnp.where(sub == rk, r0, scale[tk])
                scale[tk] = jnp.where(sub == rk + 1, r1, scale[tk])
                p, q = {}, {}
                for t in range(tk + (rk == 6), tiles):
                    p[t] = c * cols[k, t] - b * cols[k + 1, t]
                    q[t] = a * cols[k + 1, t] - b * cols[k, t]
                pd, qd = {t: v * inv for t, v in p.items()}, {t: v * inv for t, v in q.items()}
                for j in range(k + 2, last):
                    tj, rj = divmod(j, 8)
                    c0 = spread(cols[k, tj][rj : rj + 1])
                    c1 = spread(cols[k + 1, tj][rj : rj + 1])
                    for t in range(tj, tiles):
                        if j < k + 4:
                            cols[j, t] = cols[j, t] - (p[t] * c0 + q[t] * c1) * inv
                        else:
                            cols[j, t] = cols[j, t] - (pd[t] * c0 + qd[t] * c1)
                if tk in pd:
                    pd[tk], qd[tk] = (jnp.where(sub > rk + 1, v[tk], 0.0) for v in (pd, qd))
                second = jnp.where(sub == rk + 1, b * ra, 0.0)
                for h in range(2):
                    s0 = spread(rows[tk][h][rk : rk + 1])
                    s1 = spread(rows[tk][h][rk + 1 : rk + 2])
                    rows[tk][h] = rows[tk][h] - second * s0
                    for t in pd:
                        rows[t][h] = rows[t][h] - (pd[t] * s0 + qd[t] * s1)
                yield
        done = jnp.concatenate(
            [jnp.concatenate([rows[t][h] * scale[t] for h in range(2)], 1) for t in range(tiles)], 0
        )
        end = base + NB
        work_ref[base:end, :] = done
        if end < BLOCK:
            lh, ll = split(jnp.transpose(done[:, :128])[end:])
            uh, ul = split(done)
            left = jnp.concatenate([lh, lh, ll], 1)
            right = jnp.concatenate([uh, ul, uh], 0)
            work_ref[end:, :] = work_ref[end:, :] - dot(left, right)


def factor_kernel(
    place_ref, w_ref, mh_ref, ml_ref, corner_ref,
    x_ref, d_ref, work_ref, inv_ref, left_ref, right_ref, rest_ref, sems,
):
    quarters = x_ref.reshape(2, SIDE, 2, 2, BLOCK // 4, WIDTH)
    first, later = [], []
    for slot in range(2 * STEPS):
        b, k = (0, slot) if slot < STEPS else (1, other_half(slot))
        for side in range(SIDE):
            a, y = (0, side) if side < 2 else (1, SIDE - 1 - side)
            dst = quarters.at[y, :, b, a, :, k * BLOCK : (k + 1) * BLOCK]
            copy = pltpu.make_async_copy(w_ref.at[slot, side], dst, sems.at[slot * SIDE + side])
            (first if y == 0 and k == 0 else later).append(copy)
    for copy in first + later:
        copy.start()
    for copy in first:
        copy.wait()
    r = lax.broadcasted_iota(jnp.int32, (BLOCK, BLOCK), 0)
    c = lax.broadcasted_iota(jnp.int32, (BLOCK, BLOCK), 1)
    work_ref[:, :BLOCK] = x_ref[:BLOCK, :BLOCK]

    def finish_row(k, b):
        here, at = pl.ds(pl.multiple_of(k * BLOCK, BLOCK), BLOCK), slice(b * BLOCK, (b + 1) * BLOCK)
        old, inverse = x_ref[here, at], inv_ref[...]
        new = jnp.where(k == b, inverse, dot_split_128(split(inverse), split(old)))
        x_ref[here, at] = new
        hi, lo = split(new)
        right_ref[:BLOCK, at], rest_ref[:, at] = hi, lo
        mh_ref[here, at] = jnp.where(b <= k, hi, jnp.zeros_like(hi))
        ml_ref[here, at] = jnp.where(b <= k, lo, jnp.zeros_like(lo))
        right_ref[BLOCK:, at] = hi
        left_ref[at, :BLOCK], left_ref[at, BLOCK:] = split(jnp.where(b > k, jnp.transpose(new), 0.0))

    def clear(k):
        here = pl.ds(pl.multiple_of(k * BLOCK, BLOCK), BLOCK)
        block = lax.broadcasted_iota(jnp.int32, (WIDTH, BLOCK), 0) // BLOCK
        x_ref[:, here] = jnp.where(block > k, 0.0, x_ref[:, here])

    def trail(m, n):
        at, to = slice(m * BLOCK, (m + 1) * BLOCK), slice(n * 2 * BLOCK, (n + 1) * 2 * BLOCK)
        product = dot(left_ref[at, :], right_ref[:, to]) + dot(left_ref[at, :BLOCK], rest_ref[:, to])
        x_ref[at, to] = x_ref[at, to] - product

    def factor_block(others):
        work_ref[:, BLOCK:] = jnp.where(r == c, 1.0, 0.0).astype(f32)
        emitted = 0
        for place, _ in enumerate(factor_tile(work_ref)):
            until = -(-len(others) * (place + 1) // (BLOCK // 2))
            for other in others[emitted:until]:
                other()
            emitted = until

    def prepare(k):
        here = pl.ds(pl.multiple_of(k * BLOCK, BLOCK), BLOCK)
        after = pl.ds(pl.multiple_of(jnp.minimum(k + 1, STEPS - 1) * BLOCK, BLOCK), BLOCK)
        d_ref[here, :] = jnp.where(r <= c, work_ref[:, :BLOCK], 0.0)
        inverse = work_ref[:, BLOCK:]
        inv_ref[...] = inverse
        u = dot_split_128(split(inverse), split(x_ref[here, after]))
        work_ref[:, :BLOCK] = x_ref[after, after] - dot_split_128(split(jnp.transpose(u)), split(u))

    def step(k, _, lowest=1):
        others = [functools.partial(finish_row, k - 1, b) for b in range(STEPS)]
        others += [functools.partial(clear, k - 1)]
        others += [functools.partial(trail, m, n) for n in range(STEPS // 2) for m in range(lowest, STEPS)]
        factor_block(others)
        prepare(k)
        return 0

    factor_block([])
    for copy in later:
        copy.wait()
    prepare(0)
    lax.fori_loop(1, STEPS // 2, step, 0)
    lax.fori_loop(STEPS // 2, STEPS, functools.partial(step, lowest=STEPS // 2), 0)
    end = slice(WIDTH - BLOCK, WIDTH)
    x_ref[end, :] = dot_split_128(split(inv_ref[...]), split(x_ref[end, :]))
    x_ref[end, end] = inv_ref[...]
    mh_ref[end, :], ml_ref[end, :] = split(x_ref[end, :])
    row, col = place_ref[0], place_ref[1]
    mine = pl.ds(pl.multiple_of(jnp.minimum(row, STEPS - 1) * BLOCK, BLOCK), BLOCK)
    other = pl.ds(pl.multiple_of(jnp.minimum(col, STEPS - 1) * BLOCK, BLOCK), BLOCK)
    block = jnp.where(row == col, d_ref[mine, :], x_ref[other, mine])
    corner_ref[...] = jnp.where(row >= col, jnp.transpose(block), 0.0)


def factor(place, gathered):
    vmem, hbm = pl.BlockSpec(memory_space=pltpu.VMEM), pl.BlockSpec(memory_space=pltpu.HBM)
    return pl.pallas_call(
        factor_kernel,
        in_specs=[pl.BlockSpec(memory_space=pltpu.SMEM), hbm],
        out_specs=(vmem, vmem, vmem),
        out_shape=(
            jax.ShapeDtypeStruct((WIDTH, WIDTH), bf16),
            jax.ShapeDtypeStruct((WIDTH, WIDTH), bf16),
            jax.ShapeDtypeStruct((BLOCK, BLOCK), f32),
        ),
        scratch_shapes=[
            pltpu.VMEM((WIDTH, WIDTH), f32),
            pltpu.VMEM((WIDTH, BLOCK), f32),
            pltpu.VMEM((BLOCK, 2 * BLOCK), f32),
            pltpu.VMEM((BLOCK, BLOCK), f32),
            pltpu.VMEM((WIDTH, 2 * BLOCK), bf16),
            pltpu.VMEM((2 * BLOCK, WIDTH), bf16),
            pltpu.VMEM((BLOCK, WIDTH), bf16),
            pltpu.SemaphoreType.DMA((2 * STEPS * SIDE,)),
        ],
        compiler_params=pltpu.CompilerParams(vmem_limit_bytes=24 * 2**20),
        cost_estimate=pl.CostEstimate(flops=40_000_000_000, bytes_accessed=2**23, transcendentals=0),
        name="factor",
    )(place, gathered)


def apply_kernel(place_ref, mh, ml, corner_ref, *refs):
    v_hbm, outs, (vh, vl, pair_ref, four_ref, sems) = refs[:ARRIVING], refs[ARRIVING : ARRIVING + 3], refs[ARRIVING + 3 :]
    count = iter(range(sems.shape[0]))
    copy = lambda src, dst: pltpu.make_async_copy(src, dst, sems.at[next(count)])
    arriving = [copy(v, pair_ref.at[d]) for d, v in enumerate(v_hbm[:SIDE])]
    for c in arriving:
        c.start()
    row, col = place_ref[0], place_ref[1]
    near = [copy(v, four_ref.at[e]) for e, v in enumerate(v_hbm[SIDE : SIDE + 2])]
    far = [pltpu.make_async_copy(v, four_ref.at[e], sems.at[SIDE + e]) for e, v in enumerate(v_hbm[SIDE + 2 :])]
    arriving += near

    @pl.when(row < 2 * SIDE)
    def _():
        for c in near:
            c.start()

    @pl.when(row >= 2 * SIDE)
    def _():
        for c in far:
            c.start()

    other = pl.ds(pl.multiple_of(jnp.minimum(col, STEPS - 1) * BLOCK, BLOCK), BLOCK)
    sent = [copy(corner_ref, outs[2])]
    sent[0].start()
    my_y, my_x = row // SIDE, row % SIDE
    swapped = jnp.where((my_y == 1) | (my_y == 2), 1, 0)
    half = BLOCK // 2
    for n, c in enumerate(arriving):
        c.wait()
        for m in range(2 if n < SIDE else SIDE):
            d, e = (n, m) if n < SIDE else (m, n - SIDE)
            v_ref = pair_ref.at[d] if n < SIDE else four_ref.at[e]
            block = SIDE * (e + swapped - 2 * e * swapped) + (my_x + d) % SIDE
            at = pl.ds(pl.multiple_of(block * BLOCK + half * (n >= SIDE), half), half)
            vh[at], vl[at] = split(v_ref[m * half : (m + 1) * half])
    for k in reversed(range(0, WIDTH, CHUNK)):
        at, upto = slice(k, k + CHUNK), slice(0, k + CHUNK)
        vh[at], vl[at] = split(dot_split((mh[at, upto], ml[at, upto]), (vh[upto], vl[upto])))
    for k in range(0, WIDTH, CHUNK):
        at, on = slice(k, k + CHUNK), slice(k, WIDTH)
        vh[at], vl[at] = split(dot_split((mh[on, at], ml[on, at]), (vh[on], vl[on]), ((0,), (0,))))
        for v, m in ((vh, mh), (vl, ml)):
            panel = jnp.transpose(m[other, at].astype(f32)).astype(bf16)
            v[at, :BLOCK] = jnp.where(col < STEPS, panel, v[at, :BLOCK])
        for v, out in zip((vh, vl), outs):
            sent.append(copy(v.at[at], out.at[at]))
            sent[-1].start()
    for c in sent:
        c.wait()


def apply(place, mh, ml, corner, across):
    vmem, hbm = pl.BlockSpec(memory_space=pltpu.VMEM), pl.BlockSpec(memory_space=pltpu.HBM)
    square = pltpu.VMEM((WIDTH, WIDTH), bf16)
    return pl.pallas_call(
        apply_kernel,
        in_specs=[pl.BlockSpec(memory_space=pltpu.SMEM), vmem, vmem, vmem] + [hbm] * ARRIVING,
        out_specs=(hbm,) * 3,
        out_shape=(pltpu.HBM((WIDTH, WIDTH), bf16), pltpu.HBM((WIDTH, WIDTH), bf16), pltpu.HBM((BLOCK, BLOCK), f32)),
        scratch_shapes=[square, square]
        + [
            pltpu.VMEM((SIDE, BLOCK, WIDTH), f32),
            pltpu.VMEM((2, 2 * BLOCK, WIDTH), f32),
            pltpu.SemaphoreType.DMA((ARRIVING + 1 + 2 * (WIDTH // CHUNK),)),
        ],
        compiler_params=pltpu.CompilerParams(vmem_limit_bytes=20 * 2**20),
        cost_estimate=pl.CostEstimate(flops=10_000_000_000, bytes_accessed=2**23, transcendentals=0),
        name="apply",
    )(place, mh, ml, corner, *across)


def update_kernel(place_ref, a_ref, u_ref, yh_ref, yl_ref, corner_ref, out_ref):
    row, col, step = place_ref[0], place_ref[1], pl.program_id(0)
    slots = [jnp.where(step < HALF // CHUNK, j, other_half(j) - STEPS) for j in range(STEPS)]
    u = split(jnp.concatenate([u_ref[s] for s in slots], 1))
    product = dot_split(u, (yh_ref[...], yl_ref[...]))
    out_ref[:, :BLOCK] = jnp.where(col < STEPS, product[:, :BLOCK], a_ref[:, :BLOCK] - product[:, :BLOCK])
    out_ref[:, BLOCK:] = a_ref[:, BLOCK:] - product[:, BLOCK:]

    @pl.when((step == 0) & (row < STEPS))
    def _():
        out_ref[:BLOCK, :] = jnp.zeros((BLOCK, WIDTH), f32)

        @pl.when(col < STEPS)
        def _():
            out_ref[:BLOCK, :BLOCK] = corner_ref[...]


def update(place, blocked, gathered, yh, yl, corner):
    per_half = HALF // CHUNK
    whole = lambda *shape: pl.BlockSpec(shape, lambda i: (0, 0))
    return pl.pallas_call(
        update_kernel,
        grid=(WIDTH // CHUNK,),
        in_specs=[
            pl.BlockSpec(memory_space=pltpu.SMEM),
            pl.BlockSpec((CHUNK, WIDTH), lambda i: (i, 0)),
            pl.BlockSpec((STEPS, CHUNK, BLOCK), lambda i: (i // per_half, i % per_half, 0)),
            whole(WIDTH, WIDTH),
            whole(WIDTH, WIDTH),
            whole(BLOCK, BLOCK),
        ],
        out_specs=pl.BlockSpec((CHUNK, WIDTH), lambda i: (i, 0)),
        out_shape=jax.ShapeDtypeStruct((WIDTH, WIDTH), f32),
        compiler_params=pltpu.CompilerParams(vmem_limit_bytes=28 * 2**20),
        name="update",
    )(place, blocked, gathered, yh, yl, corner)


def per_device(blocked):
    rows, cols = lax.axis_size("prow"), lax.axis_size("pcol")
    row, col = lax.axis_index("prow"), lax.axis_index("pcol")
    span = range(STEPS)
    in_hbm = lambda a: pltpu.with_memory_space_constraint(a, pltpu.HBM)

    quarter = BLOCK // 4
    corner = blocked[:BLOCK, :BLOCK]
    parts = []
    for b, a in ((1, 1), (1, 0), (0, 1)):
        pairs = []
        for i in span:
            to_row = (SIDE - 1 - i // SIDE) * SIDE + i % SIDE if a else i
            for k in span:
                pairs.append((i * cols + k, to_row * cols + (other_half(k) if b else k)))
        at = (2 * b + a) * quarter
        parts.append(lax.ppermute(corner[at : at + quarter], ("prow", "pcol"), pairs))
    stays = (row < STEPS) & (col < STEPS)
    part = jnp.where(stays, corner[:quarter], parts[0] + parts[1] + parts[2])
    lower = lax.ppermute(blocked[HALF:, :BLOCK], "pcol", [(k, other_half(k)) for k in span])
    strip = lax.all_to_all(jnp.broadcast_to(part, (rows, quarter, BLOCK)), "prow", 0, 0)
    window = lax.all_gather(strip.reshape(HALF, BLOCK), "pcol", axis=0)
    window = window.reshape(cols, SIDE, SIDE, quarter, BLOCK)
    payload = jnp.where(col < STEPS, blocked[:HALF, :BLOCK], lower)

    upper, under = blocked[: BLOCK // 2], blocked[BLOCK // 2 : BLOCK]
    source = row < 2 * SIDE
    moves = ([(0, 1), (1, 0)], [(0, 3), (1, 2)], [(0, 2), (1, 3)])

    def along_y(piece):
        got = []
        for move in moves:
            pairs = [(a * SIDE + x, b * SIDE + x) for a, b in move for x in range(SIDE)]
            got.append(lax.ppermute(piece, "prow", pairs))
        return [piece] + got

    def along_x(piece, sides):
        got = [piece]
        for d in range(1, SIDE):
            pairs = [(y * SIDE + (x + d) % SIDE, y * SIDE + x) for y in range(sides) for x in range(SIDE)]
            got.append(lax.ppermute(piece, "prow", pairs))
        return got

    here, first, second, third = along_y(upper)
    pair = jnp.concatenate([jnp.where(source, here, second), jnp.where(source, first, third)], 0)
    four = jnp.concatenate(along_x(under, 2), 0)
    payload, window, _, _ = lax.optimization_barrier((payload, window, pair, four))
    panels = lax.all_gather(payload, "pcol", axis=0)
    across = along_x(pair, SIDE) + along_y(four)

    place = jnp.stack([row, col])
    mh, ml, corner = factor(place, in_hbm(window))
    applied = apply(place, mh, ml, corner, across)
    return update(place, *(in_hbm(v) for v in (blocked, panels, *applied)))


def solution(mesh):
    return jax.shard_map(
        per_device,
        mesh=mesh,
        in_specs=(P("prow", "pcol"),),
        out_specs=P("prow", "pcol"),
        check_vma=False,
    )
```

```python
import functools

import jax
import jax.numpy as jnp
from jax import lax
from jax.experimental import pallas as pl
from jax.experimental.pallas import tpu as pltpu
from jax.sharding import PartitionSpec as P


BLOCK = 128
STEPS = 8
WIDTH = STEPS * BLOCK
HALF = WIDTH // 2
SIDE = 4
NB = 32
GROUP = 16
CHUNK = 256


bf16 = jnp.bfloat16
f32 = jnp.float32


def split(x):
    hi = x.astype(bf16)
    return hi, (x - hi.astype(f32)).astype(bf16)


def dot(a, b, dims=((1,), (0,))):
    return lax.dot_general(a, b, (dims, ((), ())), preferred_element_type=f32)


def dot_split(a, b, dims=((1,), (0,))):
    return dot(a[0], b[0], dims) + dot(a[1], b[0], dims) + dot(a[0], b[1], dims)


def dot_split_128(a, b):
    (ah, al), (bh, bl) = a, b
    return dot(jnp.concatenate([ah, al], 1), jnp.concatenate([bh, bh], 0)) + dot(ah, bl)


def other_half(k):
    return 14 - k + 2 * (k % 2)


def spread(row):
    return jnp.broadcast_to(row, (8, row.shape[1]))


def factor_tile(work_ref):
    tiles = NB // 8
    sub = lax.broadcasted_iota(jnp.int32, (8, 128), 0)
    for base in range(0, BLOCK, NB):
        rows = [
            [work_ref[base + 8 * t : base + 8 * t + 8, h * 128 : h * 128 + 128] for h in range(2)]
            for t in range(tiles)
        ]
        scale = [None] * tiles
        for first in range(0, NB, GROUP):
            last = first + GROUP
            cols = {
                (j, t): jnp.broadcast_to(rows[t][0][:, base + j : base + j + 1], (8, 128))
                for j in range(first, last)
                for t in range(j // 8, tiles)
            }
            for k in range(first, last, 2):
                tk, rk = divmod(k, 8)
                a = spread(cols[k, tk][rk : rk + 1])
                b = spread(cols[k, tk][rk + 1 : rk + 2])
                c = spread(cols[k + 1, tk][rk + 1 : rk + 2])
                det = a * c - b * b
                inv, ra = 1.0 / det, 1.0 / a
                r0, r1 = lax.rsqrt(a), lax.rsqrt(det * ra)
                scale[tk] = r0 if rk == 0 else jnp.where(sub == rk, r0, scale[tk])
                scale[tk] = jnp.where(sub == rk + 1, r1, scale[tk])
                p, q = {}, {}
                for t in range(tk + (rk == 6), tiles):
                    p[t] = c * cols[k, t] - b * cols[k + 1, t]
                    q[t] = a * cols[k + 1, t] - b * cols[k, t]
                pd, qd = {t: v * inv for t, v in p.items()}, {t: v * inv for t, v in q.items()}
                for j in range(k + 2, last):
                    tj, rj = divmod(j, 8)
                    c0 = spread(cols[k, tj][rj : rj + 1])
                    c1 = spread(cols[k + 1, tj][rj : rj + 1])
                    for t in range(tj, tiles):
                        if j < k + 4:
                            cols[j, t] = cols[j, t] - (p[t] * c0 + q[t] * c1) * inv
                        else:
                            cols[j, t] = cols[j, t] - (pd[t] * c0 + qd[t] * c1)
                if tk in pd:
                    pd[tk], qd[tk] = (jnp.where(sub > rk + 1, v[tk], 0.0) for v in (pd, qd))
                second = jnp.where(sub == rk + 1, b * ra, 0.0)
                for h in range(2):
                    s0 = spread(rows[tk][h][rk : rk + 1])
                    s1 = spread(rows[tk][h][rk + 1 : rk + 2])
                    rows[tk][h] = rows[tk][h] - second * s0
                    for t in pd:
                        rows[t][h] = rows[t][h] - (pd[t] * s0 + qd[t] * s1)
                yield
        done = jnp.concatenate(
            [jnp.concatenate([rows[t][h] * scale[t] for h in range(2)], 1) for t in range(tiles)], 0
        )
        end = base + NB
        work_ref[base:end, :] = done
        if end < BLOCK:
            lh, ll = split(jnp.transpose(done[:, :128])[end:])
            uh, ul = split(done)
            left = jnp.concatenate([lh, lh, ll], 1)
            right = jnp.concatenate([uh, ul, uh], 0)
            work_ref[end:, :] = work_ref[end:, :] - dot(left, right)


def factor_kernel(
    place_ref, w_ref, mh_ref, ml_ref, corner_ref,
    x_ref, d_ref, work_ref, inv_ref, left_ref, right_ref, rest_ref, sems,
):
    quarters = x_ref.reshape(2, SIDE, 2, 2, BLOCK // 4, WIDTH)
    first, later = [], []
    for slot in range(2 * STEPS):
        b, k = (0, slot) if slot < STEPS else (1, other_half(slot))
        for side in range(SIDE):
            a, y = (0, side) if side < 2 else (1, SIDE - 1 - side)
            dst = quarters.at[y, :, b, a, :, k * BLOCK : (k + 1) * BLOCK]
            copy = pltpu.make_async_copy(w_ref.at[slot, side], dst, sems.at[slot * SIDE + side])
            (first if y == 0 and k == 0 else later).append(copy)
    for copy in first + later:
        copy.start()
    for copy in first:
        copy.wait()
    r = lax.broadcasted_iota(jnp.int32, (BLOCK, BLOCK), 0)
    c = lax.broadcasted_iota(jnp.int32, (BLOCK, BLOCK), 1)
    work_ref[:, :BLOCK] = x_ref[:BLOCK, :BLOCK]

    def finish_row(k, b):
        here, at = pl.ds(pl.multiple_of(k * BLOCK, BLOCK), BLOCK), slice(b * BLOCK, (b + 1) * BLOCK)
        old, inverse = x_ref[here, at], inv_ref[...]
        new = jnp.where(k == b, inverse, dot_split_128(split(inverse), split(old)))
        x_ref[here, at] = new
        hi, lo = split(new)
        right_ref[:BLOCK, at], rest_ref[:, at] = hi, lo
        mh_ref[here, at] = jnp.where(b <= k, hi, jnp.zeros_like(hi))
        ml_ref[here, at] = jnp.where(b <= k, lo, jnp.zeros_like(lo))
        right_ref[BLOCK:, at] = hi
        left_ref[at, :BLOCK], left_ref[at, BLOCK:] = split(jnp.where(b > k, jnp.transpose(new), 0.0))

    def clear(k):
        here = pl.ds(pl.multiple_of(k * BLOCK, BLOCK), BLOCK)
        block = lax.broadcasted_iota(jnp.int32, (WIDTH, BLOCK), 0) // BLOCK
        x_ref[:, here] = jnp.where(block > k, 0.0, x_ref[:, here])

    def trail(m, n):
        at, to = slice(m * BLOCK, (m + 1) * BLOCK), slice(n * 2 * BLOCK, (n + 1) * 2 * BLOCK)
        product = dot(left_ref[at, :], right_ref[:, to]) + dot(left_ref[at, :BLOCK], rest_ref[:, to])
        x_ref[at, to] = x_ref[at, to] - product

    def factor_block(others):
        work_ref[:, BLOCK:] = jnp.where(r == c, 1.0, 0.0).astype(f32)
        emitted = 0
        for place, _ in enumerate(factor_tile(work_ref)):
            until = -(-len(others) * (place + 1) // (BLOCK // 2))
            for other in others[emitted:until]:
                other()
            emitted = until

    def prepare(k):
        here = pl.ds(pl.multiple_of(k * BLOCK, BLOCK), BLOCK)
        after = pl.ds(pl.multiple_of(jnp.minimum(k + 1, STEPS - 1) * BLOCK, BLOCK), BLOCK)
        d_ref[here, :] = jnp.where(r <= c, work_ref[:, :BLOCK], 0.0)
        inverse = work_ref[:, BLOCK:]
        inv_ref[...] = inverse
        u = dot_split_128(split(inverse), split(x_ref[here, after]))
        work_ref[:, :BLOCK] = x_ref[after, after] - dot_split_128(split(jnp.transpose(u)), split(u))

    def step(k, _, lowest=1):
        others = [functools.partial(finish_row, k - 1, b) for b in range(STEPS)]
        others += [functools.partial(clear, k - 1)]
        others += [functools.partial(trail, m, n) for n in range(STEPS // 2) for m in range(lowest, STEPS)]
        factor_block(others)
        prepare(k)
        return 0

    factor_block([])
    for copy in later:
        copy.wait()
    prepare(0)
    lax.fori_loop(1, STEPS // 2, step, 0)
    lax.fori_loop(STEPS // 2, STEPS, functools.partial(step, lowest=STEPS // 2), 0)
    end = slice(WIDTH - BLOCK, WIDTH)
    x_ref[end, :] = dot_split_128(split(inv_ref[...]), split(x_ref[end, :]))
    x_ref[end, end] = inv_ref[...]
    mh_ref[end, :], ml_ref[end, :] = split(x_ref[end, :])
    row, col = place_ref[0], place_ref[1]
    mine = pl.ds(pl.multiple_of(jnp.minimum(row, STEPS - 1) * BLOCK, BLOCK), BLOCK)
    other = pl.ds(pl.multiple_of(jnp.minimum(col, STEPS - 1) * BLOCK, BLOCK), BLOCK)
    block = jnp.where(row == col, d_ref[mine, :], x_ref[other, mine])
    corner_ref[...] = jnp.where(row >= col, jnp.transpose(block), 0.0)


def factor(place, gathered):
    vmem, hbm = pl.BlockSpec(memory_space=pltpu.VMEM), pl.BlockSpec(memory_space=pltpu.HBM)
    return pl.pallas_call(
        factor_kernel,
        in_specs=[pl.BlockSpec(memory_space=pltpu.SMEM), hbm],
        out_specs=(vmem, vmem, vmem),
        out_shape=(
            jax.ShapeDtypeStruct((WIDTH, WIDTH), bf16),
            jax.ShapeDtypeStruct((WIDTH, WIDTH), bf16),
            jax.ShapeDtypeStruct((BLOCK, BLOCK), f32),
        ),
        scratch_shapes=[
            pltpu.VMEM((WIDTH, WIDTH), f32),
            pltpu.VMEM((WIDTH, BLOCK), f32),
            pltpu.VMEM((BLOCK, 2 * BLOCK), f32),
            pltpu.VMEM((BLOCK, BLOCK), f32),
            pltpu.VMEM((WIDTH, 2 * BLOCK), bf16),
            pltpu.VMEM((2 * BLOCK, WIDTH), bf16),
            pltpu.VMEM((BLOCK, WIDTH), bf16),
            pltpu.SemaphoreType.DMA((2 * STEPS * SIDE,)),
        ],
        compiler_params=pltpu.CompilerParams(vmem_limit_bytes=24 * 2**20),
        cost_estimate=pl.CostEstimate(flops=40_000_000_000, bytes_accessed=2**23, transcendentals=0),
        name="factor",
    )(place, gathered)


def apply_kernel(place_ref, mh, ml, corner_ref, *refs):
    v_hbm, outs, (vh, vl, v_ref, sems) = refs[:SIDE], refs[SIDE : SIDE + 3], refs[SIDE + 3 :]
    count = iter(range(sems.shape[0]))
    copy = lambda src, dst: pltpu.make_async_copy(src, dst, sems.at[next(count)])
    arriving = [copy(v, v_ref.at[d]) for d, v in enumerate(v_hbm)]
    for c in arriving:
        c.start()
    row, col = place_ref[0], place_ref[1]
    other = pl.ds(pl.multiple_of(jnp.minimum(col, STEPS - 1) * BLOCK, BLOCK), BLOCK)
    sent = [copy(corner_ref, outs[2])]
    sent[0].start()
    my_y, my_x = row // SIDE, row % SIDE
    swapped = jnp.where((my_y == 1) | (my_y == 2), 1, 0)
    for d in range(SIDE):
        arriving[d].wait()
        for e in range(2):
            block = SIDE * (e + swapped - 2 * e * swapped) + (my_x + d) % SIDE
            at = pl.ds(pl.multiple_of(block * BLOCK, BLOCK), BLOCK)
            vh[at], vl[at] = split(v_ref[d, e * BLOCK : (e + 1) * BLOCK])
    for k in reversed(range(0, WIDTH, CHUNK)):
        at, upto = slice(k, k + CHUNK), slice(0, k + CHUNK)
        vh[at], vl[at] = split(dot_split((mh[at, upto], ml[at, upto]), (vh[upto], vl[upto])))
    for k in range(0, WIDTH, CHUNK):
        at, on = slice(k, k + CHUNK), slice(k, WIDTH)
        vh[at], vl[at] = split(dot_split((mh[on, at], ml[on, at]), (vh[on], vl[on]), ((0,), (0,))))
        for v, m in ((vh, mh), (vl, ml)):
            panel = jnp.transpose(m[other, at].astype(f32)).astype(bf16)
            v[at, :BLOCK] = jnp.where(col < STEPS, panel, v[at, :BLOCK])
        for v, out in zip((vh, vl), outs):
            sent.append(copy(v.at[at], out.at[at]))
            sent[-1].start()
    for c in sent:
        c.wait()


def apply(place, mh, ml, corner, across):
    vmem, hbm = pl.BlockSpec(memory_space=pltpu.VMEM), pl.BlockSpec(memory_space=pltpu.HBM)
    square = pltpu.VMEM((WIDTH, WIDTH), bf16)
    return pl.pallas_call(
        apply_kernel,
        in_specs=[pl.BlockSpec(memory_space=pltpu.SMEM), vmem, vmem, vmem] + [hbm] * SIDE,
        out_specs=(hbm,) * 3,
        out_shape=(pltpu.HBM((WIDTH, WIDTH), bf16), pltpu.HBM((WIDTH, WIDTH), bf16), pltpu.HBM((BLOCK, BLOCK), f32)),
        scratch_shapes=[square, square]
        + [
            pltpu.VMEM((SIDE, 2 * BLOCK, WIDTH), f32),
            pltpu.SemaphoreType.DMA((SIDE + 1 + 2 * (WIDTH // CHUNK),)),
        ],
        compiler_params=pltpu.CompilerParams(vmem_limit_bytes=20 * 2**20),
        cost_estimate=pl.CostEstimate(flops=10_000_000_000, bytes_accessed=2**23, transcendentals=0),
        name="apply",
    )(place, mh, ml, corner, *across)


def update_kernel(place_ref, a_ref, u_ref, yh_ref, yl_ref, corner_ref, out_ref):
    row, col, step = place_ref[0], place_ref[1], pl.program_id(0)
    slots = [jnp.where(step < HALF // CHUNK, j, other_half(j) - STEPS) for j in range(STEPS)]
    u = split(jnp.concatenate([u_ref[s] for s in slots], 1))
    product = dot_split(u, (yh_ref[...], yl_ref[...]))
    out_ref[:, :BLOCK] = jnp.where(col < STEPS, product[:, :BLOCK], a_ref[:, :BLOCK] - product[:, :BLOCK])
    out_ref[:, BLOCK:] = a_ref[:, BLOCK:] - product[:, BLOCK:]

    @pl.when((step == 0) & (row < STEPS))
    def _():
        out_ref[:BLOCK, :] = jnp.zeros((BLOCK, WIDTH), f32)

        @pl.when(col < STEPS)
        def _():
            out_ref[:BLOCK, :BLOCK] = corner_ref[...]


def update(place, blocked, gathered, yh, yl, corner):
    per_half = HALF // CHUNK
    whole = lambda *shape: pl.BlockSpec(shape, lambda i: (0, 0))
    return pl.pallas_call(
        update_kernel,
        grid=(WIDTH // CHUNK,),
        in_specs=[
            pl.BlockSpec(memory_space=pltpu.SMEM),
            pl.BlockSpec((CHUNK, WIDTH), lambda i: (i, 0)),
            pl.BlockSpec((STEPS, CHUNK, BLOCK), lambda i: (i // per_half, i % per_half, 0)),
            whole(WIDTH, WIDTH),
            whole(WIDTH, WIDTH),
            whole(BLOCK, BLOCK),
        ],
        out_specs=pl.BlockSpec((CHUNK, WIDTH), lambda i: (i, 0)),
        out_shape=jax.ShapeDtypeStruct((WIDTH, WIDTH), f32),
        compiler_params=pltpu.CompilerParams(vmem_limit_bytes=28 * 2**20),
        name="update",
    )(place, blocked, gathered, yh, yl, corner)


def per_device(blocked):
    rows, cols = lax.axis_size("prow"), lax.axis_size("pcol")
    row, col = lax.axis_index("prow"), lax.axis_index("pcol")
    span = range(STEPS)
    in_hbm = lambda a: pltpu.with_memory_space_constraint(a, pltpu.HBM)

    quarter = BLOCK // 4
    corner = blocked[:BLOCK, :BLOCK]
    parts = []
    for b, a in ((1, 1), (1, 0), (0, 1)):
        pairs = []
        for i in span:
            to_row = (SIDE - 1 - i // SIDE) * SIDE + i % SIDE if a else i
            for k in span:
                pairs.append((i * cols + k, to_row * cols + (other_half(k) if b else k)))
        at = (2 * b + a) * quarter
        parts.append(lax.ppermute(corner[at : at + quarter], ("prow", "pcol"), pairs))
    stays = (row < STEPS) & (col < STEPS)
    part = jnp.where(stays, corner[:quarter], parts[0] + parts[1] + parts[2])
    lower = lax.ppermute(blocked[HALF:, :BLOCK], "pcol", [(k, other_half(k)) for k in span])
    strip = lax.all_to_all(jnp.broadcast_to(part, (rows, quarter, BLOCK)), "prow", 0, 0)
    window = lax.all_gather(strip.reshape(HALF, BLOCK), "pcol", axis=0)
    window = window.reshape(cols, SIDE, SIDE, quarter, BLOCK)
    payload = jnp.where(col < STEPS, blocked[:HALF, :BLOCK], lower)

    own = blocked[:BLOCK]
    moves = ([(0, 1), (1, 0)], [(0, 3), (1, 2)], [(0, 2), (1, 3)])
    got = [
        lax.ppermute(own, "prow", [(a * SIDE + x, b * SIDE + x) for a, b in move for x in range(SIDE)])
        for move in moves
    ]
    source = row < 2 * SIDE
    pair = jnp.concatenate([jnp.where(source, own, got[1]), jnp.where(source, got[0], got[2])], 0)
    payload, window, _ = lax.optimization_barrier((payload, window, pair))
    panels = lax.all_gather(payload, "pcol", axis=0)
    across = [pair]
    for d in range(1, SIDE):
        across.append(lax.ppermute(pair, "prow", [(r // SIDE * SIDE + (r + d) % SIDE, r) for r in range(rows)]))

    place = jnp.stack([row, col])
    mh, ml, corner = factor(place, in_hbm(window))
    applied = apply(place, mh, ml, corner, across)
    return update(place, *(in_hbm(v) for v in (blocked, panels, *applied)))


def solution(mesh):
    return jax.shard_map(
        per_device,
        mesh=mesh,
        in_specs=(P("prow", "pcol"),),
        out_specs=P("prow", "pcol"),
        check_vma=False,
    )
```

```python
import functools

import jax
import jax.numpy as jnp
from jax import lax
from jax.experimental import pallas as pl
from jax.experimental.pallas import tpu as pltpu
from jax.sharding import PartitionSpec as P


BLOCK = 128
STEPS = 8
WIDTH = STEPS * BLOCK
HALF = WIDTH // 2
SIDE = 4
NB = 32
GROUP = 16
CHUNK = 256


bf16 = jnp.bfloat16
f32 = jnp.float32


def split(x):
    hi = x.astype(bf16)
    return hi, (x - hi.astype(f32)).astype(bf16)


def dot(a, b, dims=((1,), (0,))):
    return lax.dot_general(a, b, (dims, ((), ())), preferred_element_type=f32)


def dot_split(a, b, dims=((1,), (0,))):
    return dot(a[0], b[0], dims) + dot(a[1], b[0], dims) + dot(a[0], b[1], dims)


def dot_split_128(a, b):
    (ah, al), (bh, bl) = a, b
    return dot(jnp.concatenate([ah, al], 1), jnp.concatenate([bh, bh], 0)) + dot(ah, bl)


def other_half(k):
    return 14 - k + 2 * (k % 2)


def spread(row):
    return jnp.broadcast_to(row, (8, row.shape[1]))


def factor_tile(work_ref):
    tiles = NB // 8
    sub = lax.broadcasted_iota(jnp.int32, (8, 128), 0)
    for base in range(0, BLOCK, NB):
        rows = [
            [work_ref[base + 8 * t : base + 8 * t + 8, h * 128 : h * 128 + 128] for h in range(2)]
            for t in range(tiles)
        ]
        scale = [None] * tiles
        for first in range(0, NB, GROUP):
            last = first + GROUP
            cols = {
                (j, t): jnp.broadcast_to(rows[t][0][:, base + j : base + j + 1], (8, 128))
                for j in range(first, last)
                for t in range(j // 8, tiles)
            }
            for k in range(first, last, 2):
                tk, rk = divmod(k, 8)
                a = spread(cols[k, tk][rk : rk + 1])
                b = spread(cols[k, tk][rk + 1 : rk + 2])
                c = spread(cols[k + 1, tk][rk + 1 : rk + 2])
                det = a * c - b * b
                inv, ra = 1.0 / det, 1.0 / a
                r0, r1 = lax.rsqrt(a), lax.rsqrt(det * ra)
                scale[tk] = r0 if rk == 0 else jnp.where(sub == rk, r0, scale[tk])
                scale[tk] = jnp.where(sub == rk + 1, r1, scale[tk])
                p, q = {}, {}
                for t in range(tk + (rk == 6), tiles):
                    p[t] = c * cols[k, t] - b * cols[k + 1, t]
                    q[t] = a * cols[k + 1, t] - b * cols[k, t]
                pd, qd = {t: v * inv for t, v in p.items()}, {t: v * inv for t, v in q.items()}
                for j in range(k + 2, last):
                    tj, rj = divmod(j, 8)
                    c0 = spread(cols[k, tj][rj : rj + 1])
                    c1 = spread(cols[k + 1, tj][rj : rj + 1])
                    for t in range(tj, tiles):
                        if j < k + 4:
                            cols[j, t] = cols[j, t] - (p[t] * c0 + q[t] * c1) * inv
                        else:
                            cols[j, t] = cols[j, t] - (pd[t] * c0 + qd[t] * c1)
                if tk in pd:
                    pd[tk], qd[tk] = (jnp.where(sub > rk + 1, v[tk], 0.0) for v in (pd, qd))
                second = jnp.where(sub == rk + 1, b * ra, 0.0)
                for h in range(2):
                    s0 = spread(rows[tk][h][rk : rk + 1])
                    s1 = spread(rows[tk][h][rk + 1 : rk + 2])
                    rows[tk][h] = rows[tk][h] - second * s0
                    for t in pd:
                        rows[t][h] = rows[t][h] - (pd[t] * s0 + qd[t] * s1)
                yield
        done = jnp.concatenate(
            [jnp.concatenate([rows[t][h] * scale[t] for h in range(2)], 1) for t in range(tiles)], 0
        )
        end = base + NB
        work_ref[base:end, :] = done
        if end < BLOCK:
            lh, ll = split(jnp.transpose(done[:, :128])[end:])
            uh, ul = split(done)
            left = jnp.concatenate([lh, lh, ll], 1)
            right = jnp.concatenate([uh, ul, uh], 0)
            work_ref[end:, :] = work_ref[end:, :] - dot(left, right)


def factor_kernel(
    place_ref, w_ref, mh_ref, ml_ref, corner_ref,
    x_ref, d_ref, work_ref, inv_ref, left_ref, right_ref, rest_ref, sems,
):
    quarters = x_ref.reshape(2, SIDE, 2, 2, BLOCK // 4, WIDTH)
    first, later = [], []
    for slot in range(2 * STEPS):
        b, k = (0, slot) if slot < STEPS else (1, other_half(slot))
        for side in range(SIDE):
            a, y = (0, side) if side < 2 else (1, SIDE - 1 - side)
            dst = quarters.at[y, :, b, a, :, k * BLOCK : (k + 1) * BLOCK]
            copy = pltpu.make_async_copy(w_ref.at[slot, side], dst, sems.at[slot * SIDE + side])
            (first if y == 0 and k == 0 else later).append(copy)
    for copy in first + later:
        copy.start()
    for copy in first:
        copy.wait()
    r = lax.broadcasted_iota(jnp.int32, (BLOCK, BLOCK), 0)
    c = lax.broadcasted_iota(jnp.int32, (BLOCK, BLOCK), 1)
    work_ref[:, :BLOCK] = x_ref[:BLOCK, :BLOCK]

    def finish_row(k, b):
        here, at = pl.ds(pl.multiple_of(k * BLOCK, BLOCK), BLOCK), slice(b * BLOCK, (b + 1) * BLOCK)
        old, inverse = x_ref[here, at], inv_ref[...]
        new = jnp.where(k == b, inverse, dot_split_128(split(inverse), split(old)))
        x_ref[here, at] = new
        hi, lo = split(new)
        right_ref[:BLOCK, at], rest_ref[:, at] = hi, lo
        mh_ref[here, at] = jnp.where(b <= k, hi, jnp.zeros_like(hi))
        ml_ref[here, at] = jnp.where(b <= k, lo, jnp.zeros_like(lo))
        right_ref[BLOCK:, at] = hi
        left_ref[at, :BLOCK], left_ref[at, BLOCK:] = split(jnp.where(b > k, jnp.transpose(new), 0.0))

    def clear(k):
        here = pl.ds(pl.multiple_of(k * BLOCK, BLOCK), BLOCK)
        block = lax.broadcasted_iota(jnp.int32, (WIDTH, BLOCK), 0) // BLOCK
        x_ref[:, here] = jnp.where(block > k, 0.0, x_ref[:, here])

    def trail(m, n):
        at, to = slice(m * BLOCK, (m + 1) * BLOCK), slice(n * 2 * BLOCK, (n + 1) * 2 * BLOCK)
        product = dot(left_ref[at, :], right_ref[:, to]) + dot(left_ref[at, :BLOCK], rest_ref[:, to])
        x_ref[at, to] = x_ref[at, to] - product

    def factor_block(others):
        work_ref[:, BLOCK:] = jnp.where(r == c, 1.0, 0.0).astype(f32)
        emitted = 0
        for place, _ in enumerate(factor_tile(work_ref)):
            until = -(-len(others) * (place + 1) // (BLOCK // 2))
            for other in others[emitted:until]:
                other()
            emitted = until

    def prepare(k):
        here = pl.ds(pl.multiple_of(k * BLOCK, BLOCK), BLOCK)
        after = pl.ds(pl.multiple_of(jnp.minimum(k + 1, STEPS - 1) * BLOCK, BLOCK), BLOCK)
        d_ref[here, :] = jnp.where(r <= c, work_ref[:, :BLOCK], 0.0)
        inverse = work_ref[:, BLOCK:]
        inv_ref[...] = inverse
        u = dot_split_128(split(inverse), split(x_ref[here, after]))
        work_ref[:, :BLOCK] = x_ref[after, after] - dot_split_128(split(jnp.transpose(u)), split(u))

    def step(k, _, lowest=1):
        others = [functools.partial(finish_row, k - 1, b) for b in range(STEPS)]
        others += [functools.partial(clear, k - 1)]
        others += [functools.partial(trail, m, n) for n in range(STEPS // 2) for m in range(lowest, STEPS)]
        factor_block(others)
        prepare(k)
        return 0

    factor_block([])
    for copy in later:
        copy.wait()
    prepare(0)
    lax.fori_loop(1, STEPS // 2, step, 0)
    lax.fori_loop(STEPS // 2, STEPS, functools.partial(step, lowest=STEPS // 2), 0)
    end = slice(WIDTH - BLOCK, WIDTH)
    x_ref[end, :] = dot_split_128(split(inv_ref[...]), split(x_ref[end, :]))
    x_ref[end, end] = inv_ref[...]
    mh_ref[end, :], ml_ref[end, :] = split(x_ref[end, :])
    row, col = place_ref[0], place_ref[1]
    mine = pl.ds(pl.multiple_of(jnp.minimum(row, STEPS - 1) * BLOCK, BLOCK), BLOCK)
    other = pl.ds(pl.multiple_of(jnp.minimum(col, STEPS - 1) * BLOCK, BLOCK), BLOCK)
    block = jnp.where(row == col, d_ref[mine, :], x_ref[other, mine])
    corner_ref[...] = jnp.where(row >= col, jnp.transpose(block), 0.0)


def factor(place, gathered):
    vmem, hbm = pl.BlockSpec(memory_space=pltpu.VMEM), pl.BlockSpec(memory_space=pltpu.HBM)
    return pl.pallas_call(
        factor_kernel,
        in_specs=[pl.BlockSpec(memory_space=pltpu.SMEM), hbm],
        out_specs=(vmem, vmem, vmem),
        out_shape=(
            jax.ShapeDtypeStruct((WIDTH, WIDTH), bf16),
            jax.ShapeDtypeStruct((WIDTH, WIDTH), bf16),
            jax.ShapeDtypeStruct((BLOCK, BLOCK), f32),
        ),
        scratch_shapes=[
            pltpu.VMEM((WIDTH, WIDTH), f32),
            pltpu.VMEM((WIDTH, BLOCK), f32),
            pltpu.VMEM((BLOCK, 2 * BLOCK), f32),
            pltpu.VMEM((BLOCK, BLOCK), f32),
            pltpu.VMEM((WIDTH, 2 * BLOCK), bf16),
            pltpu.VMEM((2 * BLOCK, WIDTH), bf16),
            pltpu.VMEM((BLOCK, WIDTH), bf16),
            pltpu.SemaphoreType.DMA((2 * STEPS * SIDE,)),
        ],
        compiler_params=pltpu.CompilerParams(vmem_limit_bytes=24 * 2**20),
        cost_estimate=pl.CostEstimate(flops=40_000_000_000, bytes_accessed=2**23, transcendentals=0),
        name="factor",
    )(place, gathered)


def apply_kernel(place_ref, mh, ml, corner_ref, *refs):
    v_hbm, outs, (vh, vl, v_ref, sems) = refs[:SIDE], refs[SIDE : SIDE + 3], refs[SIDE + 3 :]
    count = iter(range(sems.shape[0]))
    copy = lambda src, dst: pltpu.make_async_copy(src, dst, sems.at[next(count)])
    arriving = [copy(v, v_ref.at[d]) for d, v in enumerate(v_hbm)]
    for c in arriving:
        c.start()
    row, col = place_ref[0], place_ref[1]
    other = pl.ds(pl.multiple_of(jnp.minimum(col, STEPS - 1) * BLOCK, BLOCK), BLOCK)
    sent = [copy(corner_ref, outs[2])]
    sent[0].start()
    my_y, my_x = row // SIDE, row % SIDE
    swapped = jnp.where((my_y == 1) | (my_y == 2), 1, 0)
    for d in range(SIDE):
        arriving[d].wait()
        for e in range(2):
            block = SIDE * (e + swapped - 2 * e * swapped) + (my_x + d) % SIDE
            at = pl.ds(pl.multiple_of(block * BLOCK, BLOCK), BLOCK)
            vh[at], vl[at] = split(v_ref[d, e * BLOCK : (e + 1) * BLOCK])
    for k in reversed(range(0, WIDTH, CHUNK)):
        at, upto = slice(k, k + CHUNK), slice(0, k + CHUNK)
        vh[at], vl[at] = split(dot_split((mh[at, upto], ml[at, upto]), (vh[upto], vl[upto])))
    for k in range(0, WIDTH, CHUNK):
        at, on = slice(k, k + CHUNK), slice(k, WIDTH)
        vh[at], vl[at] = split(dot_split((mh[on, at], ml[on, at]), (vh[on], vl[on]), ((0,), (0,))))
        for v, m in ((vh, mh), (vl, ml)):
            panel = jnp.transpose(m[other, at].astype(f32)).astype(bf16)
            v[at, :BLOCK] = jnp.where(col < STEPS, panel, v[at, :BLOCK])
        for v, out in zip((vh, vl), outs):
            sent.append(copy(v.at[at], out.at[at]))
            sent[-1].start()
    for c in sent:
        c.wait()


def apply(place, mh, ml, corner, across):
    vmem, hbm = pl.BlockSpec(memory_space=pltpu.VMEM), pl.BlockSpec(memory_space=pltpu.HBM)
    square = pltpu.VMEM((WIDTH, WIDTH), bf16)
    return pl.pallas_call(
        apply_kernel,
        in_specs=[pl.BlockSpec(memory_space=pltpu.SMEM), vmem, vmem, vmem] + [hbm] * SIDE,
        out_specs=(hbm,) * 3,
        out_shape=(pltpu.HBM((WIDTH, WIDTH), bf16), pltpu.HBM((WIDTH, WIDTH), bf16), pltpu.HBM((BLOCK, BLOCK), f32)),
        scratch_shapes=[square, square]
        + [
            pltpu.VMEM((SIDE, 2 * BLOCK, WIDTH), f32),
            pltpu.SemaphoreType.DMA((SIDE + 1 + 2 * (WIDTH // CHUNK),)),
        ],
        compiler_params=pltpu.CompilerParams(vmem_limit_bytes=20 * 2**20),
        cost_estimate=pl.CostEstimate(flops=10_000_000_000, bytes_accessed=2**23, transcendentals=0),
        name="apply",
    )(place, mh, ml, corner, *across)


def update_kernel(place_ref, a_ref, u_ref, yh_ref, yl_ref, corner_ref, out_ref):
    row, col, step = place_ref[0], place_ref[1], pl.program_id(0)
    slots = [jnp.where(step < HALF // CHUNK, j, other_half(j) - STEPS) for j in range(STEPS)]
    u = split(jnp.concatenate([u_ref[s] for s in slots], 1))
    product = dot_split(u, (yh_ref[...], yl_ref[...]))
    out_ref[:, :BLOCK] = jnp.where(col < STEPS, product[:, :BLOCK], a_ref[:, :BLOCK] - product[:, :BLOCK])
    out_ref[:, BLOCK:] = a_ref[:, BLOCK:] - product[:, BLOCK:]

    @pl.when((step == 0) & (row < STEPS))
    def _():
        out_ref[:BLOCK, :] = jnp.zeros((BLOCK, WIDTH), f32)

        @pl.when(col < STEPS)
        def _():
            out_ref[:BLOCK, :BLOCK] = corner_ref[...]


def update(place, blocked, gathered, yh, yl, corner):
    per_half = HALF // CHUNK
    whole = lambda *shape: pl.BlockSpec(shape, lambda i: (0, 0))
    return pl.pallas_call(
        update_kernel,
        grid=(WIDTH // CHUNK,),
        in_specs=[
            pl.BlockSpec(memory_space=pltpu.SMEM),
            pl.BlockSpec((CHUNK, WIDTH), lambda i: (i, 0)),
            pl.BlockSpec((STEPS, CHUNK, BLOCK), lambda i: (i // per_half, i % per_half, 0)),
            whole(WIDTH, WIDTH),
            whole(WIDTH, WIDTH),
            whole(BLOCK, BLOCK),
        ],
        out_specs=pl.BlockSpec((CHUNK, WIDTH), lambda i: (i, 0)),
        out_shape=jax.ShapeDtypeStruct((WIDTH, WIDTH), f32),
        compiler_params=pltpu.CompilerParams(vmem_limit_bytes=28 * 2**20),
        name="update",
    )(place, blocked, gathered, yh, yl, corner)


def per_device(blocked):
    rows, cols = lax.axis_size("prow"), lax.axis_size("pcol")
    row, col = lax.axis_index("prow"), lax.axis_index("pcol")
    span = range(STEPS)
    in_hbm = lambda a: pltpu.with_memory_space_constraint(a, pltpu.HBM)

    quarter = BLOCK // 4
    corner = blocked[:BLOCK, :BLOCK]
    parts = []
    for b, a in ((1, 1), (1, 0), (0, 1)):
        pairs = []
        for i in span:
            to_row = (SIDE - 1 - i // SIDE) * SIDE + i % SIDE if a else i
            for k in span:
                pairs.append((i * cols + k, to_row * cols + (other_half(k) if b else k)))
        at = (2 * b + a) * quarter
        parts.append(lax.ppermute(corner[at : at + quarter], ("prow", "pcol"), pairs))
    stays = (row < STEPS) & (col < STEPS)
    part = jnp.where(stays, corner[:quarter], parts[0] + parts[1] + parts[2])
    lower = lax.ppermute(blocked[HALF:, :BLOCK], "pcol", [(k, other_half(k)) for k in span])
    strip = lax.all_to_all(jnp.broadcast_to(part, (rows, quarter, BLOCK)), "prow", 0, 0)
    window = lax.all_gather(strip.reshape(HALF, BLOCK), "pcol", axis=0)
    window = window.reshape(cols, SIDE, SIDE, quarter, BLOCK)
    payload = jnp.where(col < STEPS, blocked[:HALF, :BLOCK], lower)

    own = blocked[:BLOCK]
    moves = ([(0, 1), (1, 0)], [(0, 3), (1, 2)], [(0, 2), (1, 3)])
    got = []
    for move in moves:
        got.append(lax.ppermute(own, "prow", [(a * SIDE + x, b * SIDE + x) for a, b in move for x in range(SIDE)]))
    source = row < 2 * SIDE
    pair = jnp.concatenate([jnp.where(source, own, got[1]), jnp.where(source, got[0], got[2])], 0)
    payload, window, _ = lax.optimization_barrier((payload, window, pair))
    panels = lax.all_gather(payload, "pcol", axis=0)
    across = [pair]
    for d in range(1, SIDE):
        across.append(lax.ppermute(pair, "prow", [(r // SIDE * SIDE + (r + d) % SIDE, r) for r in range(rows)]))

    place = jnp.stack([row, col])
    mh, ml, corner = factor(place, in_hbm(window))
    applied = apply(place, mh, ml, corner, across)
    return update(place, *(in_hbm(v) for v in (blocked, panels, *applied)))


def solution(mesh):
    return jax.shard_map(
        per_device,
        mesh=mesh,
        in_specs=(P("prow", "pcol"),),
        out_specs=P("prow", "pcol"),
        check_vma=False,
    )
```
